32 devices in a mesh: grp: 2 (over y), lat: 4 (over z), lon: 2 (over x), ch: 2 (over core).
Axes of the slice: x: 2, y: 2, z: 4, core: 2. Of those that a mesh axis runs over, the one named last changes fastest.
Arguments:
- noisy_state: bfloat16 [256, 32, 512], P(('grp', 'ch'), 'lat', 'lon'), parts along dimension 0, may hold values from -6 to 6
- kernel_in: bfloat16 [3, 3, 128, 128], replicated, may hold values from -0.1875 to 0.1875
- bias_in: float32 [128], replicated, may hold values from -4 to 4
- kernel_out: bfloat16 [3, 3, 128, 128], replicated, may hold values from -0.1875 to 0.1875
- interp_weight: bfloat16 [64, 128, 128], P(('grp', 'lat', 'lon')), parts along dimension 0, may hold values from -0.5 to 0.5
- observed: bfloat16 [64, 128, 128], P(('grp', 'lat', 'lon'), 'ch'), parts along dimension 0, may hold values from -6 to 6
- obs_precision: bfloat16 [64, 128], P(('grp', 'lat', 'lon')), parts along dimension 0, may hold values from 0.29882812 to 3
- dest_tile: int32 [64], P(('grp', 'lat', 'lon')), parts along dimension 0, may hold values from 0 to 3, as said below
- row_offset: int32 [64], P(('grp', 'lat', 'lon')), parts along dimension 0, may hold values from 0 to 4
- col_offset: int32 [64], P(('grp', 'lat', 'lon')), parts along dimension 0, may hold values from 0 to 224
Outputs:
- next_state: float32 [256, 32, 512], P(('grp', 'ch'), 'lat', 'lon'), parts along dimension 0
- innovation: bfloat16 [64, 128, 128], P(('grp', 'lat', 'lon'), 'ch'), parts along dimension 0
The draws below stay inside these ranges and needn't reach their ends.
There are 2 independent parts, one for each index of `grp`. The reference program is written for one: setup_inputs(seed, part) draws one part's arguments, and reference() takes and returns one part's arrays. A program takes and returns all parts, laid end to end along the dimension named above; an argument that names none is the same for every part. Nothing has to cross between parts.
Inputs may be any that keep to these rules, and one draw needn't show every extreme that they name: `dest_tile`: the 4 blocks of one device name any one latitude tile at most 2 times; a block's tile lies in the longitude column of the device that holds the block.
All inputs are finite; a program needn't handle non-finite values.
Results may differ from the reference program's by a relative error of at most 0.0085.
Values may be sent and summed in bfloat16 or wider, within the bound.
A program may use at most 64 MiB of HBM per device.

```python
import math
import jax
import jax.numpy as jnp
from jax import lax

C = 128
TH = 8
TW = 256
OBS = 128
PH = 4
PW = 32
CAP = 2
P_SIZE = 128
NB_DEV = 4
BLOCKS = 32
GRID_LAT = 32
GRID_LON = 512
N_LAT = 4
N_LON = 2


def draw_dest_tile(key, part):
    base = jax.random.fold_in(key, 101)
    key_busiest, key_popular, key_scores, key_reorder = jax.random.split(base, 4)
    sources = N_LAT * N_LON
    entries = N_LAT * CAP
    busiest = jax.random.randint(key_busiest, (), 0, N_LAT)
    popular = jax.random.randint(key_popular, (N_LAT,), 0, 4)
    entry_tile = jnp.arange(entries, dtype=jnp.int32) // CAP
    random_part = jax.random.randint(key_scores, (sources, entries), 0, 65536)
    scores = random_part + popular[entry_tile][None, :] * 16384 + jnp.where(entry_tile == busiest, 1048576, 0)[None, :]
    scores = scores * entries + jnp.arange(entries, dtype=jnp.int32)[None, :]
    picked = lax.top_k(scores, NB_DEV)[1]
    lat_tiles = picked // CAP
    reorder_key = jax.random.randint(key_reorder, (sources, NB_DEV), 0, 65536) * NB_DEV + jnp.arange(NB_DEV, dtype=jnp.int32)[None, :]
    reorder = jnp.argsort(reorder_key, axis=1, stable=True)
    return jnp.take_along_axis(lat_tiles, reorder, axis=1).reshape(-1).astype(jnp.int32)


def place_ends(drawn, stream_key, least, largest):
    longest = drawn.shape.index(max(drawn.shape))
    spots = []
    for shift in (0, 1):
        where = [jax.random.randint(jax.random.fold_in(stream_key, axis), (), 0, length) for axis, length in enumerate(drawn.shape)]
        where[longest] = (where[longest] + shift) % drawn.shape[longest]
        spots.append(tuple(where))
    return drawn.at[spots[0]].set(least).at[spots[1]].set(largest)


def steps_of(key, extent, shards, low, top_value):
    level, own = 1.0, jax.random.fold_in(key, 6)
    for axis_at, shards_of in shards:
        draws = jnp.exp(jax.random.uniform(jax.random.fold_in(own, axis_at), (shards_of,), jnp.float32, low / len(shards), top_value / len(shards)))
        level = level * jnp.repeat(draws, extent[axis_at] // shards_of).reshape([-1 if axis == axis_at else 1 for axis in range(len(extent))])
    return level


def gaussian(rng, extent, deviation, most, cuts=(), held_as=jnp.bfloat16):
    result = jax.random.normal(rng, extent, jnp.float32) * deviation
    if len(cuts) > 0:
        result = steps_of(rng, extent, cuts, -0.22, 0.18) * result
    return jnp.clip(result, min=-most, max=most).astype(held_as)


def setup_inputs(seed: int = 0, part: int = 0) -> dict:
    splits = jax.random.split(jax.random.key(seed), 11)
    own_keys = jax.random.split(jax.random.fold_in(splits[10], part), 11)
    noisy_state = gaussian(own_keys[0], (C, GRID_LAT, GRID_LON), 1.0, 6.0, ((0, 2), (1, 4), (2, 2)))
    kernel_in = gaussian(splits[1], (3, 3, C, C), (9 * C) ** -0.5, 0.1875)
    bias_in = gaussian(splits[2], (C,), 1.0, 4.0, (), jnp.float32)
    kernel_out = gaussian(splits[3], (3, 3, C, C), (9 * C) ** -0.5, 0.1875)
    interp_weight = gaussian(own_keys[4], (BLOCKS, OBS, P_SIZE), P_SIZE ** -0.5, 0.5, ((0, 8),))
    observed = gaussian(own_keys[5], (BLOCKS, C, OBS), 1.0, 6.0, ((0, 8), (1, 2)))
    obs_precision = jnp.clip(jnp.exp(math.log(3.0) - 2.306499 * jax.random.uniform(own_keys[6], (BLOCKS, OBS), jnp.float32) ** steps_of(own_keys[6], (BLOCKS, OBS), ((0, 8),), -0.2, 0.2)), 0.29882812, 3.0).astype(jnp.bfloat16)
    dest_tile = draw_dest_tile(jax.random.fold_in(jax.random.fold_in(splits[10], part), 71), part)
    row_offset = place_ends(jax.random.randint(own_keys[8], (BLOCKS,), 0, TH - PH + 1), jax.random.fold_in(own_keys[8], 1), 0, TH - PH).astype(jnp.int32)
    col_offset = place_ends(jax.random.randint(own_keys[9], (BLOCKS,), 0, TW - PW + 1), jax.random.fold_in(own_keys[9], 1), 0, TW - PW).astype(jnp.int32)
    return {"noisy_state": noisy_state, "kernel_in": kernel_in, "bias_in": bias_in, "kernel_out": kernel_out, "interp_weight": interp_weight, "observed": observed, "obs_precision": obs_precision, "dest_tile": dest_tile, "row_offset": row_offset, "col_offset": col_offset}


def pad_field(grid_field):
    taller = jnp.pad(grid_field, ((0, 0), (1, 1), (0, 0)))
    return jnp.concatenate([taller[:, :, -1:], taller, taller[:, :, :1]], axis=2)


def convolve(grid_field, kernel):
    padded = pad_field(grid_field)
    channels, grid_rows, grid_cols = grid_field.shape
    summed = jnp.zeros((kernel.shape[2], grid_rows * grid_cols), jnp.float32)
    for tap_row in range(3):
        for tap_col in range(3):
            window = padded[:, tap_row:tap_row + grid_rows, tap_col:tap_col + grid_cols].reshape(channels, grid_rows * grid_cols)
            summed = summed + jnp.dot(kernel[tap_row, tap_col], window, preferred_element_type=jnp.float32)
    return summed.reshape(kernel.shape[2], grid_rows, grid_cols)


def adjoint_kernel(kernel):
    return jnp.transpose(kernel[::-1, ::-1], (0, 1, 3, 2))


def extract(grid_field, patch_rows, patch_cols):
    def take_one(row_start, col_start):
        return lax.dynamic_slice(grid_field, (jnp.zeros((), jnp.int32), row_start, col_start), (grid_field.shape[0], PH, PW))
    return jax.vmap(take_one)(patch_rows, patch_cols)


def spread(grad_patch, patch_rows, patch_cols, grid_shape):
    cell_rows = patch_rows[:, None, None] + lax.broadcasted_iota(jnp.int32, (1, PH, 1), 1)
    cell_cols = patch_cols[:, None, None] + lax.broadcasted_iota(jnp.int32, (1, 1, PW), 2)
    return jnp.zeros(grid_shape, jnp.float32).at[:, cell_rows, cell_cols].add(jnp.moveaxis(grad_patch, 1, 0))


def reference(noisy_state, kernel_in, bias_in, kernel_out, interp_weight, observed, obs_precision, dest_tile, row_offset, col_offset):
    pre_act = convolve(noisy_state, kernel_in) + bias_in[:, None, None]
    hidden = jax.nn.silu(pre_act).astype(jnp.bfloat16)
    denoised = (noisy_state.astype(jnp.float32) + convolve(hidden, kernel_out)).astype(jnp.bfloat16)
    blocks = dest_tile.shape[0]
    device_of = jnp.arange(blocks, dtype=jnp.int32) // NB_DEV
    patch_rows = (dest_tile * TH + row_offset).astype(jnp.int32)
    patch_cols = ((device_of % N_LON) * TW + col_offset).astype(jnp.int32)
    patches = extract(denoised, patch_rows, patch_cols).reshape(blocks, noisy_state.shape[0], PH * PW)
    predicted = jnp.einsum("scp,sop->sco", patches.astype(jnp.float32), interp_weight.astype(jnp.float32))
    residual = predicted - observed.astype(jnp.float32)
    innovation = residual.astype(jnp.bfloat16)
    weighted = (residual * obs_precision.astype(jnp.float32)[:, None, :]).astype(jnp.bfloat16)
    pulled = jnp.einsum("sco,sop->scp", weighted.astype(jnp.float32), interp_weight.astype(jnp.float32))
    grad_field = spread(pulled.reshape(blocks, noisy_state.shape[0], PH, PW), patch_rows, patch_cols, noisy_state.shape)
    grad_round = grad_field.astype(jnp.bfloat16)
    back_hidden = convolve(grad_round, adjoint_kernel(kernel_out))
    sigmoid_act = jax.nn.sigmoid(pre_act)
    grad_pre = (back_hidden * sigmoid_act * (1.0 + pre_act * (1.0 - sigmoid_act))).astype(jnp.bfloat16)
    grad_state = grad_field + convolve(grad_pre, adjoint_kernel(kernel_in))
    next_state = 0.6 * noisy_state.astype(jnp.float32) + 0.4 * denoised.astype(jnp.float32) - 0.3 * grad_state
    return next_state, innovation
```

```python
import functools

import jax
import jax.numpy as jnp
from jax import lax
from jax.experimental import pallas as pl
from jax.experimental.pallas import tpu as pltpu
from jax.sharding import PartitionSpec as P

PH = 4
PW = 32
CAP = 2
HALO = 2
SIDE = 16
META = 16
GROUP = 8
WIDE = 4

keep_rate = 0.6
blend_rate = 0.4
guide_rate = 0.3

MESH = pl.DeviceIdType.MESH
F32 = jnp.float32
BF16 = jnp.bfloat16


def kernel(
    n_lat, n_lon, rows, width, half, blocks,
    dest, row_off, col_off, x_hbm, kin_hbm, kout_hbm, bias, weight_hbm, values_hbm, scale_hbm,
    out, inn_out,
    xv, xs, x_send, kin, kout, weight, values, scale_raw, scale, kfi, kfo, load_sem,
    both, X, X3, H3, pre, base, D, E, pay, R, G, GF, inn, inn_r, out_h, out_s, out_r, pulled_s,
    plan, heard_up, heard_down,
    halo_s, halo_r, pair_s, pair_r, pay_s, pay_r, inn_ss, inn_rs,
):
    lat, lon, ch = lax.axis_index("lat"), lax.axis_index("lon"), lax.axis_index("ch")
    other = 1 - ch
    chans = 2 * half
    obs = weight_hbm.shape[1]
    cells = PH * PW
    pitch = width + 2 * SIDE
    slots = n_lat * CAP
    px = rows * width
    lon_right = lax.rem(lon + ch, n_lon)
    lon_left = lax.rem(lon + n_lon - other, n_lon)
    has_up = lat > 0
    has_down = lat < n_lat - 1
    sibling = {"ch": other}

    def at(dlat, side):
        place = {"lat": lat + dlat}
        if side:
            place["lon"] = lon_right if side > 0 else lon_left
            place["ch"] = other
        return place

    loads = [
        pltpu.make_async_copy(src, dst, load_sem.at[i])
        for i, (src, dst) in enumerate(
            [(x_hbm, xv), (weight_hbm, weight), (values_hbm, values), (scale_hbm, scale_raw),
             (kin_hbm, kin), (kout_hbm, kout)]
        )
    ]
    for load in loads:
        load.start()
    barrier = pltpu.get_barrier_semaphore()

    def greet(place):
        pl.semaphore_signal(barrier, inc=1, device_id=place, device_id_type=MESH)

    greet(at(0, -1))
    greet(at(0, 1))

    @pl.when(has_up)
    def _():
        for side in (-1, 0, 1):
            greet(at(-1, side))

    @pl.when(has_down)
    def _():
        for side in (-1, 0, 1):
            greet(at(1, side))

    def count_block(b, _):
        def earlier(e, rank):
            return rank + jnp.where(dest[e] == dest[b], 1, 0)

        plan[b] = dest[b] * CAP + lax.fori_loop(0, b, earlier, 0)
        return 0

    for b in range(blocks) if blocks <= 8 else ():
        rank = 0
        for e in range(b):
            rank = rank + jnp.where(dest[e] == dest[b], 1, 0)
        plan[b] = dest[b] * CAP + rank
    if blocks > 8:
        lax.fori_loop(0, blocks, count_block, 0)

    def pack_slot(s, _):
        def look(b, found):
            return jnp.where(plan[b] == s, b, found)

        found = lax.fori_loop(0, blocks, look, -1)
        source = jnp.maximum(found, 0)
        fill = jnp.where(found >= 0, 1.0, 0.0)
        w = (weight[source].astype(F32) * fill).astype(BF16)
        t = s // CAP
        k = s % CAP
        pay[t, k, 0:half] = w_half(w)
        pay[t, k, half:chans] = values[source]
        level = lax.broadcasted_iota(jnp.int32, (META, obs), 0)
        r0 = row_off[source].astype(F32)
        q0 = col_off[source].astype(F32)
        meta = jnp.where(level == 0, scale[pl.ds(source, 1), :], jnp.where(level == 1, r0, q0))
        pay[t, k, chans : chans + META] = meta.astype(BF16)
        return 0

    def w_half(w):
        return jnp.where(ch == 0, w[0:half].astype(F32), w[half:chans].astype(F32)).astype(BF16)

    loads[0].wait()
    for h in range(2):
        part = xv[:, :, h * width : (h + 1) * width].astype(F32)
        xs[h] = part.reshape(half * rows, width)
    for r in range(rows):
        both[ch, r] = xs[ch, pl.ds(r, half, stride=rows), :].astype(BF16)
        x_send[r] = xs[other, pl.ds(r, half, stride=rows), :].astype(BF16)

    tops = (lat + n_lat - 1) // n_lat
    bottoms = (2 * n_lat - 2 - lat) // n_lat
    pl.semaphore_wait(barrier, 2 + 3 * tops + 3 * bottoms)

    def tell(sem, dlat):
        pl.semaphore_signal(sem, inc=1, device_id={"lat": lat + dlat}, device_id_type=MESH)

    @pl.when((lat == 1) & has_down)
    def _():
        tell(heard_up, 1)

    @pl.when((lat == n_lat - 2) & has_up)
    def _():
        tell(heard_down, -1)

    def pair_copy(src, dst, i):
        return pltpu.make_async_remote_copy(
            src_ref=src, dst_ref=dst, send_sem=pair_s.at[i], recv_sem=pair_r.at[i],
            device_id=sibling, device_id_type=MESH,
        )

    reshard = pair_copy(x_send, both.at[ch], 0)
    reshard.start()
    for load in loads[1:4]:
        load.wait()
    scale[...] = scale_raw[...].astype(F32)
    lax.fori_loop(0, slots, pack_slot, 0)

    top, left = HALO, SIDE
    spans_r = {-1: (top, 0 + rows + top), 0: (top, top), 1: (top + rows - HALO, 0)}
    spans_c = {-1: (left, left + width), 0: (left, left), 1: (left + width - SIDE, 0)}
    size_r = {-1: HALO, 0: rows, 1: HALO}
    size_c = {-1: SIDE, 0: width, 1: SIDE}
    routes = [(0, -1), (0, 1), (-1, 0), (-1, -1), (-1, 1), (1, 0), (1, -1), (1, 1)]

    def halo_copy(buf, i, base_sem):
        dl, side = routes[i]
        sr, dr = spans_r[dl]
        sc, dc = spans_c[side]
        src = buf.at[pl.ds(sr, size_r[dl]), pl.ds(sc, size_c[side])]
        dst = buf.at[pl.ds(dr, size_r[dl]), pl.ds(dc, size_c[side])]
        return pltpu.make_async_remote_copy(
            src_ref=src, dst_ref=dst,
            send_sem=halo_s.at[base_sem + i], recv_sem=halo_r.at[base_sem + i],
            device_id=at(dl, side), device_id_type=MESH,
        )

    def halo_wait_recv(buf, i, base_sem):
        halo_copy(buf, i, base_sem).wait_recv()

    def guarded(dl, fn):
        if dl == 0:
            fn()
        else:
            pl.when(has_up if dl < 0 else has_down)(fn)

    def halo_start(buf, base_sem):
        for dl in (-1, 1, 0):
            def go(dl=dl):
                for i, route in enumerate(routes):
                    if route[0] == dl:
                        halo_copy(buf, i, base_sem).start()

            guarded(dl, go)

    def halo_finish(buf, base_sem, rows_of):
        for dl in rows_of:
            def go(dl=dl):
                for i, route in enumerate(routes):
                    if route[0] == dl:
                        halo_copy(buf, i, base_sem).wait_send()

            def got(dl=dl):
                for i, route in enumerate(routes):
                    if route[0] == dl:
                        halo_wait_recv(buf, i, base_sem)

            guarded(dl, go)
            guarded(-dl, got)

    def rim_conv(buf, base_sem, step):
        halo_finish(buf, base_sem, (0,))
        for r in range(HALO, HALO + rows):
            put_row(X3, r, buf[r].astype(F32))
        for r0 in range(HALO, rows, CH):
            step(r0)
        halo_finish(buf, base_sem, (-1, 1))
        for r in (0, 1, HALO + rows, HALO + rows + 1):
            put_row(X3, r, buf[r].astype(F32))
        for r0 in (0, rows):
            step(r0)

    CH = 2

    def clear_poles(buf):
        @pl.when(lat == 0)
        def _():
            buf[0:HALO] = jnp.zeros((HALO, pitch, chans), BF16)

        @pl.when(lat == n_lat - 1)
        def _():
            buf[rows + HALO : rows + 2 * HALO] = jnp.zeros((HALO, pitch, chans), BF16)

    def put_row(taps, r, v):
        taps[r * pitch : (r + 1) * pitch, 0:chans] = pltpu.roll(v, 1, 0).astype(BF16)
        taps[r * pitch : (r + 1) * pitch, chans : 2 * chans] = v.astype(BF16)
        taps[r * pitch : (r + 1) * pitch, 2 * chans :] = pltpu.roll(v, pitch - 1, 0).astype(BF16)

    def conv(taps, kmat, first, count):
        acc = None
        for a in range(3):
            part = jnp.dot(
                taps[(first + a) * pitch : (first + a + count) * pitch, :], kmat(a),
                preferred_element_type=F32,
            )
            acc = part if acc is None else acc + part
        return acc

    def mirrored(k, a):
        return jnp.concatenate([k[2 - a, 2], k[2 - a, 1], k[2 - a, 0]], axis=0)

    def edge_factor(r):
        if r == 0:
            return jnp.where(has_up, 1.0, 0.0)
        if r == rows + 1:
            return jnp.where(has_down, 1.0, 0.0)
        return None

    clear_poles(X)
    clear_poles(G)

    reshard.wait()
    for r in range(rows):
        X[top + r, left : left + width] = (
            jnp.concatenate([both[0, r], both[1, r]], axis=0).astype(F32).T.astype(BF16)
        )
    halo_start(X, 0)

    def pay_copy(i, step):
        peer = lax.rem(lat + step, n_lat)
        return pltpu.make_async_remote_copy(
            src_ref=pay.at[peer], dst_ref=R.at[lat, ch],
            send_sem=pay_s.at[i], recv_sem=pay_r.at[i],
            device_id={"lat": peer}, device_id_type=MESH,
        )

    def is_near(step):
        peer = lax.rem(lat + step, n_lat)
        return (peer == lat + 1) | (peer == lat - 1)

    for step in range(1, n_lat):
        @pl.when(is_near(step))
        def _(step=step):
            pay_copy(step - 1, step).start()

    @pl.when(lat >= 2)
    def _():
        pl.semaphore_wait(heard_up, 1)

        @pl.when(has_down)
        def _():
            tell(heard_up, 1)

    @pl.when(lat <= n_lat - 3)
    def _():
        pl.semaphore_wait(heard_down, 1)

        @pl.when(has_up)
        def _():
            tell(heard_down, -1)

    for step in range(1, n_lat):
        @pl.when(jnp.logical_not(is_near(step)))
        def _(step=step):
            pay_copy(step - 1, step).start()
    R[lat, ch] = pay[lat]
    for load in loads[4:]:
        load.wait()
    for a in range(3):
        for b in range(3):
            kfi[a, b * chans : (b + 1) * chans] = kin[a, b].astype(F32).T.astype(BF16)
            kfo[a, b * chans : (b + 1) * chans] = kout[a, b].astype(F32).T.astype(BF16)

    def hidden_rows(r0):
        acc = conv(X3, lambda a: kfi[a], r0, CH) + bias[...]
        pre[r0 * pitch : (r0 + CH) * pitch, :] = acc
        h = acc / (1.0 + jnp.exp(-acc))
        for i in range(CH):
            row = h[i * pitch : (i + 1) * pitch]
            f = edge_factor(r0 + i)
            if f is not None:
                row = row * f
            put_row(H3, r0 + i, row.astype(BF16).astype(F32))

    rim_conv(X, 0, hidden_rows)

    for r0 in range(0, rows, WIDE):
        acc = conv(H3, lambda a: kfo[a], r0, WIDE)
        for i in range(WIDE):
            r = r0 + i
            state = X[top + r, left : left + width].astype(F32)
            den = (state + acc[i * pitch + left : i * pitch + left + width]).astype(BF16)
            base[r * width : (r + 1) * width, :] = keep_rate * state + blend_rate * den.astype(F32)
            D[ch, :, r * width : (r + 1) * width] = den.astype(F32).T.astype(BF16)
    swap = pair_copy(D.at[ch], D.at[ch], 2)
    swap.start()

    for step in range(1, n_lat):
        pay_copy(step - 1, step).wait()
    forward = pair_copy(R.at[:, ch], R.at[:, ch], 1)
    forward.start()

    lane = lax.broadcasted_iota(jnp.int32, (1, cells), 1)
    cell_r = (lane // PW).astype(F32)
    cell_c = (lane % PW).astype(F32)

    def each_group(fn):
        if slots == GROUP:
            fn(0)
        else:
            lax.fori_loop(0, slots // GROUP, lambda g, _: fn(g) or 0, 0)

    def place_group(g):
        def place_rows(n, _):
            index = lax.broadcasted_iota(jnp.int32, (width, cells), 0) + n * width
            index = index.astype(F32)
            for i in range(GROUP):
                s = g * GROUP + i
                meta = R[s // CAP, ch, s % CAP, chans : chans + META].astype(F32)
                q = meta[2:3] + cell_c
                target = (meta[1:2] + cell_r) * width + q
                target = target + jnp.where(q >= width, float(px - width), 0.0)
                E[g, pl.ds(pl.multiple_of(n * width, width), width), i * cells : (i + 1) * cells] = (
                    jnp.where(index == target, 1.0, 0.0).astype(BF16)
                )
            return 0

        lax.fori_loop(0, 2 * rows, place_rows, 0)

    each_group(place_group)
    forward.wait()
    swap.wait()

    def observe_group(g):
        patches = jnp.dot(D[0], E[g, 0:px], preferred_element_type=F32) + jnp.dot(
            D[1], E[g, px : 2 * px], preferred_element_type=F32
        )
        patches = patches.astype(BF16)
        for i in range(GROUP):
            s = g * GROUP + i
            t = s // CAP
            k = s % CAP
            own = slice(i * cells, (i + 1) * cells)
            w = jnp.concatenate([R[t, 0, k, 0:half], R[t, 1, k, 0:half]], axis=0)
            val = jnp.concatenate([R[t, 0, k, half:chans], R[t, 1, k, half:chans]], axis=0)
            predicted = lax.dot_general(
                patches[:, own], w, (((1,), (1,)), ((), ())), preferred_element_type=F32
            )
            residual = predicted - val.astype(F32)
            inn[t, k] = jnp.where(ch == 0, residual[0:half], residual[half:chans]).astype(BF16)
            sc = R[t, 0, k, chans : chans + META].astype(F32)[0:1]
            weighted = (residual * sc).astype(BF16)
            pulled_s[g, :, own] = jnp.dot(weighted, w, preferred_element_type=F32).astype(BF16)

    each_group(observe_group)

    def spread_group(g):
        added = lax.dot_general(
            E[g, pl.ds(pl.multiple_of(ch * px, px), px)], pulled_s[g],
            (((1,), (1,)), ((), ())), preferred_element_type=F32,
        )
        if slots == GROUP:
            GF[...] = added
        else:
            GF[...] += added

    if slots != GROUP:
        GF[...] = jnp.zeros((px, chans), F32)
    each_group(spread_group)
    for r in range(rows):
        G[top + r, left : left + width] = GF[r * width : (r + 1) * width, :].astype(BF16)
    halo_start(G, 8)

    def inn_copy(i, step):
        peer = lax.rem(lat + step, n_lat)
        return pltpu.make_async_remote_copy(
            src_ref=inn.at[peer], dst_ref=inn_r.at[lat],
            send_sem=inn_ss.at[i], recv_sem=inn_rs.at[i],
            device_id={"lat": peer}, device_id_type=MESH,
        )

    for step in range(1, n_lat):
        inn_copy(step - 1, step).start()
    inn_r[lat] = inn[lat]

    def grad_rows(r0):
        back = conv(X3, lambda a: mirrored(kout, a), r0, CH)
        v = pre[r0 * pitch : (r0 + CH) * pitch, :]
        s = 1.0 / (1.0 + jnp.exp(-v))
        g = back * s * (1.0 + v * (1.0 - s))
        for i in range(CH):
            row = g[i * pitch : (i + 1) * pitch]
            f = edge_factor(r0 + i)
            if f is not None:
                row = row * f
            put_row(H3, r0 + i, row.astype(BF16).astype(F32))

    rim_conv(G, 8, grad_rows)
    mine = pl.ds(pl.multiple_of(ch * width, width), width)
    theirs = pl.ds(pl.multiple_of(other * width, width), width)
    back_home = []
    for r0 in range(0, rows, WIDE):
        acc = conv(H3, lambda a: mirrored(kin, a), r0, WIDE)
        for i in range(WIDE):
            r = r0 + i
            own = slice(r * width, (r + 1) * width)
            grad = GF[own, :] + acc[i * pitch + left : i * pitch + left + width]
            res = (base[own, :] - guide_rate * grad).T
            out_h[0, pl.ds(r, half, stride=rows), :] = jnp.where(ch == 0, res[0:half], res[half:chans])
            out_s[r] = jnp.where(ch == 0, res[half:chans], res[0:half]).astype(BF16)
        sent = pl.ds(r0, WIDE)
        back_home.append(pair_copy(out_s.at[sent], out_r.at[sent], 3 + r0 // WIDE))
        back_home[-1].start()
    out[:, mine] = out_h[0]
    for step in range(1, n_lat):
        inn_copy(step - 1, step).wait()

    def fetch(b, _):
        slot = plan[b]
        inn_out[b] = inn_r[slot // CAP, slot % CAP]
        return 0

    lax.fori_loop(0, blocks, fetch, 0)
    for i, copy in enumerate(back_home):
        copy.wait()
        for r in range(i * WIDE, (i + 1) * WIDE):
            out_h[1, pl.ds(r, half, stride=rows), :] = out_r[r].astype(F32)
    out[:, theirs] = out_h[1]


def body(n_lat, n_lon, noisy_state, kernel_in, bias_in, kernel_out, interp_weight, observed,
         obs_precision, dest_tile, row_offset, col_offset):
    half, rows, cols = noisy_state.shape
    chans = 2 * half
    width = cols // 2
    blocks, obs, cells = interp_weight.shape
    slots = n_lat * CAP
    pitch = width + 2 * SIDE
    px = rows * width
    vmem = pl.BlockSpec(memory_space=pltpu.VMEM)
    hbm = pl.BlockSpec(memory_space=pltpu.HBM)
    smem = pl.BlockSpec(memory_space=pltpu.SMEM)
    place = pltpu.VMEM if slots <= GROUP else jax.ShapeDtypeStruct
    call = pl.pallas_call(
        functools.partial(kernel, n_lat, n_lon, rows, width, half, blocks),
        out_shape=(
            place((half * rows, cols), F32),
            place((blocks, half, obs), BF16),
        ),
        in_specs=[smem] * 3 + [hbm] * 3 + [vmem] + [hbm] * 3,
        out_specs=(vmem, vmem),
        scratch_shapes=[
            pltpu.VMEM((half, rows, cols), BF16),
            pltpu.VMEM((2, half * rows, width), F32),
            pltpu.VMEM((rows, half, width), BF16),
            pltpu.VMEM(kernel_in.shape, BF16),
            pltpu.VMEM(kernel_out.shape, BF16),
            pltpu.VMEM(interp_weight.shape, BF16),
            pltpu.VMEM(observed.shape, BF16),
            pltpu.VMEM(obs_precision.shape, BF16),
            pltpu.VMEM(obs_precision.shape, F32),
            pltpu.VMEM((3, 3 * chans, chans), BF16),
            pltpu.VMEM((3, 3 * chans, chans), BF16),
            pltpu.SemaphoreType.DMA((6,)),
            pltpu.VMEM((2, rows, half, width), BF16),
            pltpu.VMEM((rows + 4, pitch, chans), BF16),
            pltpu.VMEM(((rows + 4) * pitch, 3 * chans), BF16),
            pltpu.VMEM(((rows + 2) * pitch, 3 * chans), BF16),
            pltpu.VMEM(((rows + 2) * pitch, chans), F32),
            pltpu.VMEM((px, chans), F32),
            pltpu.VMEM((2, chans, px), BF16),
            pltpu.VMEM((slots // GROUP, 2 * px, GROUP * cells), BF16),
            pltpu.VMEM((n_lat, CAP, chans + META, obs), BF16),
            pltpu.VMEM((n_lat, 2, CAP, chans + META, obs), BF16),
            pltpu.VMEM((rows + 4, pitch, chans), BF16),
            pltpu.VMEM((px, chans), F32),
            pltpu.VMEM((n_lat, CAP, half, obs), BF16),
            pltpu.VMEM((n_lat, CAP, half, obs), BF16),
            pltpu.VMEM((2, half * rows, width), F32),
            pltpu.VMEM((rows, half, width), BF16),
            pltpu.VMEM((rows, half, width), BF16),
            pltpu.VMEM((slots // GROUP, chans, GROUP * cells), BF16),
            pltpu.SMEM((blocks,), jnp.int32),
            pltpu.SemaphoreType.REGULAR,
            pltpu.SemaphoreType.REGULAR,
            pltpu.SemaphoreType.DMA((16,)),
            pltpu.SemaphoreType.DMA((16,)),
            pltpu.SemaphoreType.DMA((3 + rows // WIDE,)),
            pltpu.SemaphoreType.DMA((3 + rows // WIDE,)),
            pltpu.SemaphoreType.DMA((n_lat - 1,)),
            pltpu.SemaphoreType.DMA((n_lat - 1,)),
            pltpu.SemaphoreType.DMA((n_lat - 1,)),
            pltpu.SemaphoreType.DMA((n_lat - 1,)),
        ],
        compiler_params=pltpu.CompilerParams(
            collective_id=0, has_side_effects=True, vmem_limit_bytes=63 * 1024 * 1024
        ),
    )
    out, innovation = call(
        dest_tile, row_offset, col_offset, noisy_state, kernel_in, kernel_out,
        bias_in.reshape(1, chans), interp_weight, observed, obs_precision,
    )
    return out.reshape(half, rows, cols), innovation


def solution(mesh):
    return jax.shard_map(
        functools.partial(body, mesh.shape["lat"], mesh.shape["lon"]),
        mesh=mesh,
        in_specs=(
            P(("grp", "ch"), "lat", "lon"),
            P(),
            P(),
            P(),
            P(("grp", "lat", "lon"), None, None),
            P(("grp", "lat", "lon"), "ch", None),
            P(("grp", "lat", "lon"), None),
            P(("grp", "lat", "lon")),
            P(("grp", "lat", "lon")),
            P(("grp", "lat", "lon")),
        ),
        out_specs=(P(("grp", "ch"), "lat", "lon"), P(("grp", "lat", "lon"), "ch", None)),
        check_vma=False,
    )
```

```python
import functools

import jax
import jax.numpy as jnp
from jax import lax
from jax.experimental import pallas as pl
from jax.experimental.pallas import tpu as pltpu
from jax.sharding import PartitionSpec as P

PH = 4
PW = 32
CAP = 2
HALO = 2
SIDE = 16
GROUP = 8
WIDE = 4
SMALL = 8

keep_rate = 0.6
blend_rate = 0.4
guide_rate = 0.3

MESH = pl.DeviceIdType.MESH
F32 = jnp.float32
BF16 = jnp.bfloat16
I32 = jnp.int32


def sigmoid(v):
    return 0.5 + 0.5 * jnp.tanh(0.5 * v)


def each(count, fn):
    if count <= 8:
        for i in range(count):
            fn(i)
    else:
        lax.fori_loop(0, count, lambda i, _: fn(i) or 0, 0)


def kernel(
    n_lat, n_lon, rows, width, half, blocks,
    dest, row_off, col_off, x_hbm, kin_hbm, kout_hbm, bias, weight_hbm, values_hbm, scale_hbm,
    out, inn_out,
    xv, xs, x_send, kin, kout, weight, values, scale_raw, scale, kw, load_sem,
    both, X, X3, H3, slope, base, DF, den_s, den_r, pay, pay_at, pay_p, R, R_at, R_p, at_s,
    res_t, Z, G, GW, inn, inn_r, out_h, out_s, out_r,
    plan, heard_up, heard_down,
    halo_s, halo_r, pair_s, pair_r, pay_ss, pay_rs, at_ss, at_rs, p_ss, p_rs, fwd_s, fwd_r, copy_sem, inn_ss, inn_rs,
):
    lat, lon, ch = lax.axis_index("lat"), lax.axis_index("lon"), lax.axis_index("ch")
    other = 1 - ch
    chans = 2 * half
    obs = weight_hbm.shape[1]
    cells = PH * PW
    cols = 2 * width
    pitch = width + 2 * SIDE
    reach = width + SIDE
    strip = 2 * reach + PW
    blank = GROUP * PH * strip
    slots = n_lat * CAP
    sources = GROUP // CAP
    px = rows * width
    top, left = HALO, SIDE
    lon_right = lax.rem(lon + ch, n_lon)
    lon_left = lax.rem(lon + n_lon - other, n_lon)
    has_up = lat > 0
    has_down = lat < n_lat - 1
    sibling = {"ch": other}

    def at(dlat, side):
        place = {"lat": lat + dlat}
        if side:
            place["lon"] = lon_right if side > 0 else lon_left
            place["ch"] = other
        return place

    def outward(dlat):
        return {"lat": lat + dlat, "lon": jnp.where(ch == 0, lon_left, lon_right), "ch": other}

    def peer_of(j):
        m = jnp.minimum(lat, n_lat - 1 - lat)
        step = jnp.where(j < 2 * m, j // 2 + 1, j - m + 1)
        below = jnp.where(j < 2 * m, j % 2 == 0, lat > n_lat - 1 - lat)
        return jnp.where(below, lat - step, lat + step)

    loads = [
        pltpu.make_async_copy(src, dst, load_sem.at[i])
        for i, (src, dst) in enumerate(
            [(x_hbm, xv), (weight_hbm, weight), (values_hbm, values), (scale_hbm, scale_raw),
             (kin_hbm, kin), (kout_hbm, kout)]
        )
    ]
    for load in loads:
        load.start()
    barrier = pltpu.get_barrier_semaphore()

    def greet(place):
        pl.semaphore_signal(barrier, inc=1, device_id=place, device_id_type=MESH)

    greet(at(0, -1))
    greet(at(0, 1))

    @pl.when(has_up)
    def _():
        for side in (-1, 0, 1):
            greet(at(-1, side))

    @pl.when(has_down)
    def _():
        for side in (-1, 0, 1):
            greet(at(1, side))

    def count_block(b, _):
        def earlier(e, rank):
            return rank + jnp.where(dest[e] == dest[b], 1, 0)

        plan[b] = dest[b] * CAP + lax.fori_loop(0, b, earlier, 0)
        return 0

    for b in range(blocks) if blocks <= 8 else ():
        rank = 0
        for e in range(b):
            rank = rank + jnp.where(dest[e] == dest[b], 1, 0)
        plan[b] = dest[b] * CAP + rank
    if blocks > 8:
        lax.fori_loop(0, blocks, count_block, 0)

    def w_half(w):
        return jnp.where(ch == 0, w[0:half].astype(F32), w[half:chans].astype(F32)).astype(BF16)

    def pack_slot(s, _):
        def look(b, found):
            return jnp.where(plan[b] == s, b, found)

        found = lax.fori_loop(0, blocks, look, -1)
        source = jnp.maximum(found, 0)
        fill = jnp.where(found >= 0, 1.0, 0.0)
        w = (weight[source].astype(F32) * fill).astype(BF16)
        t = s // CAP
        k = s % CAP
        pay[t, k, 0:half] = w_half(w)
        pay[t, k, half:chans] = values[source]
        pay_p[t, pl.ds(k, 1), :] = scale[pl.ds(source, 1), :]
        pay_at[t, pl.ds(2 * k, 1), :] = jnp.full((1, obs), row_off[source], I32)
        pay_at[t, pl.ds(2 * k + 1, 1), :] = jnp.full((1, obs), col_off[source], I32)
        return 0

    loads[0].wait()
    for h in range(2):
        part = xv[:, :, h * width : (h + 1) * width].astype(F32)
        xs[h] = part.reshape(half * rows, width)
    for r in range(rows):
        both[ch, r] = xs[ch, pl.ds(r, half, stride=rows), :].astype(BF16)
        x_send[r] = xs[other, pl.ds(r, half, stride=rows), :].astype(BF16)

    tops = (lat + n_lat - 1) // n_lat
    bottoms = (2 * n_lat - 2 - lat) // n_lat
    pl.semaphore_wait(barrier, 2 + 3 * tops + 3 * bottoms)

    def tell(sem, dlat):
        pl.semaphore_signal(sem, inc=1, device_id={"lat": lat + dlat}, device_id_type=MESH)

    @pl.when((lat == 1) & has_down)
    def _():
        tell(heard_up, 1)

    @pl.when((lat == n_lat - 2) & has_up)
    def _():
        tell(heard_down, -1)

    def pair_copy(src, dst, i):
        return pltpu.make_async_remote_copy(
            src_ref=src, dst_ref=dst, send_sem=pair_s.at[i], recv_sem=pair_r.at[i],
            device_id=sibling, device_id_type=MESH,
        )

    reshard = pair_copy(x_send, both.at[ch], 0)
    reshard.start()
    for load in loads[1:4]:
        load.wait()
    scale[...] = scale_raw[...].astype(F32)
    pay_at[...] = jnp.zeros(pay_at.shape, I32)
    pay_p[...] = jnp.zeros(pay_p.shape, F32)
    lax.fori_loop(0, slots, pack_slot, 0)

    def put_row(taps, r, v):
        taps[r * pitch : (r + 1) * pitch, 0:chans] = pltpu.roll(v, 1, 0).astype(BF16)
        taps[r * pitch : (r + 1) * pitch, chans : 2 * chans] = v.astype(BF16)
        taps[r * pitch : (r + 1) * pitch, 2 * chans :] = pltpu.roll(v, pitch - 1, 0).astype(BF16)

    def conv(taps, kind, first, count):
        acc = None
        for a in range(3):
            part = jnp.dot(
                taps[(first + a) * pitch : (first + a + count) * pitch, :], kw[kind, a],
                preferred_element_type=F32,
            )
            acc = part if acc is None else acc + part
        return acc

    def edge_factor(r):
        if r == 0:
            return jnp.where(has_up, 1.0, 0.0)
        if r == rows + 1:
            return jnp.where(has_down, 1.0, 0.0)
        return None

    def guarded(dl, fn):
        if dl == 0:
            fn()
        else:
            pl.when(has_up if dl < 0 else has_down)(fn)

    def span(start, size):
        return pl.ds(start if isinstance(start, int) else pl.multiple_of(start, SIDE), size)

    def remote(buf, place, sr, dr, nr, sc, dc, nc, i):
        return pltpu.make_async_remote_copy(
            src_ref=buf.at[pl.ds(sr, nr), span(sc, nc)], dst_ref=buf.at[pl.ds(dr, nr), span(dc, nc)],
            send_sem=halo_s.at[i], recv_sem=halo_r.at[i], device_id=place, device_id_type=MESH,
        )

    span_r = {-1: (top, rows + top, HALO), 0: (top, top, rows), 1: (top + rows - HALO, 0, HALO)}
    span_c = {-1: (left, left + width, SIDE), 0: (left, left, width), 1: (left + width - SIDE, 0, SIDE)}

    def x_routes():
        i = 0
        routes = {-1: [], 0: [], 1: []}
        for dl, side in [(0, -1), (0, 1), (-1, 0), (-1, -1), (-1, 1), (1, 0), (1, -1), (1, 1)]:
            sr, dr, nr = span_r[dl]
            sc, dc, nc = span_c[side]
            routes[dl].append(remote(X, at(dl, side), sr, dr, nr, sc, dc, nc, i))
            i += 1
        return routes

    def g_routes():
        i = 8
        routes = {-1: [], 0: [], 1: []}
        out_src = left + ch * (width - SIDE)
        out_dst = other * (left + width)
        for dl in (0, -1, 1):
            sr, dr, nr = span_r[dl]
            if dl:
                routes[dl].append(remote(G, at(dl, 0), sr, dr, nr, other * SIDE, other * SIDE, reach, i))
                i += 1
            routes[dl].append(remote(G, outward(dl), sr, dr, nr, out_src, out_dst, SIDE, i))
            i += 1
        return routes

    def halo_start(routes, order):
        for dl in order:
            def go(dl=dl):
                for copy in routes[dl]:
                    copy.start()

            guarded(dl, go)

    def halo_finish(routes, order):
        for dl in order:
            def sent(dl=dl):
                for copy in routes[dl]:
                    copy.wait_send()

            def got(dl=dl):
                for copy in routes[dl]:
                    copy.wait_recv()

            guarded(dl, sent)
            guarded(-dl, got)

    def clear_poles(buf):
        @pl.when(lat == 0)
        def _():
            buf[0:HALO] = jnp.zeros((HALO, pitch, chans), BF16)

        @pl.when(lat == n_lat - 1)
        def _():
            buf[rows + HALO : rows + 2 * HALO] = jnp.zeros((HALO, pitch, chans), BF16)

    clear_poles(X)
    clear_poles(G)

    reshard.wait()
    for r in range(rows):
        X[top + r, left : left + width] = (
            jnp.concatenate([both[0, r], both[1, r]], axis=0).astype(F32).T.astype(BF16)
        )
    x_halo = x_routes()
    halo_start(x_halo, (-1, 1, 0))

    def pay_copies(peer):
        return [
            pltpu.make_async_remote_copy(
                src_ref=src.at[peer], dst_ref=dst, send_sem=ss.at[peer], recv_sem=rs.at[lat],
                device_id={"lat": peer}, device_id_type=MESH,
            )
            for src, dst, ss, rs in [
                (pay_at, R_at.at[lat], at_ss, at_rs), (pay_p, R_p.at[lat], p_ss, p_rs),
                (pay, R.at[lat, ch], pay_ss, pay_rs),
            ]
        ]

    def arrival(kind, peer):
        src, dst, ss, rs = [
            (pay_at.at[peer], R_at.at[peer], at_ss, at_rs), (pay_p.at[peer], R_p.at[peer], p_ss, p_rs),
            (pay.at[peer], R.at[peer, ch], pay_ss, pay_rs),
        ][kind]
        return pltpu.make_async_remote_copy(
            src_ref=src, dst_ref=dst, send_sem=ss.at[peer], recv_sem=rs.at[peer],
            device_id={"lat": peer}, device_id_type=MESH,
        )

    def start_pay(j, near):
        peer = peer_of(j)
        is_near = (peer == lat + 1) | (peer == lat - 1)

        @pl.when(is_near if near else jnp.logical_not(is_near))
        def _():
            for copy in pay_copies(peer):
                copy.start()

    each(min(2, n_lat - 1), lambda j: start_pay(j, True))

    @pl.when(lat >= 2)
    def _():
        pl.semaphore_wait(heard_up, 1)

        @pl.when(has_down)
        def _():
            tell(heard_up, 1)

    @pl.when(lat <= n_lat - 3)
    def _():
        pl.semaphore_wait(heard_down, 1)

        @pl.when(has_up)
        def _():
            tell(heard_down, -1)

    each(n_lat - 1, lambda j: start_pay(j, False))

    R[lat, ch] = pay[lat]
    R_at[lat] = pay_at[lat]
    R_p[lat] = pay_p[lat]

    def forward(t):
        return pltpu.make_async_remote_copy(
            src_ref=R.at[t, ch], dst_ref=R.at[t, ch], send_sem=fwd_s.at[t], recv_sem=fwd_r.at[t],
            device_id=sibling, device_id_type=MESH,
        )

    forward(lat).start()
    for load in loads[4:]:
        load.wait()
    for kind, k in enumerate((kin, kout, kout, kin)):
        for a in range(3):
            for b in range(3):
                tap = k[a, b].astype(F32).T.astype(BF16) if kind < 2 else k[2 - a, 2 - b]
                kw[kind, a, b * chans : (b + 1) * chans] = tap
    Z[...] = jnp.zeros(Z.shape, F32)

    def hidden_rows(r0, count):
        acc = conv(X3, 0, r0, count) + bias[...]
        s = sigmoid(acc)
        slope[r0 * pitch : (r0 + count) * pitch, :] = s * (1.0 + acc * (1.0 - s))
        h = acc * s
        for i in range(count):
            row = h[i * pitch : (i + 1) * pitch]
            f = edge_factor(r0 + i)
            if f is not None:
                row = row * f
            put_row(H3, r0 + i, row.astype(BF16).astype(F32))

    halo_finish(x_halo, (0,))
    for r in range(top, top + rows):
        put_row(X3, r, X[r].astype(F32))
    for r0 in range(HALO, rows, 2):
        hidden_rows(r0, 2)
    halo_finish(x_halo, (-1, 1))
    for r in (0, 1, top + rows, top + rows + 1):
        put_row(X3, r, X[r].astype(F32))
    hidden_rows(0, HALO)
    hidden_rows(rows, HALO)

    swaps = []
    for r0 in range(0, rows, WIDE):
        acc = conv(H3, 1, r0, WIDE)
        for i in range(WIDE):
            r = r0 + i
            state = X[top + r, left : left + width].astype(F32)
            den = (state + acc[i * pitch + left : i * pitch + left + width]).astype(BF16)
            den_s[r] = den
            wide = den.astype(F32)
            base[r * width : (r + 1) * width, :] = keep_rate * state + blend_rate * wide
            DF[pl.ds(pl.multiple_of(r * cols + ch * width, width), width), :] = wide
        part = pl.ds(r0, WIDE)
        swaps.append(pair_copy(den_s.at[part], den_r.at[part], 1 + r0 // WIDE))
        swaps[-1].start()

    def local_copy(t):
        return pltpu.make_async_copy(R_at.at[t], at_s.at[t], copy_sem.at[t])

    def take_small(j):
        peer = peer_of(j)
        for kind in (0, 1):
            arrival(kind, peer).wait()
        local_copy(peer).start()

    local_copy(lat).start()
    each(n_lat - 1, take_small)

    def take_pay(j):
        peer = peer_of(j)
        arrival(2, peer).wait()
        forward(peer).start()

    each(n_lat - 1, take_pay)
    for i, swap in enumerate(swaps):
        swap.wait()
        for r in range(i * WIDE, (i + 1) * WIDE):
            DF[pl.ds(pl.multiple_of(r * cols + other * width, width), width), :] = den_r[r].astype(F32)
    each(n_lat, lambda t: local_copy(t).wait())

    start = ch * (cols - reach)

    def source_of(j):
        return jnp.where(j == 0, lat, peer_of(jnp.maximum(j - 1, 0)))

    def observe(g, first):
        owners = [source_of(g * sources + i) for i in range(sources)]
        for t in owners:
            forward(t).wait()
        for i in range(GROUP):
            t, k = owners[i // CAP], i % CAP
            r0 = at_s[t, 2 * k, 0]
            q0 = at_s[t, 2 * k + 1, 0]
            w = jnp.concatenate([R[t, 0, k, 0:half], R[t, 1, k, 0:half]], axis=0)
            val = jnp.concatenate([R[t, 0, k, half:chans], R[t, 1, k, half:chans]], axis=0)
            prec = jnp.broadcast_to(R_p[t, k : k + 1, :], (chans, obs)).T
            patch = jnp.concatenate(
                [DF[pl.ds((r0 + a) * cols + q0, PW), :] for a in range(PH)], axis=0
            ).astype(BF16)
            predicted = jnp.dot(w, patch, preferred_element_type=F32)
            residual = predicted - val.astype(F32).T
            res_t[t, k] = residual
            weighted = (residual * prec).astype(BF16)
            pulled = jnp.dot(w.T, weighted, preferred_element_type=F32)
            for a in range(PH):
                Z[pl.ds((i * PH + a) * strip + reach, PW), :] = pulled[a * PW : (a + 1) * PW]
        for r in (0, 1, rows - 2, rows - 1, *range(2, rows - 2)):
            total = None
            for i in range(GROUP):
                t, k = owners[i // CAP], i % CAP
                r0 = at_s[t, 2 * k, 0]
                place = jnp.clip(at_s[t, 2 * k + 1, 0] - start, -PW, reach)
                inside = (r >= r0) & (r < r0 + PH)
                begin = jnp.where(inside, (i * PH + r - r0) * strip + reach - place, blank)
                v = Z[pl.ds(begin, reach), :]
                total = v if total is None else total + v
            span_w = pl.ds(pl.multiple_of(r * pitch + other * SIDE, SIDE), reach)
            if not first:
                total = total + GW[span_w, :]
            GW[span_w, :] = total
            G[top + r, pl.ds(pl.multiple_of(other * SIDE, SIDE), reach)] = total.astype(BF16)

    observe(0, True)
    if slots != GROUP:
        lax.fori_loop(1, slots // GROUP, lambda g, _: observe(g, False) or 0, 0)
    g_halo = g_routes()
    halo_start(g_halo, (-1, 1, 0))

    def turn(t):
        for k in range(CAP):
            res = res_t[t, k].T
            inn[t, k] = jnp.where(ch == 0, res[0:half], res[half:chans]).astype(BF16)

    each(n_lat, turn)

    def inn_copy(peer, landing):
        return pltpu.make_async_remote_copy(
            src_ref=inn.at[peer], dst_ref=inn_r.at[landing],
            send_sem=inn_ss.at[peer], recv_sem=inn_rs.at[landing],
            device_id={"lat": peer}, device_id_type=MESH,
        )

    each(n_lat - 1, lambda j: inn_copy(peer_of(j), lat).start())
    inn_r[lat] = inn[lat]

    def grad_rows(r0, count):
        g = conv(X3, 2, r0, count) * slope[r0 * pitch : (r0 + count) * pitch, :]
        for i in range(count):
            row = g[i * pitch : (i + 1) * pitch]
            f = edge_factor(r0 + i)
            if f is not None:
                row = row * f
            put_row(H3, r0 + i, row.astype(BF16).astype(F32))

    halo_finish(g_halo, (0,))
    for r in range(top, top + rows):
        put_row(X3, r, G[r].astype(F32))
    for r0 in range(HALO, rows, 2):
        grad_rows(r0, 2)
    halo_finish(g_halo, (-1, 1))
    for r in (0, 1, top + rows, top + rows + 1):
        put_row(X3, r, G[r].astype(F32))
    grad_rows(0, HALO)
    grad_rows(rows, HALO)

    mine = pl.ds(pl.multiple_of(ch * width, width), width)
    theirs = pl.ds(pl.multiple_of(other * width, width), width)
    back_home = []
    for r0 in range(0, rows, WIDE):
        acc = conv(H3, 3, r0, WIDE)
        for i in range(WIDE):
            r = r0 + i
            grad = GW[r * pitch + left : r * pitch + left + width, :] + acc[i * pitch + left : i * pitch + left + width]
            res = (base[r * width : (r + 1) * width, :] - guide_rate * grad).T
            out_h[0, pl.ds(r, half, stride=rows), :] = jnp.where(ch == 0, res[0:half], res[half:chans])
            out_s[r] = jnp.where(ch == 0, res[half:chans], res[0:half]).astype(BF16)
        sent = pl.ds(r0, WIDE)
        back_home.append(pair_copy(out_s.at[sent], out_r.at[sent], 1 + (rows + r0) // WIDE))
        back_home[-1].start()
    out[:, mine] = out_h[0]

    def take_inn(j):
        peer = peer_of(j)
        inn_copy(peer, peer).wait()

    each(n_lat - 1, take_inn)

    def fetch(b, _):
        slot = plan[b]
        inn_out[b] = inn_r[slot // CAP, slot % CAP]
        return 0

    lax.fori_loop(0, blocks, fetch, 0)
    for i, copy in enumerate(back_home):
        copy.wait()
        for r in range(i * WIDE, (i + 1) * WIDE):
            out_h[1, pl.ds(r, half, stride=rows), :] = out_r[r].astype(F32)
    out[:, theirs] = out_h[1]


def body(n_lat, n_lon, noisy_state, kernel_in, bias_in, kernel_out, interp_weight, observed,
         obs_precision, dest_tile, row_offset, col_offset):
    half, rows, cols = noisy_state.shape
    chans = 2 * half
    width = cols // 2
    blocks, obs, cells = interp_weight.shape
    slots = n_lat * CAP
    pitch = width + 2 * SIDE
    reach = width + SIDE
    px = rows * width
    pairs = 1 + 2 * (rows // WIDE)
    vmem = pl.BlockSpec(memory_space=pltpu.VMEM)
    hbm = pl.BlockSpec(memory_space=pltpu.HBM)
    smem = pl.BlockSpec(memory_space=pltpu.SMEM)
    dma = pltpu.SemaphoreType.DMA
    call = pl.pallas_call(
        functools.partial(kernel, n_lat, n_lon, rows, width, half, blocks),
        out_shape=(
            pltpu.VMEM((half * rows, cols), F32),
            pltpu.VMEM((blocks, half, obs), BF16),
        ),
        in_specs=[smem] * 3 + [hbm] * 3 + [vmem] + [hbm] * 3,
        out_specs=(vmem, vmem),
        scratch_shapes=[
            pltpu.VMEM((half, rows, cols), BF16),
            pltpu.VMEM((2, half * rows, width), F32),
            pltpu.VMEM((rows, half, width), BF16),
            pltpu.VMEM(kernel_in.shape, BF16),
            pltpu.VMEM(kernel_out.shape, BF16),
            pltpu.VMEM(interp_weight.shape, BF16),
            pltpu.VMEM(observed.shape, BF16),
            pltpu.VMEM(obs_precision.shape, BF16),
            pltpu.VMEM(obs_precision.shape, F32),
            pltpu.VMEM((4, 3, 3 * chans, chans), BF16),
            dma((6,)),
            pltpu.VMEM((2, rows, half, width), BF16),
            pltpu.VMEM((rows + 4, pitch, chans), BF16),
            pltpu.VMEM(((rows + 4) * pitch, 3 * chans), BF16),
            pltpu.VMEM(((rows + 2) * pitch, 3 * chans), BF16),
            pltpu.VMEM(((rows + 2) * pitch, chans), F32),
            pltpu.VMEM((px, chans), F32),
            pltpu.VMEM((rows * cols, chans), F32),
            pltpu.VMEM((rows, width, chans), BF16),
            pltpu.VMEM((rows, width, chans), BF16),
            pltpu.VMEM((n_lat, CAP, chans, obs), BF16),
            pltpu.VMEM((n_lat, SMALL, obs), I32),
            pltpu.VMEM((n_lat, SMALL, obs), F32),
            pltpu.VMEM((n_lat, 2, CAP, chans, obs), BF16),
            pltpu.VMEM((n_lat, SMALL, obs), I32),
            pltpu.VMEM((n_lat, SMALL, obs), F32),
            pltpu.SMEM((n_lat, SMALL, obs), I32),
            pltpu.VMEM((n_lat, CAP, obs, chans), F32),
            pltpu.VMEM((GROUP * PH * (2 * reach + PW) + reach, chans), F32),
            pltpu.VMEM((rows + 4, pitch, chans), BF16),
            pltpu.VMEM((rows * pitch, chans), F32),
            pltpu.VMEM((n_lat, CAP, half, obs), BF16),
            pltpu.VMEM((n_lat, CAP, half, obs), BF16),
            pltpu.VMEM((2, half * rows, width), F32),
            pltpu.VMEM((rows, half, width), BF16),
            pltpu.VMEM((rows, half, width), BF16),
            pltpu.SMEM((blocks,), I32),
            pltpu.SemaphoreType.REGULAR,
            pltpu.SemaphoreType.REGULAR,
            dma((13,)), dma((13,)),
            dma((pairs,)), dma((pairs,)),
            dma((n_lat,)), dma((n_lat,)),
            dma((n_lat,)), dma((n_lat,)),
            dma((n_lat,)), dma((n_lat,)),
            dma((n_lat,)), dma((n_lat,)),
            dma((n_lat,)),
            dma((n_lat,)), dma((n_lat,)),
        ],
        compiler_params=pltpu.CompilerParams(
            collective_id=0, has_side_effects=True, vmem_limit_bytes=(63 if slots <= GROUP else 48) * 1024 * 1024
        ),
    )
    out, innovation = call(
        dest_tile, row_offset, col_offset, noisy_state, kernel_in, kernel_out,
        bias_in.reshape(1, chans), interp_weight, observed, obs_precision,
    )
    return out.reshape(half, rows, cols), innovation


def solution(mesh):
    return jax.shard_map(
        functools.partial(body, mesh.shape["lat"], mesh.shape["lon"]),
        mesh=mesh,
        in_specs=(
            P(("grp", "ch"), "lat", "lon"),
            P(),
            P(),
            P(),
            P(("grp", "lat", "lon"), None, None),
            P(("grp", "lat", "lon"), "ch", None),
            P(("grp", "lat", "lon"), None),
            P(("grp", "lat", "lon")),
            P(("grp", "lat", "lon")),
            P(("grp", "lat", "lon")),
        ),
        out_specs=(P(("grp", "ch"), "lat", "lon"), P(("grp", "lat", "lon"), "ch", None)),
        check_vma=False,
    )
```

```python
import functools

import jax
import jax.numpy as jnp
from jax import lax
from jax.experimental import pallas as pl
from jax.experimental.pallas import tpu as pltpu
from jax.sharding import PartitionSpec as P

PH = 4
PW = 32
CAP = 2
HALO = 2
SIDE = 16
GROUP = 8
WIDE = 4
SMALL = 8

keep_rate = 0.6
blend_rate = 0.4
guide_rate = 0.3

MESH = pl.DeviceIdType.MESH
F32 = jnp.float32
BF16 = jnp.bfloat16
I32 = jnp.int32


def sigmoid(v):
    return 0.5 + 0.5 * jnp.tanh(0.5 * v)


def each(count, fn):
    if count <= 8:
        for i in range(count):
            fn(i)
    else:
        lax.fori_loop(0, count, lambda i, _: fn(i) or 0, 0)


def kernel(
    n_lat, n_lon, rows, width, half, blocks,
    dest, row_off, col_off, x_hbm, kin_hbm, kout_hbm, bias, weight_hbm, values_hbm, scale_hbm,
    out, inn_out,
    xv, xs, x_send, kin, kout, weight, values, scale_raw, scale, kw, load_sem,
    both, X, X3, H3, slope, base, DF, den_s, den_r, block_a, block_b, block_d,
    pay, pay_at, pay_p, R, R_at, R_p, at_s, patches, pat_s, pat_r, Z, G, GW, out_h, out_s, out_r,
    plan, heard_up, heard_down,
    halo_s, halo_r, pair_s, pair_r, pay_ss, pay_rs, at_ss, at_rs, p_ss, p_rs, fwd_s, fwd_r, copy_sem, pat_ss, pat_rs,
):
    lat, lon, ch = lax.axis_index("lat"), lax.axis_index("lon"), lax.axis_index("ch")
    other = 1 - ch
    chans = 2 * half
    obs = weight_hbm.shape[1]
    cells = PH * PW
    cols = 2 * width
    pitch = width + 2 * SIDE
    reach = width + SIDE
    strip = 2 * reach + PW
    blank = GROUP * PH * strip
    slots = n_lat * CAP
    sources = GROUP // CAP
    px = rows * width
    top, left = HALO, SIDE
    lon_right = lax.rem(lon + ch, n_lon)
    lon_left = lax.rem(lon + n_lon - other, n_lon)
    has_up = lat > 0
    has_down = lat < n_lat - 1
    sibling = {"ch": other}

    def at(dlat, side):
        place = {"lat": lat + dlat}
        if side:
            place["lon"] = lon_right if side > 0 else lon_left
            place["ch"] = other
        return place

    def outward(dlat):
        return {"lat": lat + dlat, "lon": jnp.where(ch == 0, lon_left, lon_right), "ch": other}

    def peer_of(j):
        m = jnp.minimum(lat, n_lat - 1 - lat)
        step = jnp.where(j < 2 * m, j // 2 + 1, j - m + 1)
        below = jnp.where(j < 2 * m, j % 2 == 0, lat > n_lat - 1 - lat)
        return jnp.where(below, lat - step, lat + step)

    loads = [
        pltpu.make_async_copy(src, dst, load_sem.at[i])
        for i, (src, dst) in enumerate(
            [(x_hbm, xv), (weight_hbm, weight), (values_hbm, values), (scale_hbm, scale_raw),
             (kin_hbm, kin), (kout_hbm, kout)]
        )
    ]
    for load in loads:
        load.start()
    barrier = pltpu.get_barrier_semaphore()

    def greet(place):
        pl.semaphore_signal(barrier, inc=1, device_id=place, device_id_type=MESH)

    greet(at(0, -1))
    greet(at(0, 1))

    @pl.when(has_up)
    def _():
        for side in (-1, 0, 1):
            greet(at(-1, side))

    @pl.when(has_down)
    def _():
        for side in (-1, 0, 1):
            greet(at(1, side))

    def count_block(b, _):
        def earlier(e, rank):
            return rank + jnp.where(dest[e] == dest[b], 1, 0)

        plan[b] = dest[b] * CAP + lax.fori_loop(0, b, earlier, 0)
        return 0

    for b in range(blocks) if blocks <= 8 else ():
        rank = 0
        for e in range(b):
            rank = rank + jnp.where(dest[e] == dest[b], 1, 0)
        plan[b] = dest[b] * CAP + rank
    if blocks > 8:
        lax.fori_loop(0, blocks, count_block, 0)

    quarter = half // 2
    packed = quarter + half

    def corner():
        return (
            lax.broadcasted_iota(I32, (half, cells), 0), lax.broadcasted_iota(I32, (half, cells), 1)
        )

    def prepare(b):
        row, lane = corner()
        w = weight[b]
        p = scale[pl.ds(b, 1), :]
        normal = jnp.dot((w.astype(F32).T * p).astype(BF16), w, preferred_element_type=F32)
        low = normal[half:cells]
        tri = jnp.where((lane < half) & (lane > row), pltpu.roll(low, half, 1), normal[0:half])
        tri = jnp.where(lane == row, 0.5 * tri, tri)
        block_a[b] = jnp.where(ch == 0, tri[0:quarter], tri[quarter:half])
        block_d[pl.ds(b, 1), :] = jnp.sum(jnp.where(lane == row + half, 0.5 * low, 0.0), axis=0, keepdims=True)
        block_b[b] = jnp.dot((values[b].astype(F32) * p).astype(BF16), w, preferred_element_type=F32)

    def pack_slot(s):
        def look(b, found):
            return jnp.where(plan[b] == s, b, found)

        found = lax.fori_loop(0, blocks, look, -1, unroll=blocks <= 8)
        source = jnp.maximum(found, 0)
        fill = jnp.where(found >= 0, 1.0, 0.0)
        t = s // CAP
        k = s % CAP
        pay[t, k, 0:quarter] = (block_a[source] * fill).astype(BF16)
        pay[t, k, quarter:packed] = (block_b[source] * fill).astype(BF16)
        pay_p[t, pl.ds(k, 1), :] = block_d[pl.ds(source, 1), :] * fill
        pay_at[t, pl.ds(2 * k, 1), :] = jnp.full((1, obs), row_off[source], I32)
        pay_at[t, pl.ds(2 * k + 1, 1), :] = jnp.full((1, obs), col_off[source], I32)

    loads[0].wait()
    for h in range(2):
        part = xv[:, :, h * width : (h + 1) * width].astype(F32)
        xs[h] = part.reshape(half * rows, width)
    for r in range(rows):
        both[ch, r] = xs[ch, pl.ds(r, half, stride=rows), :].astype(BF16)
        x_send[r] = xs[other, pl.ds(r, half, stride=rows), :].astype(BF16)

    tops = (lat + n_lat - 1) // n_lat
    bottoms = (2 * n_lat - 2 - lat) // n_lat
    pl.semaphore_wait(barrier, 2 + 3 * tops + 3 * bottoms)

    def tell(sem, dlat):
        pl.semaphore_signal(sem, inc=1, device_id={"lat": lat + dlat}, device_id_type=MESH)

    @pl.when((lat == 1) & has_down)
    def _():
        tell(heard_up, 1)

    @pl.when((lat == n_lat - 2) & has_up)
    def _():
        tell(heard_down, -1)

    def pair_copy(src, dst, i):
        return pltpu.make_async_remote_copy(
            src_ref=src, dst_ref=dst, send_sem=pair_s.at[i], recv_sem=pair_r.at[i],
            device_id=sibling, device_id_type=MESH,
        )

    reshard = pair_copy(x_send, both.at[ch], 0)
    reshard.start()
    for load in loads[1:4]:
        load.wait()
    scale[...] = scale_raw[...].astype(F32)
    pay_at[...] = jnp.zeros(pay_at.shape, I32)
    pay_p[...] = jnp.zeros(pay_p.shape, F32)
    each(blocks, prepare)
    each(slots, pack_slot)
    def pay_copies(peer, kinds):
        return [
            pltpu.make_async_remote_copy(
                src_ref=src.at[peer], dst_ref=dst, send_sem=ss.at[peer], recv_sem=rs.at[lat],
                device_id={"lat": peer}, device_id_type=MESH,
            )
            for src, dst, ss, rs in (
                (pay_at, R_at.at[lat], at_ss, at_rs), (pay_p, R_p.at[lat], p_ss, p_rs),
                (pay, R.at[lat, ch], pay_ss, pay_rs),
            )[kinds]
        ]

    def arrival(kind, peer):
        src, dst, ss, rs = [
            (pay_at.at[peer], R_at.at[peer], at_ss, at_rs), (pay_p.at[peer], R_p.at[peer], p_ss, p_rs),
            (pay.at[peer], R.at[peer, ch], pay_ss, pay_rs),
        ][kind]
        return pltpu.make_async_remote_copy(
            src_ref=src, dst_ref=dst, send_sem=ss.at[peer], recv_sem=rs.at[peer],
            device_id={"lat": peer}, device_id_type=MESH,
        )

    def start_pay(j, near, kinds=slice(0, 3)):
        peer = peer_of(j)
        is_near = (peer == lat + 1) | (peer == lat - 1)

        @pl.when(is_near if near else jnp.logical_not(is_near))
        def _():
            for copy in pay_copies(peer, kinds):
                copy.start()

    each(min(2, n_lat - 1), lambda j: start_pay(j, True))

    def put_row(taps, r, v):
        taps[r * pitch : (r + 1) * pitch, 0:chans] = pltpu.roll(v, 1, 0).astype(BF16)
        taps[r * pitch : (r + 1) * pitch, chans : 2 * chans] = v.astype(BF16)
        taps[r * pitch : (r + 1) * pitch, 2 * chans :] = pltpu.roll(v, pitch - 1, 0).astype(BF16)

    def conv(taps, kind, first, count):
        acc = None
        for a in range(3):
            part = jnp.dot(
                taps[(first + a) * pitch : (first + a + count) * pitch, :], kw[kind, a],
                preferred_element_type=F32,
            )
            acc = part if acc is None else acc + part
        return acc

    def edge_factor(r):
        if r == 0:
            return jnp.where(has_up, 1.0, 0.0)
        if r == rows + 1:
            return jnp.where(has_down, 1.0, 0.0)
        return None

    def guarded(dl, fn):
        if dl == 0:
            fn()
        else:
            pl.when(has_up if dl < 0 else has_down)(fn)

    def span(start, size):
        return pl.ds(start if isinstance(start, int) else pl.multiple_of(start, SIDE), size)

    def remote(buf, place, sr, dr, nr, sc, dc, nc, i):
        return pltpu.make_async_remote_copy(
            src_ref=buf.at[pl.ds(sr, nr), span(sc, nc)], dst_ref=buf.at[pl.ds(dr, nr), span(dc, nc)],
            send_sem=halo_s.at[i], recv_sem=halo_r.at[i], device_id=place, device_id_type=MESH,
        )

    span_r = {-1: (top, rows + top, HALO), 0: (top, top, rows), 1: (top + rows - HALO, 0, HALO)}
    span_c = {-1: (left, left + width, SIDE), 0: (left, left, width), 1: (left + width - SIDE, 0, SIDE)}

    def x_routes():
        i = 0
        routes = {-1: [], 0: [], 1: []}
        for dl, side in [(0, -1), (0, 1), (-1, 0), (-1, -1), (-1, 1), (1, 0), (1, -1), (1, 1)]:
            sr, dr, nr = span_r[dl]
            sc, dc, nc = span_c[side]
            routes[dl].append(remote(X, at(dl, side), sr, dr, nr, sc, dc, nc, i))
            i += 1
        return routes

    def g_routes():
        i = 8
        routes = {-1: [], 0: [], 1: []}
        out_src = left + ch * (width - SIDE)
        out_dst = other * (left + width)
        for dl in (0, -1, 1):
            sr, dr, nr = span_r[dl]
            if dl:
                routes[dl].append(remote(G, at(dl, 0), sr, dr, nr, other * SIDE, other * SIDE, reach, i))
                i += 1
            routes[dl].append(remote(G, outward(dl), sr, dr, nr, out_src, out_dst, SIDE, i))
            i += 1
        return routes

    def halo_start(routes, order):
        for dl in order:
            def go(dl=dl):
                for copy in routes[dl]:
                    copy.start()

            guarded(dl, go)

    def halo_finish(routes, order):
        for dl in order:
            def sent(dl=dl):
                for copy in routes[dl]:
                    copy.wait_send()

            def got(dl=dl):
                for copy in routes[dl]:
                    copy.wait_recv()

            guarded(dl, sent)
            guarded(-dl, got)

    def clear_poles(buf):
        @pl.when(lat == 0)
        def _():
            buf[0:HALO] = jnp.zeros((HALO, pitch, chans), BF16)

        @pl.when(lat == n_lat - 1)
        def _():
            buf[rows + HALO : rows + 2 * HALO] = jnp.zeros((HALO, pitch, chans), BF16)

    clear_poles(X)
    clear_poles(G)

    reshard.wait()
    for r in range(rows):
        X[top + r, left : left + width] = (
            jnp.concatenate([both[0, r], both[1, r]], axis=0).astype(F32).T.astype(BF16)
        )
    x_halo = x_routes()
    halo_start(x_halo, (-1, 1, 0))

    @pl.when(lat >= 2)
    def _():
        pl.semaphore_wait(heard_up, 1)

        @pl.when(has_down)
        def _():
            tell(heard_up, 1)

    @pl.when(lat <= n_lat - 3)
    def _():
        pl.semaphore_wait(heard_down, 1)

        @pl.when(has_up)
        def _():
            tell(heard_down, -1)

    each(n_lat - 1, lambda j: start_pay(j, False, slice(0, 2)))
    each(n_lat - 1, lambda j: start_pay(j, False, slice(2, 3)))

    R[lat, ch] = pay[lat]
    R_at[lat] = pay_at[lat]
    R_p[lat] = pay_p[lat]

    def forward(t):
        return pltpu.make_async_remote_copy(
            src_ref=R.at[t, ch], dst_ref=R.at[t, ch], send_sem=fwd_s.at[t], recv_sem=fwd_r.at[t],
            device_id=sibling, device_id_type=MESH,
        )

    forward(lat).start()
    for load in loads[4:]:
        load.wait()
    for kind, k in enumerate((kin, kout, kout, kin)):
        for a in range(3):
            for b in range(3):
                tap = k[a, b].astype(F32).T.astype(BF16) if kind < 2 else k[2 - a, 2 - b]
                kw[kind, a, b * chans : (b + 1) * chans] = tap
    Z[...] = jnp.zeros(Z.shape, F32)

    def hidden_rows(r0, count):
        acc = conv(X3, 0, r0, count) + bias[...]
        s = sigmoid(acc)
        slope[r0 * pitch : (r0 + count) * pitch, :] = s * (1.0 + acc * (1.0 - s))
        h = acc * s
        for i in range(count):
            row = h[i * pitch : (i + 1) * pitch]
            f = edge_factor(r0 + i)
            if f is not None:
                row = row * f
            put_row(H3, r0 + i, row.astype(BF16).astype(F32))

    halo_finish(x_halo, (0,))
    for r in range(top, top + rows):
        put_row(X3, r, X[r].astype(F32))
    for r0 in range(HALO, rows, 2):
        hidden_rows(r0, 2)
    swaps = []

    def denoise_rows(r0, count):
        acc = conv(H3, 1, r0, count)
        for i in range(count):
            r = r0 + i
            state = X[top + r, left : left + width].astype(F32)
            den = (state + acc[i * pitch + left : i * pitch + left + width]).astype(BF16)
            den_s[r] = den
            wide = den.astype(F32)
            base[r * width : (r + 1) * width, :] = keep_rate * state + blend_rate * wide
            DF[pl.ds(pl.multiple_of(r * cols + ch * width, width), width), :] = wide
        part = pl.ds(r0, count)
        swaps.append((r0, count, pair_copy(den_s.at[part], den_r.at[part], 1 + len(swaps))))
        swaps[-1][2].start()

    inner = [(r0, min(WIDE, rows - HALO - r0)) for r0 in range(HALO, rows - HALO, WIDE)]
    outer = [(0, HALO), (rows - HALO, HALO)]
    for r0, count in inner:
        denoise_rows(r0, count)
    halo_finish(x_halo, (-1, 1))
    for r in (0, 1, top + rows, top + rows + 1):
        put_row(X3, r, X[r].astype(F32))
    hidden_rows(0, HALO)
    hidden_rows(rows, HALO)
    for r0, count in outer:
        denoise_rows(r0, count)

    def local_copy(t):
        return pltpu.make_async_copy(R_at.at[t], at_s.at[t], copy_sem.at[t])

    def take_at(j):
        peer = peer_of(j)
        arrival(0, peer).wait()
        local_copy(peer).start()

    local_copy(lat).start()
    each(n_lat - 1, take_at)

    def take_pay(j):
        peer = peer_of(j)
        for kind in (1, 2):
            arrival(kind, peer).wait()
        forward(peer).start()

    each(n_lat - 1, take_pay)
    for r0, count, swap in swaps:
        swap.wait()
        for r in range(r0, r0 + count):
            DF[pl.ds(pl.multiple_of(r * cols + other * width, width), width), :] = den_r[r].astype(F32)
    each(n_lat, lambda t: local_copy(t).wait())

    def gather(t):
        lane = lax.broadcasted_iota(I32, (half, chans), 1)
        for k in range(CAP):
            r0 = at_s[t, 2 * k, 0]
            q0 = at_s[t, 2 * k + 1, 0]
            cut = [DF[pl.ds((r0 + a) * cols + q0, PW), :] for a in range(PH)]
            first = jnp.concatenate(cut[: PH // 2], axis=0)
            second = jnp.concatenate(cut[PH // 2 :], axis=0)
            patches[t, k, 0:half] = first.astype(BF16)
            patches[t, k, half:cells] = second.astype(BF16)
            keep_first = jnp.where(ch == 0, first, pltpu.roll(first, half, 1))
            keep_second = jnp.where(ch == 0, pltpu.roll(second, half, 1), second)
            pat_s[t, k] = jnp.where(lane < half, keep_first, keep_second).astype(BF16)

    each(n_lat, gather)

    def patch_copy(peer, landing):
        return pltpu.make_async_remote_copy(
            src_ref=pat_s.at[peer], dst_ref=pat_r.at[landing],
            send_sem=pat_ss.at[peer], recv_sem=pat_rs.at[landing],
            device_id={"lat": peer}, device_id_type=MESH,
        )

    each(n_lat - 1, lambda j: patch_copy(peer_of(j), lat).start())
    pat_r[lat] = pat_s[lat]
    start = ch * (cols - reach)

    def source_of(j):
        return jnp.where(j == 0, lat, peer_of(jnp.maximum(j - 1, 0)))

    def observe(g, first):
        owners = [source_of(g * sources + i) for i in range(sources)]
        for t in owners:
            forward(t).wait()
        for i in range(GROUP):
            t, k = owners[i // CAP], i % CAP
            row, lane = corner()
            tri = jnp.concatenate([R[t, 0, k, 0:quarter], R[t, 1, k, 0:quarter]], axis=0).astype(F32)
            upper = jnp.where((lane <= row) | (lane >= half), tri, 0.0)
            lower = jnp.where(lane > row + half, pltpu.roll(tri, half, 1), 0.0)
            lower = jnp.where(lane == row + half, R_p[t, k : k + 1, :], lower)
            side = jnp.concatenate([upper, lower], axis=0).astype(BF16)
            normal = side + side.T
            pull = jnp.concatenate([R[t, 0, k, quarter:packed], R[t, 1, k, quarter:packed]], axis=0)
            pulled = jnp.dot(normal, patches[t, k], preferred_element_type=F32) - pull.astype(F32).T
            for a in range(PH):
                Z[pl.ds((i * PH + a) * strip + reach, PW), :] = pulled[a * PW : (a + 1) * PW]
        for r in (0, 1, rows - 2, rows - 1, *range(2, rows - 2)):
            total = None
            for i in range(GROUP):
                t, k = owners[i // CAP], i % CAP
                r0 = at_s[t, 2 * k, 0]
                place = jnp.clip(at_s[t, 2 * k + 1, 0] - start, -PW, reach)
                inside = (r >= r0) & (r < r0 + PH)
                begin = jnp.where(inside, (i * PH + r - r0) * strip + reach - place, blank)
                v = Z[pl.ds(begin, reach), :]
                total = v if total is None else total + v
            span_w = pl.ds(pl.multiple_of(r * pitch + other * SIDE, SIDE), reach)
            if not first:
                total = total + GW[span_w, :]
            GW[span_w, :] = total
            G[top + r, pl.ds(pl.multiple_of(other * SIDE, SIDE), reach)] = total.astype(BF16)

    observe(0, True)
    if slots != GROUP:
        lax.fori_loop(1, slots // GROUP, lambda g, _: observe(g, False) or 0, 0)
    g_halo = g_routes()
    halo_start(g_halo, (-1, 1, 0))

    def grad_rows(r0, count):
        g = conv(X3, 2, r0, count) * slope[r0 * pitch : (r0 + count) * pitch, :]
        for i in range(count):
            row = g[i * pitch : (i + 1) * pitch]
            f = edge_factor(r0 + i)
            if f is not None:
                row = row * f
            put_row(H3, r0 + i, row.astype(BF16).astype(F32))

    halo_finish(g_halo, (0,))
    for r in range(top, top + rows):
        put_row(X3, r, G[r].astype(F32))
    for r0 in range(HALO, rows, 2):
        grad_rows(r0, 2)
    back_home = []

    def finish_rows(r0, count):
        acc = conv(H3, 3, r0, count)
        for i in range(count):
            r = r0 + i
            grad = GW[r * pitch + left : r * pitch + left + width, :] + acc[i * pitch + left : i * pitch + left + width]
            res = (base[r * width : (r + 1) * width, :] - guide_rate * grad).T
            out_s[r] = jnp.where(ch == 0, res[half:chans], res[0:half]).astype(BF16)
            out_h[0, pl.ds(r, half, stride=rows), :] = jnp.where(ch == 0, res[0:half], res[half:chans])
        part = pl.ds(r0, count)
        back_home.append((r0, count, pair_copy(out_s.at[part], out_r.at[part], 1 + len(swaps) + len(back_home))))
        back_home[-1][2].start()

    for r0, count in inner:
        finish_rows(r0, count)
    each(n_lat - 1, lambda j: patch_copy(peer_of(j), peer_of(j)).wait())

    def innovate(b):
        slot = plan[b]
        part = pat_r[slot // CAP, slot % CAP].astype(F32)
        patch = jnp.concatenate([part, pltpu.roll(part, half, 1)], axis=0).astype(BF16)
        predicted = jnp.dot(weight[b], patch, preferred_element_type=F32).T
        inn_out[b] = (predicted[0:half] - values[b].astype(F32)).astype(BF16)

    each(blocks, innovate)
    halo_finish(g_halo, (-1, 1))
    for r in (0, 1, top + rows, top + rows + 1):
        put_row(X3, r, G[r].astype(F32))
    grad_rows(0, HALO)
    grad_rows(rows, HALO)
    for r0, count in outer:
        finish_rows(r0, count)
    mine = pl.ds(pl.multiple_of(ch * width, width), width)
    theirs = pl.ds(pl.multiple_of(other * width, width), width)
    out[:, mine] = out_h[0]

    for r0, count, copy in back_home:
        copy.wait()
        for r in range(r0, r0 + count):
            out_h[1, pl.ds(r, half, stride=rows), :] = out_r[r].astype(F32)
    out[:, theirs] = out_h[1]


def store(out, innovation, out_hbm, innovation_hbm, sem):
    copies = [
        pltpu.make_async_copy(out, out_hbm, sem.at[0]),
        pltpu.make_async_copy(innovation, innovation_hbm, sem.at[1]),
    ]
    for copy in copies:
        copy.start()
    for copy in copies:
        copy.wait()


def body(n_lat, n_lon, noisy_state, kernel_in, bias_in, kernel_out, interp_weight, observed,
         obs_precision, dest_tile, row_offset, col_offset):
    half, rows, cols = noisy_state.shape
    chans = 2 * half
    width = cols // 2
    blocks, obs, cells = interp_weight.shape
    slots = n_lat * CAP
    pitch = width + 2 * SIDE
    reach = width + SIDE
    px = rows * width
    pairs = 1 + 2 * (2 - (HALO + HALO - rows) // WIDE)
    vmem = pl.BlockSpec(memory_space=pltpu.VMEM)
    hbm = pl.BlockSpec(memory_space=pltpu.HBM)
    smem = pl.BlockSpec(memory_space=pltpu.SMEM)
    dma = pltpu.SemaphoreType.DMA
    call = pl.pallas_call(
        functools.partial(kernel, n_lat, n_lon, rows, width, half, blocks),
        out_shape=(
            pltpu.VMEM((half * rows, cols), F32),
            pltpu.VMEM((blocks, half, obs), BF16),
        ),
        in_specs=[smem] * 3 + [hbm] * 3 + [vmem] + [hbm] * 3,
        out_specs=(vmem, vmem),
        scratch_shapes=[
            pltpu.VMEM((half, rows, cols), BF16),
            pltpu.VMEM((2, half * rows, width), F32),
            pltpu.VMEM((rows, half, width), BF16),
            pltpu.VMEM(kernel_in.shape, BF16),
            pltpu.VMEM(kernel_out.shape, BF16),
            pltpu.VMEM(interp_weight.shape, BF16),
            pltpu.VMEM(observed.shape, BF16),
            pltpu.VMEM(obs_precision.shape, BF16),
            pltpu.VMEM(obs_precision.shape, F32),
            pltpu.VMEM((4, 3, 3 * chans, chans), BF16),
            dma((6,)),
            pltpu.VMEM((2, rows, half, width), BF16),
            pltpu.VMEM((rows + 4, pitch, chans), BF16),
            pltpu.VMEM(((rows + 4) * pitch, 3 * chans), BF16),
            pltpu.VMEM(((rows + 2) * pitch, 3 * chans), BF16),
            pltpu.VMEM(((rows + 2) * pitch, chans), F32),
            pltpu.VMEM((px, chans), F32),
            pltpu.VMEM((rows * cols, chans), F32),
            pltpu.VMEM((rows, width, chans), BF16),
            pltpu.VMEM((rows, width, chans), BF16),
            pltpu.VMEM((blocks, half // 2, cells), F32),
            pltpu.VMEM((blocks, half, cells), F32),
            pltpu.VMEM((blocks, cells), F32),
            pltpu.VMEM((n_lat, CAP, half + half // 2, cells), BF16),
            pltpu.VMEM((n_lat, SMALL, obs), I32),
            pltpu.VMEM((n_lat, SMALL, obs), F32),
            pltpu.VMEM((n_lat, 2, CAP, half + half // 2, cells), BF16),
            pltpu.VMEM((n_lat, SMALL, obs), I32),
            pltpu.VMEM((n_lat, SMALL, obs), F32),
            pltpu.SMEM((n_lat, SMALL, obs), I32),
            pltpu.VMEM((n_lat, CAP, cells, chans), BF16),
            pltpu.VMEM((n_lat, CAP, half, chans), BF16),
            pltpu.VMEM((n_lat, CAP, half, chans), BF16),
            pltpu.VMEM((GROUP * PH * (2 * reach + PW) + reach, chans), F32),
            pltpu.VMEM((rows + 4, pitch, chans), BF16),
            pltpu.VMEM((rows * pitch, chans), F32),
            pltpu.VMEM((2, half * rows, width), F32),
            pltpu.VMEM((rows, half, width), BF16),
            pltpu.VMEM((rows, half, width), BF16),
            pltpu.SMEM((blocks,), I32),
            pltpu.SemaphoreType.REGULAR,
            pltpu.SemaphoreType.REGULAR,
            dma((13,)), dma((13,)),
            dma((pairs,)), dma((pairs,)),
            dma((n_lat,)), dma((n_lat,)),
            dma((n_lat,)), dma((n_lat,)),
            dma((n_lat,)), dma((n_lat,)),
            dma((n_lat,)), dma((n_lat,)),
            dma((n_lat,)),
            dma((n_lat,)), dma((n_lat,)),
        ],
        compiler_params=pltpu.CompilerParams(
            collective_id=0, has_side_effects=True, vmem_limit_bytes=(63 if slots <= GROUP else 48) * 1024 * 1024
        ),
    )
    out, innovation = call(
        dest_tile, row_offset, col_offset, noisy_state, kernel_in, kernel_out,
        bias_in.reshape(1, chans), interp_weight, observed, obs_precision,
    )
    out, innovation = pl.pallas_call(
        store,
        out_shape=(
            jax.ShapeDtypeStruct((half * rows, cols), F32),
            jax.ShapeDtypeStruct((blocks, half, obs), BF16),
        ),
        in_specs=[vmem, vmem],
        out_specs=(hbm, hbm),
        scratch_shapes=[dma((2,))],
    )(*(pltpu.with_memory_space_constraint(a, pltpu.VMEM) for a in (out, innovation)))
    return out.reshape(half, rows, cols), innovation


def solution(mesh):
    return jax.shard_map(
        functools.partial(body, mesh.shape["lat"], mesh.shape["lon"]),
        mesh=mesh,
        in_specs=(
            P(("grp", "ch"), "lat", "lon"),
            P(),
            P(),
            P(),
            P(("grp", "lat", "lon"), None, None),
            P(("grp", "lat", "lon"), "ch", None),
            P(("grp", "lat", "lon"), None),
            P(("grp", "lat", "lon")),
            P(("grp", "lat", "lon")),
            P(("grp", "lat", "lon")),
        ),
        out_specs=(P(("grp", "ch"), "lat", "lon"), P(("grp", "lat", "lon"), "ch", None)),
        check_vma=False,
    )
```

```python
import functools

import jax
import jax.numpy as jnp
from jax import lax
from jax.experimental import pallas as pl
from jax.experimental.pallas import tpu as pltpu
from jax.sharding import PartitionSpec as P

PH = 4
PW = 32
CAP = 2
HALO = 2
SIDE = 16
GROUP = 4
WIDE = 4
SMALL = 8

keep_rate = 0.6
blend_rate = 0.4
guide_rate = 0.3

MESH = pl.DeviceIdType.MESH
F32 = jnp.float32
BF16 = jnp.bfloat16
I32 = jnp.int32


def sigmoid(v):
    return 0.5 + 0.5 * jnp.tanh(0.5 * v)


def each(count, fn):
    if count <= 8:
        for i in range(count):
            fn(i)
    else:
        lax.fori_loop(0, count, lambda i, _: fn(i) or 0, 0)


def kernel(
    n_lat, n_lon, rows, width, half, blocks,
    dest, row_off, col_off, x_hbm, kin_hbm, kout_hbm, bias, weight_hbm, values_hbm, scale_hbm,
    out, inn_out,
    xv, xs, x_send, kin, kout, weight, values, scale_raw, scale, kw, load_sem,
    both, edge, edge_r, raw, edge_ss, edge_rs, raw_s, raw_r, X, X3, H3, slope, base, DF, den_s, den_r, block_a, block_b, block_d,
    pay, pay_at, pay_p, R, R_at, R_p, at_s, patches, pat_s, pat_r, Z, G, GW, out_h, out_s, out_r,
    plan, heard_up, heard_down,
    halo_s, halo_r, pair_s, pair_r, pay_ss, pay_rs, at_ss, at_rs, p_ss, p_rs, fwd_s, fwd_r, fat_s, fat_r, fp_s, fp_r, copy_sem, pat_ss, pat_rs,
):
    lat, lon, ch = lax.axis_index("lat"), lax.axis_index("lon"), lax.axis_index("ch")
    other = 1 - ch
    chans = 2 * half
    obs = weight_hbm.shape[1]
    cells = PH * PW
    cols = 2 * width
    pitch = width + 2 * SIDE
    reach = width + SIDE
    strip = 2 * reach + PW
    blank = GROUP * PH * strip
    slots = n_lat * CAP
    sources = GROUP // CAP
    px = rows * width
    top, left = HALO, SIDE
    lon_right = lax.rem(lon + ch, n_lon)
    lon_left = lax.rem(lon + n_lon - other, n_lon)
    has_up = lat > 0
    has_down = lat < n_lat - 1
    sibling = {"ch": other}

    def at(dlat, side):
        place = {"lat": lat + dlat}
        if side:
            place["lon"] = lon_right if side > 0 else lon_left
            place["ch"] = other
        return place

    def outward(dlat):
        return {"lat": lat + dlat, "lon": jnp.where(ch == 0, lon_left, lon_right), "ch": other}

    def peer_of(j):
        m = jnp.minimum(lat, n_lat - 1 - lat)
        step = jnp.where(j < 2 * m, j // 2 + 1, j - m + 1)
        below = jnp.where(j < 2 * m, j % 2 == 0, lat > n_lat - 1 - lat)
        return jnp.where(below, lat - step, lat + step)

    loads = [
        pltpu.make_async_copy(src, dst, load_sem.at[i])
        for i, (src, dst) in enumerate(
            [(x_hbm, xv), (weight_hbm, weight), (values_hbm, values), (scale_hbm, scale_raw),
             (kin_hbm, kin), (kout_hbm, kout)]
        )
    ]
    for load in loads:
        load.start()
    barrier = pltpu.get_barrier_semaphore()

    def greet(place):
        pl.semaphore_signal(barrier, inc=1, device_id=place, device_id_type=MESH)

    greet(at(0, -1))
    greet(at(0, 1))
    chip_left = lax.rem(lon + n_lon - 1, n_lon)
    chip_right = lax.rem(lon + 1, n_lon)
    greet({"lon": chip_left})
    greet({"lon": chip_right})

    @pl.when(has_up)
    def _():
        for side in (-1, 0, 1):
            greet(at(-1, side))

    @pl.when(has_down)
    def _():
        for side in (-1, 0, 1):
            greet(at(1, side))

    def count_block(b, _):
        def earlier(e, rank):
            return rank + jnp.where(dest[e] == dest[b], 1, 0)

        plan[b] = dest[b] * CAP + lax.fori_loop(0, b, earlier, 0)
        return 0

    for b in range(blocks) if blocks <= 8 else ():
        rank = 0
        for e in range(b):
            rank = rank + jnp.where(dest[e] == dest[b], 1, 0)
        plan[b] = dest[b] * CAP + rank
    if blocks > 8:
        lax.fori_loop(0, blocks, count_block, 0)

    def corner():
        return (
            lax.broadcasted_iota(I32, (half, cells), 0), lax.broadcasted_iota(I32, (half, cells), 1)
        )

    def prepare(b):
        row, lane = corner()
        w = weight[b]
        p = scale[pl.ds(b, 1), :]
        normal = jnp.dot((w.astype(F32).T * p).astype(BF16), w, preferred_element_type=F32)
        low = normal[half:cells]
        tri = jnp.where((lane < half) & (lane > row), pltpu.roll(low, half, 1), normal[0:half])
        tri = jnp.where(lane == row, 0.5 * tri, tri)
        block_a[b] = tri
        block_d[pl.ds(b, 1), :] = jnp.sum(jnp.where(lane == row + half, 0.5 * low, 0.0), axis=0, keepdims=True)
        block_b[b] = jnp.dot((values[b].astype(F32) * p).astype(BF16), w, preferred_element_type=F32)

    def pack_slot(s):
        def look(b, found):
            return jnp.where(plan[b] == s, b, found)

        found = lax.fori_loop(0, blocks, look, -1, unroll=blocks <= 8)
        source = jnp.maximum(found, 0)
        fill = jnp.where(found >= 0, 1.0, 0.0)
        t = s // CAP
        k = s % CAP
        pay[t, k, 0:half] = (block_b[source] * fill).astype(BF16)
        pay[t, k, half:chans] = (block_a[source] * fill).astype(BF16)
        pay_p[t, pl.ds(k, 1), :] = block_d[pl.ds(source, 1), :] * fill
        pay_at[t, pl.ds(2 * k, 1), :] = jnp.full((1, obs), row_off[source], I32)
        pay_at[t, pl.ds(2 * k + 1, 1), :] = jnp.full((1, obs), col_off[source], I32)

    loads[0].wait()
    for h in range(2):
        part = xv[:, :, h * width : (h + 1) * width].astype(F32)
        xs[h] = part.reshape(half * rows, width)
    for r in range(rows):
        both[ch, r] = xs[ch, pl.ds(r, half, stride=rows), :].astype(BF16)
        x_send[r] = xs[other, pl.ds(r, half, stride=rows), :].astype(BF16)
    lane = lax.broadcasted_iota(I32, (half, width), 1)
    for n, (h, first) in enumerate(((0, True), (1, False), (1, True), (0, False))):
        tile = None
        for r in range(rows):
            v = pltpu.roll(xs[h, pl.ds(r, half, stride=rows), :], (SIDE * r + (0 if first else SIDE)) % width, 1)
            tile = v if tile is None else jnp.where(lane // SIDE == r, v, tile)
        edge[n] = tile.astype(BF16)
    edge_r[other, ch] = edge[2 + ch]

    tops = (lat + n_lat - 1) // n_lat
    bottoms = (2 * n_lat - 2 - lat) // n_lat
    pl.semaphore_wait(barrier, 4 + 3 * tops + 3 * bottoms)

    def tell(sem, dlat):
        pl.semaphore_signal(sem, inc=1, device_id={"lat": lat + dlat}, device_id_type=MESH)

    @pl.when((lat == 1) & has_down)
    def _():
        tell(heard_up, 1)

    @pl.when((lat == n_lat - 2) & has_up)
    def _():
        tell(heard_down, -1)

    def pair_copy(src, dst, i):
        return pltpu.make_async_remote_copy(
            src_ref=src, dst_ref=dst, send_sem=pair_s.at[i], recv_sem=pair_r.at[i],
            device_id=sibling, device_id_type=MESH,
        )

    reshard = pair_copy(x_send, both.at[ch], 0)
    reshard.start()

    def raw_row(dl, mine):
        row = 0 if dl < 0 else rows - HALO
        src = both.at[ch, pl.ds(row, HALO)] if mine else x_send.at[pl.ds(row, HALO)]
        side = 1 if dl < 0 else 0
        return pltpu.make_async_remote_copy(
            src_ref=src, dst_ref=raw.at[side, ch], send_sem=raw_s.at[2 * side + mine],
            recv_sem=raw_r.at[2 * side + ch],
            device_id={"lat": lat + dl, "ch": ch if mine else other}, device_id_type=MESH,
        )

    def raw_got(dl, c):
        side = 0 if dl < 0 else 1
        return pltpu.make_async_remote_copy(
            src_ref=x_send.at[pl.ds(0, HALO)], dst_ref=raw.at[side, c], send_sem=raw_s.at[2 * side],
            recv_sem=raw_r.at[2 * side + c], device_id={"lat": lat + dl}, device_id_type=MESH,
        )

    def edge_copy(n, src, side, place):
        return pltpu.make_async_remote_copy(
            src_ref=edge.at[src], dst_ref=edge_r.at[side, ch], send_sem=edge_ss.at[n],
            recv_sem=edge_rs.at[2 * side + ch], device_id=place, device_id_type=MESH,
        )

    def edge_got(side, c):
        return pltpu.make_async_remote_copy(
            src_ref=edge.at[0], dst_ref=edge_r.at[side, c], send_sem=edge_ss.at[0],
            recv_sem=edge_rs.at[2 * side + c], device_id=sibling, device_id_type=MESH,
        )

    for dl in (-1, 1):
        @pl.when(has_up if dl < 0 else has_down)
        def _(dl=dl):
            raw_row(dl, 0).start()
            raw_row(dl, 1).start()

    edges = [
        edge_copy(0, 0, 1, {"lon": chip_left, "ch": 1}),
        edge_copy(1, 1, 0, {"lon": chip_right, "ch": 0}),
        edge_copy(2, 3 - ch, ch, sibling),
    ]
    for copy in edges:
        copy.start()
    for load in loads[1:4]:
        load.wait()
    scale[...] = scale_raw[...].astype(F32)
    pay_at[...] = jnp.zeros(pay_at.shape, I32)
    pay_p[...] = jnp.zeros(pay_p.shape, F32)
    each(blocks, prepare)
    each(slots, pack_slot)
    def by_core(fn):
        for c in (0, 1):
            pl.when(ch == c)(functools.partial(fn, c))

    def big(peer, landing, c):
        part = pl.ds(0, half * (1 + c))
        return pltpu.make_async_remote_copy(
            src_ref=pay.at[peer, :, part], dst_ref=R.at[landing, c, :, part],
            send_sem=pay_ss.at[peer], recv_sem=pay_rs.at[landing],
            device_id={"lat": peer}, device_id_type=MESH,
        )

    def small(peer, landing, kind):
        src, dst, ss, rs = ((pay_at, R_at, at_ss, at_rs), (pay_p, R_p, p_ss, p_rs))[kind]
        return pltpu.make_async_remote_copy(
            src_ref=src.at[peer], dst_ref=dst.at[landing], send_sem=ss.at[peer], recv_sem=rs.at[landing],
            device_id={"lat": peer}, device_id_type=MESH,
        )

    def start_small(peer):
        @pl.when(ch == 1)
        def _():
            small(peer, lat, 0).start()
            small(peer, lat, 1).start()

    def start_big(peer):
        by_core(lambda c: big(peer, lat, c).start())

    middle = has_up & has_down

    def send_far():
        last = n_lat - 2
        each(last, lambda j: pl.when(far_off(peer_of(last - j)))(lambda: start_small(peer_of(last - j))))
        each(n_lat - 1, lambda j: start_big(peer_of(last - j)))

    def far_off(peer):
        return (peer > lat + 1) | (peer < lat - 1)

    def send_near_small():
        pl.when(has_up)(lambda: start_small(lat - 1))
        pl.when(has_down)(lambda: start_small(lat + 1))

    def put_row(taps, r, v):
        taps[r * pitch : (r + 1) * pitch, 0:chans] = pltpu.roll(v, 1, 0).astype(BF16)
        taps[r * pitch : (r + 1) * pitch, chans : 2 * chans] = v.astype(BF16)
        taps[r * pitch : (r + 1) * pitch, 2 * chans :] = pltpu.roll(v, pitch - 1, 0).astype(BF16)

    def conv(taps, kind, first, count):
        acc = None
        for a in range(3):
            parts = [taps[(f + a) * pitch : (f + a + count) * pitch, :] for f in first]
            part = jnp.dot(jnp.concatenate(parts, axis=0), kw[kind, a], preferred_element_type=F32)
            acc = part if acc is None else acc + part
        return acc

    def edge_factor(r):
        if r == 0:
            return jnp.where(has_up, 1.0, 0.0)
        if r == rows + 1:
            return jnp.where(has_down, 1.0, 0.0)
        return None

    def guarded(dl, fn):
        if dl == 0:
            fn()
        else:
            pl.when(has_up if dl < 0 else has_down)(fn)

    def span(start, size):
        return pl.ds(start if isinstance(start, int) else pl.multiple_of(start, SIDE), size)

    def remote(buf, place, sr, dr, nr, sc, dc, nc, i):
        return pltpu.make_async_remote_copy(
            src_ref=buf.at[pl.ds(sr, nr), span(sc, nc)], dst_ref=buf.at[pl.ds(dr, nr), span(dc, nc)],
            send_sem=halo_s.at[i], recv_sem=halo_r.at[i], device_id=place, device_id_type=MESH,
        )

    span_r = {-1: (top, rows + top, HALO), 0: (top, top, rows), 1: (top + rows - HALO, 0, HALO)}
    span_c = {-1: (left, left + width, SIDE), 0: (left, left, width), 1: (left + width - SIDE, 0, SIDE)}

    def x_routes():
        i = 0
        routes = {-1: [], 0: [], 1: []}
        for dl, side in [(-1, -1), (-1, 1), (1, -1), (1, 1)]:
            sr, dr, nr = span_r[dl]
            sc, dc, nc = span_c[side]
            routes[dl].append(remote(X, at(dl, side), sr, dr, nr, sc, dc, nc, i))
            i += 1
        return routes

    def g_routes():
        i = 8
        routes = {-1: [], 0: [], 1: []}
        out_src = left + ch * (width - SIDE)
        out_dst = other * (left + width)
        for dl in (0, -1, 1):
            sr, dr, nr = span_r[dl]
            if dl:
                routes[dl].append(remote(G, at(dl, 0), sr, dr, nr, other * SIDE, other * SIDE, reach, i))
                i += 1
            routes[dl].append(remote(G, outward(dl), sr, dr, nr, out_src, out_dst, SIDE, i))
            i += 1
        return routes

    def halo_start(routes, order):
        for dl in order:
            def go(dl=dl):
                for copy in routes[dl]:
                    copy.start()

            guarded(dl, go)

    def halo_finish(routes, order):
        for dl in order:
            def sent(dl=dl):
                for copy in routes[dl]:
                    copy.wait_send()

            def got(dl=dl):
                for copy in routes[dl]:
                    copy.wait_recv()

            guarded(dl, sent)
            guarded(-dl, got)

    def clear_poles(buf):
        @pl.when(lat == 0)
        def _():
            buf[0:HALO] = jnp.zeros((HALO, pitch, chans), BF16)

        @pl.when(lat == n_lat - 1)
        def _():
            buf[rows + HALO : rows + 2 * HALO] = jnp.zeros((HALO, pitch, chans), BF16)

    clear_poles(X)
    clear_poles(G)

    reshard.wait()
    for r in range(rows):
        X[top + r, left : left + width] = (
            jnp.concatenate([both[0, r], both[1, r]], axis=0).astype(F32).T.astype(BF16)
        )
    x_halo = x_routes()
    halo_start(x_halo, (-1, 1))

    send_near_small()

    @pl.when(middle)
    def _():
        @pl.when(lat >= 2)
        def _():
            pl.semaphore_wait(heard_up, 1)
            tell(heard_up, 1)

        @pl.when(lat <= n_lat - 3)
        def _():
            pl.semaphore_wait(heard_down, 1)
            tell(heard_down, -1)

        send_far()

    R[lat, ch] = pay[lat]
    R_at[lat] = pay_at[lat]
    R_p[lat] = pay_p[lat]

    def forward(t, c):
        part = pl.ds(0, half * (1 + c))
        return pltpu.make_async_remote_copy(
            src_ref=R.at[t, c, :, part], dst_ref=R.at[t, c, :, part], send_sem=fwd_s.at[t], recv_sem=fwd_r.at[t],
            device_id=sibling, device_id_type=MESH,
        )

    def forward_small(t, kind):
        ref, ss, rs = ((R_at, fat_s, fat_r), (R_p, fp_s, fp_r))[kind]
        return pltpu.make_async_remote_copy(
            src_ref=ref.at[t], dst_ref=ref.at[t], send_sem=ss.at[t], recv_sem=rs.at[t],
            device_id=sibling, device_id_type=MESH,
        )

    by_core(lambda c: forward(lat, c).start())
    for load in loads[4:]:
        load.wait()
    for kind, k in enumerate((kin, kout, kout, kin)):
        for a in range(3):
            for b in range(3):
                tap = k[a, b].astype(F32).T.astype(BF16) if kind < 2 else k[2 - a, 2 - b]
                kw[kind, a, b * chans : (b + 1) * chans] = tap
    Z[...] = jnp.zeros(Z.shape, F32)

    @pl.when(jnp.logical_not(middle))
    def _():
        @pl.when(lat >= 2)
        def _():
            pl.semaphore_wait(heard_up, 1)

        @pl.when(lat <= n_lat - 3)
        def _():
            pl.semaphore_wait(heard_down, 1)

        send_far()

    def hidden_rows(first, count):
        acc = conv(X3, 0, first, count) + bias[...]
        s = sigmoid(acc)
        steep = s * (1.0 + acc * (1.0 - s))
        h = acc * s
        for i, r in enumerate(f + n for f in first for n in range(count)):
            own = slice(i * pitch, (i + 1) * pitch)
            slope[r * pitch : (r + 1) * pitch, :] = steep[own]
            row = h[own]
            f = edge_factor(r)
            if f is not None:
                row = row * f
            put_row(H3, r, row.astype(BF16).astype(F32))

    for copy in edges:
        copy.wait_send()
    edge_got(other, other).wait_recv()
    for c in (0, 1):
        edge_got(ch, c).wait_recv()
    for side in (0, 1):
        turned = jnp.concatenate([edge_r[side, 0], edge_r[side, 1]], axis=0).astype(F32).T.astype(BF16)
        for r in range(rows):
            X[top + r, side * (left + width) : side * (left + width) + SIDE] = turned[r * SIDE : (r + 1) * SIDE]
    for r in range(top, top + rows):
        put_row(X3, r, X[r].astype(F32))
    for r0 in range(HALO, rows, 2):
        hidden_rows([r0], 2)
    swaps = []

    def denoise_rows(first, count):
        acc = conv(H3, 1, first, count)
        for i, r in enumerate(f + n for f in first for n in range(count)):
            state = X[top + r, left : left + width].astype(F32)
            den = (state + acc[i * pitch + left : i * pitch + left + width]).astype(BF16)
            den_s[r] = den
            wide = den.astype(F32)
            base[r * width : (r + 1) * width, :] = keep_rate * state + blend_rate * wide
            DF[pl.ds(pl.multiple_of(r * cols + ch * width, width), width), :] = wide
        for f in first:
            part = pl.ds(f, count)
            swaps.append((f, count, pair_copy(den_s.at[part], den_r.at[part], 1 + len(swaps))))
            swaps[-1][2].start()

    inner = [([r0], min(WIDE, rows - HALO - r0)) for r0 in range(HALO, rows - HALO, WIDE)]
    outer = [([0, rows - HALO], HALO)]
    for first, count in inner:
        denoise_rows(first, count)
    halo_finish(x_halo, (-1, 1))
    for dl in (-1, 1):
        @pl.when(has_up if dl < 0 else has_down)
        def _(dl=dl):
            for mine in (0, 1):
                raw_row(dl, mine).wait_send()
            for c in (0, 1):
                raw_got(dl, c).wait_recv()
            for i in range(HALO):
                side = 0 if dl < 0 else 1
                X[side * (top + rows) + i, left : left + width] = (
                    jnp.concatenate([raw[side, 0, i], raw[side, 1, i]], axis=0).astype(F32).T.astype(BF16)
                )

    for r in (0, 1, top + rows, top + rows + 1):
        put_row(X3, r, X[r].astype(F32))
    hidden_rows([0, rows], HALO)
    for first, count in outer:
        denoise_rows(first, count)

    def local_copy(t):
        return pltpu.make_async_copy(R_at.at[t], at_s.at[t], copy_sem.at[t])

    def take_at(j):
        peer = peer_of(j)

        @pl.when(ch == 1)
        def _():
            for kind in (0, 1):
                small(peer, peer, kind).wait()
                forward_small(peer, kind).start()

        @pl.when(ch == 0)
        def _():
            forward_small(peer, 0).wait_recv()

        local_copy(peer).start()

    local_copy(lat).start()
    each(n_lat - 1, take_at)

    def take_pay(j):
        peer = peer_of(j)

        def go(c):
            big(peer, peer, c).wait()
            forward(peer, c).start()

        by_core(go)

    def take_from(j0):
        each(n_lat - 1 - j0, lambda j: take_pay(j + j0))

    batches = slots // GROUP
    split = batches == 2
    if split:
        take_pay(0)
        pl.when(middle)(lambda: take_from(1))
    else:
        take_from(0)
    for r0, count, swap in swaps:
        swap.wait()
        for r in range(r0, r0 + count):
            DF[pl.ds(pl.multiple_of(r * cols + other * width, width), width), :] = den_r[r].astype(F32)
    each(n_lat, lambda t: local_copy(t).wait())

    def gather(t):
        lane = lax.broadcasted_iota(I32, (half, chans), 1)
        for k in range(CAP):
            r0 = at_s[t, 2 * k, 0]
            q0 = at_s[t, 2 * k + 1, 0]
            cut = [DF[pl.ds((r0 + a) * cols + q0, PW), :] for a in range(PH)]
            first = jnp.concatenate(cut[: PH // 2], axis=0)
            second = jnp.concatenate(cut[PH // 2 :], axis=0)
            patches[t, k, 0:half] = first.astype(BF16)
            patches[t, k, half:cells] = second.astype(BF16)
            keep_first = jnp.where(ch == 0, first, pltpu.roll(first, half, 1))
            keep_second = jnp.where(ch == 0, pltpu.roll(second, half, 1), second)
            pat_s[t, k] = jnp.where(lane < half, keep_first, keep_second).astype(BF16)

    each(n_lat, gather)

    def patch_copy(peer, landing):
        return pltpu.make_async_remote_copy(
            src_ref=pat_s.at[peer], dst_ref=pat_r.at[landing],
            send_sem=pat_ss.at[peer], recv_sem=pat_rs.at[landing],
            device_id={"lat": peer}, device_id_type=MESH,
        )

    each(n_lat - 1, lambda j: patch_copy(peer_of(j), lat).start())
    pat_r[lat] = pat_s[lat]
    start = ch * (cols - reach)

    def source_of(j):
        return jnp.where(j == 0, lat, peer_of(jnp.maximum(j - 1, 0)))

    def settle(t):
        def go(c):
            forward(t, c).wait_send()
            forward(t, 1 - c).wait_recv()

        by_core(go)

        @pl.when((ch == 0) & (t != lat))
        def _():
            forward_small(t, 1).wait_recv()

        @pl.when((ch == 1) & (t != lat))
        def _():
            for kind in (0, 1):
                forward_small(t, kind).wait_send()

    g_halo = g_routes()

    def observe(g, first, last):
        owners = [source_of(g * sources + i) for i in range(sources)]
        for t in owners:
            settle(t)
        for i in range(GROUP):
            t, k = owners[i // CAP], i % CAP
            row, lane = corner()
            tri = R[t, 1, k, half:chans].astype(F32)
            upper = jnp.where((lane <= row) | (lane >= half), tri, 0.0)
            lower = jnp.where(lane > row + half, pltpu.roll(tri, half, 1), 0.0)
            lower = jnp.where(lane == row + half, R_p[t, k : k + 1, :], lower)
            side = jnp.concatenate([upper, lower], axis=0).astype(BF16)
            normal = side + side.T
            pull = jnp.concatenate([R[t, 0, k, 0:half], R[t, 1, k, 0:half]], axis=0)
            pulled = jnp.dot(normal, patches[t, k], preferred_element_type=F32) - pull.astype(F32).T
            for a in range(PH):
                Z[pl.ds((i * PH + a) * strip + reach, PW), :] = pulled[a * PW : (a + 1) * PW]
        for n, r in enumerate((0, 1, rows - 2, rows - 1, *range(2, rows - 2))):
            total = None
            for i in range(GROUP):
                t, k = owners[i // CAP], i % CAP
                r0 = at_s[t, 2 * k, 0]
                place = jnp.clip(at_s[t, 2 * k + 1, 0] - start, -PW, reach)
                inside = (r >= r0) & (r < r0 + PH)
                begin = jnp.where(inside, (i * PH + r - r0) * strip + reach - place, blank)
                v = Z[pl.ds(begin, reach), :]
                total = v if total is None else total + v
            span_w = pl.ds(pl.multiple_of(r * pitch + other * SIDE, SIDE), reach)
            if not first:
                total = total + GW[span_w, :]
            GW[span_w, :] = total
            if last:
                G[top + r, pl.ds(pl.multiple_of(other * SIDE, SIDE), reach)] = total.astype(BF16)
                if n == 3:
                    halo_start(g_halo, (-1, 1))
        if last:
            halo_start(g_halo, (0,))

    if split:
        observe(0, True, False)
        pl.when(jnp.logical_not(middle))(lambda: take_from(1))
        observe(1, False, True)
    elif batches == 1:
        observe(0, True, True)
    else:
        observe(0, True, False)
        lax.fori_loop(1, batches - 1, lambda g, _: observe(g, False, False) or 0, 0)
        observe(batches - 1, False, True)

    def grad_rows(first, count):
        back = conv(X3, 2, first, count)
        for i, r in enumerate(f + n for f in first for n in range(count)):
            row = back[i * pitch : (i + 1) * pitch] * slope[r * pitch : (r + 1) * pitch, :]
            f = edge_factor(r)
            if f is not None:
                row = row * f
            put_row(H3, r, row.astype(BF16).astype(F32))

    halo_finish(g_halo, (0,))
    for r in range(top, top + rows):
        put_row(X3, r, G[r].astype(F32))
    for r0 in range(HALO, rows, 2):
        grad_rows([r0], 2)
    back_home = []

    def finish_rows(first, count):
        acc = conv(H3, 3, first, count)
        for i, r in enumerate(f + n for f in first for n in range(count)):
            grad = GW[r * pitch + left : r * pitch + left + width, :] + acc[i * pitch + left : i * pitch + left + width]
            res = (base[r * width : (r + 1) * width, :] - guide_rate * grad).T
            out_s[r] = jnp.where(ch == 0, res[half:chans], res[0:half]).astype(BF16)
            out_h[0, pl.ds(r, half, stride=rows), :] = jnp.where(ch == 0, res[0:half], res[half:chans])
        for f in first:
            part = pl.ds(f, count)
            back_home.append((f, count, pair_copy(out_s.at[part], out_r.at[part], 1 + len(swaps) + len(back_home))))
            back_home[-1][2].start()

    for first, count in inner:
        finish_rows(first, count)
    each(n_lat - 1, lambda j: patch_copy(peer_of(j), peer_of(j)).wait())

    def innovate(b):
        slot = plan[b]
        part = pat_r[slot // CAP, slot % CAP].astype(F32)
        patch = jnp.concatenate([part, pltpu.roll(part, half, 1)], axis=0).astype(BF16)
        predicted = jnp.dot(weight[b], patch, preferred_element_type=F32).T
        inn_out[b] = (predicted[0:half] - values[b].astype(F32)).astype(BF16)

    each(blocks, innovate)
    halo_finish(g_halo, (-1, 1))
    for r in (0, 1, top + rows, top + rows + 1):
        put_row(X3, r, G[r].astype(F32))
    grad_rows([0, rows], HALO)
    for first, count in outer:
        finish_rows(first, count)
    mine = pl.ds(pl.multiple_of(ch * width, width), width)
    theirs = pl.ds(pl.multiple_of(other * width, width), width)
    out[:, mine] = out_h[0]

    for r0, count, copy in back_home:
        copy.wait()
        for r in range(r0, r0 + count):
            out_h[1, pl.ds(r, half, stride=rows), :] = out_r[r].astype(F32)
    out[:, theirs] = out_h[1]


def store(out, innovation, out_hbm, innovation_hbm, sem):
    copies = [
        pltpu.make_async_copy(out, out_hbm, sem.at[0]),
        pltpu.make_async_copy(innovation, innovation_hbm, sem.at[1]),
    ]
    for copy in copies:
        copy.start()
    for copy in copies:
        copy.wait()


def body(n_lat, n_lon, noisy_state, kernel_in, bias_in, kernel_out, interp_weight, observed,
         obs_precision, dest_tile, row_offset, col_offset):
    half, rows, cols = noisy_state.shape
    chans = 2 * half
    width = cols // 2
    blocks, obs, cells = interp_weight.shape
    slots = n_lat * CAP
    pitch = width + 2 * SIDE
    reach = width + SIDE
    px = rows * width
    pairs = 1 + 2 * (2 - (HALO + HALO - rows) // WIDE)
    vmem = pl.BlockSpec(memory_space=pltpu.VMEM)
    hbm = pl.BlockSpec(memory_space=pltpu.HBM)
    smem = pl.BlockSpec(memory_space=pltpu.SMEM)
    dma = pltpu.SemaphoreType.DMA
    call = pl.pallas_call(
        functools.partial(kernel, n_lat, n_lon, rows, width, half, blocks),
        out_shape=(
            pltpu.VMEM((half * rows, cols), F32),
            pltpu.VMEM((blocks, half, obs), BF16),
        ),
        in_specs=[smem] * 3 + [hbm] * 3 + [vmem] + [hbm] * 3,
        out_specs=(vmem, vmem),
        scratch_shapes=[
            pltpu.VMEM((half, rows, cols), BF16),
            pltpu.VMEM((2, half * rows, width), F32),
            pltpu.VMEM((rows, half, width), BF16),
            pltpu.VMEM(kernel_in.shape, BF16),
            pltpu.VMEM(kernel_out.shape, BF16),
            pltpu.VMEM(interp_weight.shape, BF16),
            pltpu.VMEM(observed.shape, BF16),
            pltpu.VMEM(obs_precision.shape, BF16),
            pltpu.VMEM(obs_precision.shape, F32),
            pltpu.VMEM((4, 3, 3 * chans, chans), BF16),
            dma((6,)),
            pltpu.VMEM((2, rows, half, width), BF16),
            pltpu.VMEM((4, half, width), BF16),
            pltpu.VMEM((2, 2, half, width), BF16),
            pltpu.VMEM((2, 2, HALO, half, width), BF16),
            dma((3,)), dma((4,)),
            dma((4,)), dma((4,)),
            pltpu.VMEM((rows + 4, pitch, chans), BF16),
            pltpu.VMEM(((rows + 4) * pitch, 3 * chans), BF16),
            pltpu.VMEM(((rows + 2) * pitch, 3 * chans), BF16),
            pltpu.VMEM(((rows + 2) * pitch, chans), F32),
            pltpu.VMEM((px, chans), F32),
            pltpu.VMEM((rows * cols, chans), F32),
            pltpu.VMEM((rows, width, chans), BF16),
            pltpu.VMEM((rows, width, chans), BF16),
            pltpu.VMEM((blocks, half, cells), F32),
            pltpu.VMEM((blocks, half, cells), F32),
            pltpu.VMEM((blocks, cells), F32),
            pltpu.VMEM((n_lat, CAP, chans, cells), BF16),
            pltpu.VMEM((n_lat, SMALL, obs), I32),
            pltpu.VMEM((n_lat, SMALL, obs), F32),
            pltpu.VMEM((n_lat, 2, CAP, chans, cells), BF16),
            pltpu.VMEM((n_lat, SMALL, obs), I32),
            pltpu.VMEM((n_lat, SMALL, obs), F32),
            pltpu.SMEM((n_lat, SMALL, obs), I32),
            pltpu.VMEM((n_lat, CAP, cells, chans), BF16),
            pltpu.VMEM((n_lat, CAP, half, chans), BF16),
            pltpu.VMEM((n_lat, CAP, half, chans), BF16),
            pltpu.VMEM((GROUP * PH * (2 * reach + PW) + reach, chans), F32),
            pltpu.VMEM((rows + 4, pitch, chans), BF16),
            pltpu.VMEM((rows * pitch, chans), F32),
            pltpu.VMEM((2, half * rows, width), F32),
            pltpu.VMEM((rows, half, width), BF16),
            pltpu.VMEM((rows, half, width), BF16),
            pltpu.SMEM((blocks,), I32),
            pltpu.SemaphoreType.REGULAR,
            pltpu.SemaphoreType.REGULAR,
            dma((13,)), dma((13,)),
            dma((pairs,)), dma((pairs,)),
            dma((n_lat,)), dma((n_lat,)),
            dma((n_lat,)), dma((n_lat,)),
            dma((n_lat,)), dma((n_lat,)),
            dma((n_lat,)), dma((n_lat,)),
            dma((n_lat,)), dma((n_lat,)),
            dma((n_lat,)), dma((n_lat,)),
            dma((n_lat,)),
            dma((n_lat,)), dma((n_lat,)),
        ],
        compiler_params=pltpu.CompilerParams(
            collective_id=0, has_side_effects=True, vmem_limit_bytes=(63 if slots <= 2 * GROUP else 48) * 1024 * 1024
        ),
    )
    out, innovation = call(
        dest_tile, row_offset, col_offset, noisy_state, kernel_in, kernel_out,
        bias_in.reshape(1, chans), interp_weight, observed, obs_precision,
    )
    out, innovation = pl.pallas_call(
        store,
        out_shape=(
            jax.ShapeDtypeStruct((half * rows, cols), F32),
            jax.ShapeDtypeStruct((blocks, half, obs), BF16),
        ),
        in_specs=[vmem, vmem],
        out_specs=(hbm, hbm),
        scratch_shapes=[dma((2,))],
    )(*(pltpu.with_memory_space_constraint(a, pltpu.VMEM) for a in (out, innovation)))
    return out.reshape(half, rows, cols), innovation


def solution(mesh):
    return jax.shard_map(
        functools.partial(body, mesh.shape["lat"], mesh.shape["lon"]),
        mesh=mesh,
        in_specs=(
            P(("grp", "ch"), "lat", "lon"),
            P(),
            P(),
            P(),
            P(("grp", "lat", "lon"), None, None),
            P(("grp", "lat", "lon"), "ch", None),
            P(("grp", "lat", "lon"), None),
            P(("grp", "lat", "lon")),
            P(("grp", "lat", "lon")),
            P(("grp", "lat", "lon")),
        ),
        out_specs=(P(("grp", "ch"), "lat", "lon"), P(("grp", "lat", "lon"), "ch", None)),
        check_vma=False,
    )
```

```python
import functools

import jax
import jax.numpy as jnp
from jax import lax
from jax.experimental import pallas as pl
from jax.experimental.pallas import tpu as pltpu
from jax.sharding import PartitionSpec as P

PH = 4
PW = 32
CAP = 2
HALO = 2
SIDE = 16
GROUP = 4
WIDE = 4
SMALL = 8

keep_rate = 0.6
blend_rate = 0.4
guide_rate = 0.3

MESH = pl.DeviceIdType.MESH
F32 = jnp.float32
BF16 = jnp.bfloat16
I32 = jnp.int32


def sigmoid(v):
    return 0.5 + 0.5 * jnp.tanh(0.5 * v)


def each(count, fn):
    if count <= 8:
        for i in range(count):
            fn(i)
    else:
        lax.fori_loop(0, count, lambda i, _: fn(i) or 0, 0)


def kernel(
    n_lat, n_lon, rows, width, half, blocks,
    dest_hbm, row_hbm, col_hbm, x_hbm, kin_hbm, kout_hbm, bias_hbm, weight_hbm, values_hbm, scale_hbm,
    out, inn_out,
    dest, row_off, col_off, bias,
    xv, xs, x_send, kin, kout, weight, values, scale_raw, scale, kw, load_sem,
    both, edge, edge_r, raw, edge_ss, edge_rs, raw_s, raw_r, X, X3, H3, slope, base, DF, den_s, den_r, block_a, block_b, block_d,
    pay, pay_at, pay_p, R, R_p, at_s, patches, pat_s, pat_r, Z, G, GW, out_h, out_s, out_r,
    plan, heard_up, heard_down,
    halo_s, halo_r, pair_s, pair_r, pay_ss, pay_rs, at_ss, at_rs, p_ss, p_rs, fwd_s, fwd_r, fp_s, copy_sem, pat_ss, pat_rs,
):
    lat, lon, ch = lax.axis_index("lat"), lax.axis_index("lon"), lax.axis_index("ch")
    other = 1 - ch
    chans = 2 * half
    obs = weight_hbm.shape[1]
    cells = PH * PW
    cols = 2 * width
    pitch = width + 2 * SIDE
    reach = width + SIDE
    strip = 2 * reach + PW
    blank = GROUP * PH * strip
    slots = n_lat * CAP
    sources = GROUP // CAP
    px = rows * width
    top, left = HALO, SIDE
    lon_right = lax.rem(lon + ch, n_lon)
    lon_left = lax.rem(lon + n_lon - other, n_lon)
    has_up = lat > 0
    has_down = lat < n_lat - 1
    sibling = {"ch": other}

    def at(dlat, side):
        place = {"lat": lat + dlat}
        if side:
            place["lon"] = lon_right if side > 0 else lon_left
            place["ch"] = other
        return place

    def outward(dlat):
        return {"lat": lat + dlat, "lon": jnp.where(ch == 0, lon_left, lon_right), "ch": other}

    def peer_of(j):
        m = jnp.minimum(lat, n_lat - 1 - lat)
        step = jnp.where(j < 2 * m, j // 2 + 1, j - m + 1)
        below = jnp.where(j < 2 * m, j % 2 == 0, lat > n_lat - 1 - lat)
        return jnp.where(below, lat - step, lat + step)

    loads = [
        pltpu.make_async_copy(src, dst, load_sem.at[i])
        for i, (src, dst) in enumerate(
            [(x_hbm, xv), (dest_hbm, dest), (row_hbm, row_off), (col_hbm, col_off),
             (weight_hbm, weight), (values_hbm, values), (scale_hbm, scale_raw),
             (kin_hbm, kin), (kout_hbm, kout), (bias_hbm, bias)]
        )
    ]
    for load in loads:
        load.start()
    barrier = pltpu.get_barrier_semaphore()

    def greet(place):
        pl.semaphore_signal(barrier, inc=1, device_id=place, device_id_type=MESH)

    greet(at(0, -1))
    greet(at(0, 1))
    chip_left = lax.rem(lon + n_lon - 1, n_lon)
    chip_right = lax.rem(lon + 1, n_lon)
    greet({"lon": chip_left})
    greet({"lon": chip_right})

    @pl.when(has_up)
    def _():
        for side in (-1, 0, 1):
            greet(at(-1, side))

    @pl.when(has_down)
    def _():
        for side in (-1, 0, 1):
            greet(at(1, side))

    def corner():
        return (
            lax.broadcasted_iota(I32, (half, cells), 0), lax.broadcasted_iota(I32, (half, cells), 1)
        )

    def prepare(b):
        row, lane = corner()
        w = weight[b]
        p = scale[pl.ds(b, 1), :]
        normal = jnp.dot((w.astype(F32).T * p).astype(BF16), w, preferred_element_type=F32)
        low = normal[half:cells]
        tri = jnp.where((lane < half) & (lane > row), pltpu.roll(low, half, 1), normal[0:half])
        tri = jnp.where(lane == row, 0.5 * tri, tri)
        block_a[b] = tri
        block_d[pl.ds(b, 1), :] = jnp.sum(jnp.where(lane == row + half, 0.5 * low, 0.0), axis=0, keepdims=True)
        block_b[b] = jnp.dot((values[b].astype(F32) * p).astype(BF16), w, preferred_element_type=F32)

    def pack_slot(s):
        def look(b, found):
            return jnp.where(plan[b] == s, b, found)

        found = lax.fori_loop(0, blocks, look, -1, unroll=blocks <= 8)
        source = jnp.maximum(found, 0)
        fill = jnp.where(found >= 0, 1.0, 0.0)
        t = s // CAP
        k = s % CAP
        pay[t, k, 0:half] = (block_b[source] * fill).astype(BF16)
        pay[t, k, half:chans] = (block_a[source] * fill).astype(BF16)
        pay_p[t, pl.ds(k, 1), :] = block_d[pl.ds(source, 1), :] * fill
        pay_at[t, pl.ds(2 * k, 1), :] = jnp.full((1, obs), row_off[source], I32)
        pay_at[t, pl.ds(2 * k + 1, 1), :] = jnp.full((1, obs), col_off[source], I32)

    loads[0].wait()
    for h in range(2):
        part = xv[:, :, h * width : (h + 1) * width].astype(F32)
        xs[h] = part.reshape(half * rows, width)
    for r in range(rows):
        both[ch, r] = xs[ch, pl.ds(r, half, stride=rows), :].astype(BF16)
        x_send[r] = xs[other, pl.ds(r, half, stride=rows), :].astype(BF16)
    lane = lax.broadcasted_iota(I32, (half, width), 1)
    for n, (h, first) in enumerate(((0, True), (1, False), (1, True), (0, False))):
        tile = None
        for r in range(rows):
            v = pltpu.roll(xs[h, pl.ds(r, half, stride=rows), :], (SIDE * r + (0 if first else SIDE)) % width, 1)
            tile = v if tile is None else jnp.where(lane // SIDE == r, v, tile)
        edge[n] = tile.astype(BF16)
    edge_r[other, ch] = edge[2 + ch]

    tops = (lat + n_lat - 1) // n_lat
    bottoms = (2 * n_lat - 2 - lat) // n_lat
    pl.semaphore_wait(barrier, 4 + 3 * tops + 3 * bottoms)

    def tell(sem, dlat):
        pl.semaphore_signal(sem, inc=1, device_id={"lat": lat + dlat}, device_id_type=MESH)

    @pl.when((lat == 1) & has_down)
    def _():
        tell(heard_up, 1)

    @pl.when((lat == n_lat - 2) & has_up)
    def _():
        tell(heard_down, -1)

    def pair_copy(src, dst, i):
        return pltpu.make_async_remote_copy(
            src_ref=src, dst_ref=dst, send_sem=pair_s.at[i], recv_sem=pair_r.at[i],
            device_id=sibling, device_id_type=MESH,
        )

    reshard = pair_copy(x_send, both.at[ch], 0)
    reshard.start()

    def raw_row(dl, mine):
        row = 0 if dl < 0 else rows - HALO
        src = both.at[ch, pl.ds(row, HALO)] if mine else x_send.at[pl.ds(row, HALO)]
        side = 1 if dl < 0 else 0
        return pltpu.make_async_remote_copy(
            src_ref=src, dst_ref=raw.at[side, ch], send_sem=raw_s.at[side],
            recv_sem=raw_r.at[2 * side + ch],
            device_id={"lat": lat + dl, "ch": ch if mine else other}, device_id_type=MESH,
        )

    def raw_got(dl, c):
        side = 0 if dl < 0 else 1
        return pltpu.make_async_remote_copy(
            src_ref=x_send.at[pl.ds(0, HALO)], dst_ref=raw.at[side, c], send_sem=raw_s.at[side],
            recv_sem=raw_r.at[2 * side + c], device_id={"lat": lat + dl}, device_id_type=MESH,
        )

    def edge_copy(n, src, side, place):
        return pltpu.make_async_remote_copy(
            src_ref=edge.at[src], dst_ref=edge_r.at[side, ch], send_sem=edge_ss,
            recv_sem=edge_rs.at[2 * side + ch], device_id=place, device_id_type=MESH,
        )

    def edge_got(side, c):
        return pltpu.make_async_remote_copy(
            src_ref=edge.at[0], dst_ref=edge_r.at[side, c], send_sem=edge_ss,
            recv_sem=edge_rs.at[2 * side + c], device_id=sibling, device_id_type=MESH,
        )

    for dl in (-1, 1):
        @pl.when(has_up if dl < 0 else has_down)
        def _(dl=dl):
            raw_row(dl, 0).start()
            raw_row(dl, 1).start()

    edges = [
        edge_copy(0, 0, 1, {"lon": chip_left, "ch": 1}),
        edge_copy(1, 1, 0, {"lon": chip_right, "ch": 0}),
        edge_copy(2, 3 - ch, ch, sibling),
    ]
    for copy in edges:
        copy.start()
    for load in loads[1:7]:
        load.wait()
    def count_block(b, _):
        def earlier(e, rank):
            return rank + jnp.where(dest[e] == dest[b], 1, 0)

        plan[b] = dest[b] * CAP + lax.fori_loop(0, b, earlier, 0)
        return 0

    for b in range(blocks) if blocks <= 8 else ():
        rank = 0
        for e in range(b):
            rank = rank + jnp.where(dest[e] == dest[b], 1, 0)
        plan[b] = dest[b] * CAP + rank
    if blocks > 8:
        lax.fori_loop(0, blocks, count_block, 0)

    scale[...] = scale_raw[...].astype(F32)
    pay_at[...] = jnp.zeros(pay_at.shape, I32)
    pay_p[...] = jnp.zeros(pay_p.shape, F32)
    each(blocks, prepare)
    each(slots, pack_slot)
    def by_core(fn):
        for c in (0, 1):
            pl.when(ch == c)(functools.partial(fn, c))

    def big(peer, landing, c):
        part = pl.ds(0, half * (1 + c))
        return pltpu.make_async_remote_copy(
            src_ref=pay.at[peer, :, part], dst_ref=R.at[landing, c, :, part],
            send_sem=pay_ss, recv_sem=pay_rs.at[landing],
            device_id={"lat": peer}, device_id_type=MESH,
        )

    def small(peer, landing, kind):
        src, dst, ss, rs = ((pay_at, at_s, at_ss, at_rs), (pay_p, R_p, p_ss, p_rs))[kind]
        return pltpu.make_async_remote_copy(
            src_ref=src.at[peer], dst_ref=dst.at[landing], send_sem=ss, recv_sem=rs.at[landing],
            device_id={"lat": peer}, device_id_type=MESH,
        )

    def start_small(peer):
        small(peer, lat, 0).start()

        @pl.when(ch == 1)
        def _():
            small(peer, lat, 1).start()

    def start_big(peer):
        by_core(lambda c: big(peer, lat, c).start())

    middle = has_up & has_down

    def upward(j):
        return j + jnp.where(lat <= j, 1, 0)

    def send_far():
        each(n_lat - 1, lambda j: pl.when(far_off(upward(j)))(lambda: start_small(upward(j))))
        each(n_lat - 1, lambda j: start_big(upward(j)))

    def far_off(peer):
        return (peer > lat + 1) | (peer < lat - 1)

    def send_near_small():
        pl.when(has_up)(lambda: start_small(lat - 1))
        pl.when(has_down)(lambda: start_small(lat + 1))

    def put_row(taps, r, v):
        taps[r * pitch : (r + 1) * pitch, 0:chans] = pltpu.roll(v, 1, 0).astype(BF16)
        taps[r * pitch : (r + 1) * pitch, chans : 2 * chans] = v.astype(BF16)
        taps[r * pitch : (r + 1) * pitch, 2 * chans :] = pltpu.roll(v, pitch - 1, 0).astype(BF16)

    def conv(taps, kind, first, count):
        acc = None
        for a in range(3):
            parts = [taps[(f + a) * pitch : (f + a + count) * pitch, :] for f in first]
            part = jnp.dot(jnp.concatenate(parts, axis=0), kw[kind, a], preferred_element_type=F32)
            acc = part if acc is None else acc + part
        return acc

    def edge_factor(r):
        if r == 0:
            return jnp.where(has_up, 1.0, 0.0)
        if r == rows + 1:
            return jnp.where(has_down, 1.0, 0.0)
        return None

    def guarded(dl, fn):
        if dl == 0:
            fn()
        else:
            pl.when(has_up if dl < 0 else has_down)(fn)

    def span(start, size):
        return pl.ds(start if isinstance(start, int) else pl.multiple_of(start, SIDE), size)

    def remote(buf, place, sr, dr, nr, sc, dc, nc, i):
        return pltpu.make_async_remote_copy(
            src_ref=buf.at[pl.ds(sr, nr), span(sc, nc)], dst_ref=buf.at[pl.ds(dr, nr), span(dc, nc)],
            send_sem=halo_s.at[i], recv_sem=halo_r.at[i], device_id=place, device_id_type=MESH,
        )

    span_r = {-1: (top, rows + top, HALO), 0: (top, top, rows), 1: (top + rows - HALO, 0, HALO)}
    span_c = {-1: (left, left + width, SIDE), 0: (left, left, width), 1: (left + width - SIDE, 0, SIDE)}

    def x_routes():
        i = 0
        routes = {-1: [], 0: [], 1: []}
        for dl, side in [(-1, -1), (-1, 1), (1, -1), (1, 1)]:
            sr, dr, nr = span_r[dl]
            sc, dc, nc = span_c[side]
            routes[dl].append(remote(X, at(dl, side), sr, dr, nr, sc, dc, nc, i))
            i += 1
        return routes

    def g_routes():
        i = 4
        routes = {-1: [], 0: [], 1: []}
        out_src = left + ch * (width - SIDE)
        out_dst = other * (left + width)
        for dl in (0, -1, 1):
            sr, dr, nr = span_r[dl]
            if dl:
                routes[dl].append(remote(G, at(dl, 0), sr, dr, nr, other * SIDE, other * SIDE, reach, i))
                i += 1
            routes[dl].append(remote(G, outward(dl), sr, dr, nr, out_src, out_dst, SIDE, i))
            i += 1
        return routes

    def halo_start(routes, order):
        for dl in order:
            def go(dl=dl):
                for copy in routes[dl]:
                    copy.start()

            guarded(dl, go)

    def halo_finish(routes, order):
        for dl in order:
            def sent(dl=dl):
                for copy in routes[dl]:
                    copy.wait_send()

            def got(dl=dl):
                for copy in routes[dl]:
                    copy.wait_recv()

            guarded(dl, sent)
            guarded(-dl, got)

    def clear_poles(buf):
        @pl.when(lat == 0)
        def _():
            buf[0:HALO] = jnp.zeros((HALO, pitch, chans), BF16)

        @pl.when(lat == n_lat - 1)
        def _():
            buf[rows + HALO : rows + 2 * HALO] = jnp.zeros((HALO, pitch, chans), BF16)

    clear_poles(X)
    clear_poles(G)

    reshard.wait()
    for r in range(rows):
        X[top + r, left : left + width] = (
            jnp.concatenate([both[0, r], both[1, r]], axis=0).astype(F32).T.astype(BF16)
        )
    x_halo = x_routes()
    halo_start(x_halo, (-1, 1))

    send_near_small()

    @pl.when(middle)
    def _():
        @pl.when(lat >= 2)
        def _():
            pl.semaphore_wait(heard_up, 1)
            tell(heard_up, 1)

        @pl.when(lat <= n_lat - 3)
        def _():
            pl.semaphore_wait(heard_down, 1)
            tell(heard_down, -1)

        send_far()

    R[lat, ch] = pay[lat]
    own_at = pltpu.make_async_copy(pay_at.at[lat], at_s.at[lat], copy_sem)
    own_at.start()
    R_p[lat] = pay_p[lat]

    def forward(t, c):
        part = pl.ds(0, half * (1 + c))
        return pltpu.make_async_remote_copy(
            src_ref=R.at[t, c, :, part], dst_ref=R.at[t, c, :, part], send_sem=fwd_s, recv_sem=fwd_r.at[t],
            device_id=sibling, device_id_type=MESH,
        )

    def forward_small(t):
        return pltpu.make_async_remote_copy(
            src_ref=R_p.at[t], dst_ref=R_p.at[t], send_sem=fp_s, recv_sem=p_rs.at[t],
            device_id=sibling, device_id_type=MESH,
        )

    by_core(lambda c: forward(lat, c).start())
    for load in loads[7:]:
        load.wait()
    for kind, k in enumerate((kin, kout, kout, kin)):
        for a in range(3):
            for b in range(3):
                tap = k[a, b].astype(F32).T.astype(BF16) if kind < 2 else k[2 - a, 2 - b]
                kw[kind, a, b * chans : (b + 1) * chans] = tap
    Z[...] = jnp.zeros(Z.shape, F32)

    @pl.when(jnp.logical_not(middle))
    def _():
        @pl.when(lat >= 2)
        def _():
            pl.semaphore_wait(heard_up, 1)

        @pl.when(lat <= n_lat - 3)
        def _():
            pl.semaphore_wait(heard_down, 1)

        send_far()

    def hidden_rows(first, count):
        acc = conv(X3, 0, first, count) + bias[...]
        s = sigmoid(acc)
        steep = s * (1.0 + acc * (1.0 - s))
        h = acc * s
        for i, r in enumerate(f + n for f in first for n in range(count)):
            own = slice(i * pitch, (i + 1) * pitch)
            slope[r * pitch : (r + 1) * pitch, :] = steep[own]
            row = h[own]
            f = edge_factor(r)
            if f is not None:
                row = row * f
            put_row(H3, r, row.astype(BF16).astype(F32))

    pltpu.make_async_remote_copy(
        src_ref=edge.at[0:3], dst_ref=edge.at[0:3], send_sem=edge_ss, recv_sem=edge_rs.at[0],
        device_id=sibling, device_id_type=MESH,
    ).wait_send()
    edge_got(other, other).wait_recv()
    for c in (0, 1):
        edge_got(ch, c).wait_recv()
    for side in (0, 1):
        turned = jnp.concatenate([edge_r[side, 0], edge_r[side, 1]], axis=0).astype(F32).T.astype(BF16)
        for r in range(rows):
            X[top + r, side * (left + width) : side * (left + width) + SIDE] = turned[r * SIDE : (r + 1) * SIDE]
    for r in range(top, top + rows):
        put_row(X3, r, X[r].astype(F32))
    for r0 in range(HALO, rows, 2):
        hidden_rows([r0], 2)
    swaps = []

    def denoise_rows(first, count):
        acc = conv(H3, 1, first, count)
        for i, r in enumerate(f + n for f in first for n in range(count)):
            state = X[top + r, left : left + width].astype(F32)
            den = (state + acc[i * pitch + left : i * pitch + left + width]).astype(BF16)
            den_s[r] = den
            wide = den.astype(F32)
            base[r * width : (r + 1) * width, :] = keep_rate * state + blend_rate * wide
            DF[pl.ds(pl.multiple_of(r * cols + ch * width, width), width), :] = wide
        for f in first:
            part = pl.ds(f, count)
            swaps.append((f, count, pair_copy(den_s.at[part], den_r.at[part], 1 + len(swaps))))
            swaps[-1][2].start()

    inner = [([r0], min(WIDE, rows - HALO - r0)) for r0 in range(HALO, rows - HALO, WIDE)]
    outer = [([0, rows - HALO], HALO)]
    for first, count in inner:
        denoise_rows(first, count)
    halo_finish(x_halo, (-1, 1))
    for dl in (-1, 1):
        @pl.when(has_up if dl < 0 else has_down)
        def _(dl=dl):
            pltpu.make_async_remote_copy(
                src_ref=x_send.at[pl.ds(0, 2 * HALO)], dst_ref=x_send.at[pl.ds(0, 2 * HALO)],
                send_sem=raw_s.at[1 if dl < 0 else 0], recv_sem=raw_r.at[0],
                device_id=sibling, device_id_type=MESH,
            ).wait_send()
            for c in (0, 1):
                raw_got(dl, c).wait_recv()
            for i in range(HALO):
                side = 0 if dl < 0 else 1
                X[side * (top + rows) + i, left : left + width] = (
                    jnp.concatenate([raw[side, 0, i], raw[side, 1, i]], axis=0).astype(F32).T.astype(BF16)
                )

    for r in (0, 1, top + rows, top + rows + 1):
        put_row(X3, r, X[r].astype(F32))
    hidden_rows([0, rows], HALO)
    for first, count in outer:
        denoise_rows(first, count)

    own_at.wait()
    each(n_lat - 1, lambda j: small(peer_of(j), peer_of(j), 0).wait_recv())

    def take_pay(j):
        peer = peer_of(j)

        def go(c):
            big(peer, peer, c).wait_recv()
            forward(peer, c).start()
            if c == 1:
                small(peer, peer, 1).wait_recv()
                forward_small(peer).start()

        by_core(go)

    def take_from(j0):
        each(n_lat - 1 - j0, lambda j: take_pay(j + j0))

    batches = slots // GROUP
    split = batches == 2
    if split:
        pl.when(jnp.logical_not(middle))(lambda: take_pay(0))
    for r0, count, swap in swaps:
        swap.wait()
        for r in range(r0, r0 + count):
            DF[pl.ds(pl.multiple_of(r * cols + other * width, width), width), :] = den_r[r].astype(F32)

    def gather(t):
        lane = lax.broadcasted_iota(I32, (half, chans), 1)
        for k in range(CAP):
            r0 = at_s[t, 2 * k, 0]
            q0 = at_s[t, 2 * k + 1, 0]
            cut = [DF[pl.ds((r0 + a) * cols + q0, PW), :] for a in range(PH)]
            first = jnp.concatenate(cut[: PH // 2], axis=0)
            second = jnp.concatenate(cut[PH // 2 :], axis=0)
            patches[t, k, 0:half] = first.astype(BF16)
            patches[t, k, half:cells] = second.astype(BF16)
            keep_first = jnp.where(ch == 0, first, pltpu.roll(first, half, 1))
            keep_second = jnp.where(ch == 0, pltpu.roll(second, half, 1), second)
            pat_s[t, k] = jnp.where(lane < half, keep_first, keep_second).astype(BF16)

    each(n_lat, gather)

    def patch_copy(peer, landing):
        return pltpu.make_async_remote_copy(
            src_ref=pat_s.at[peer], dst_ref=pat_r.at[landing],
            send_sem=pat_ss, recv_sem=pat_rs.at[landing],
            device_id={"lat": peer}, device_id_type=MESH,
        )

    each(n_lat - 1, lambda j: patch_copy(peer_of(j), lat).start())
    pat_r[lat] = pat_s[lat]
    start = ch * (cols - reach)

    def source_of(j):
        return jnp.where(j == 0, lat, peer_of(jnp.maximum(j - 1, 0)))

    def settle(t):
        by_core(lambda c: forward(t, 1 - c).wait_recv())

        @pl.when((ch == 0) & (t != lat))
        def _():
            forward_small(t).wait_recv()

    def drain(src, dst, sem):
        pltpu.make_async_remote_copy(
            src_ref=src, dst_ref=dst, send_sem=sem, recv_sem=pay_rs.at[0],
            device_id=sibling, device_id_type=MESH,
        ).wait_send()

    def drain_all():
        others = pl.ds(0, n_lat - 1)

        def go(c):
            part = pl.ds(0, half * (1 + c))
            drain(pay.at[others, :, part], R.at[others, c, :, part], pay_ss)
            drain(R.at[:, c, :, part], R.at[:, c, :, part], fwd_s)
            if c == 1:
                drain(pay_p.at[others], R_p.at[others], p_ss)
                drain(R_p.at[others], R_p.at[others], fp_s)

        by_core(go)
        drain(pay_at.at[others], at_s.at[others], at_ss)
        drain(pat_s.at[others], pat_r.at[others], pat_ss)

    g_halo = g_routes()

    def observe(g, first, last):
        owners = [source_of(g * sources + i) for i in range(sources)]
        for t in owners:
            settle(t)
        for i in range(GROUP):
            t, k = owners[i // CAP], i % CAP
            row, lane = corner()
            tri = R[t, 1, k, half:chans].astype(F32)
            upper = jnp.where((lane <= row) | (lane >= half), tri, 0.0)
            lower = jnp.where(lane > row + half, pltpu.roll(tri, half, 1), 0.0)
            lower = jnp.where(lane == row + half, R_p[t, k : k + 1, :], lower)
            side = jnp.concatenate([upper, lower], axis=0).astype(BF16)
            normal = side + side.T
            pull = jnp.concatenate([R[t, 0, k, 0:half], R[t, 1, k, 0:half]], axis=0)
            pulled = jnp.dot(normal, patches[t, k], preferred_element_type=F32) - pull.astype(F32).T
            for a in range(PH):
                Z[pl.ds((i * PH + a) * strip + reach, PW), :] = pulled[a * PW : (a + 1) * PW]
        for n, r in enumerate((0, 1, rows - 2, rows - 1, *range(2, rows - 2))):
            total = None
            for i in range(GROUP):
                t, k = owners[i // CAP], i % CAP
                r0 = at_s[t, 2 * k, 0]
                place = jnp.clip(at_s[t, 2 * k + 1, 0] - start, -PW, reach)
                inside = (r >= r0) & (r < r0 + PH)
                begin = jnp.where(inside, (i * PH + r - r0) * strip + reach - place, blank)
                v = Z[pl.ds(begin, reach), :]
                total = v if total is None else total + v
            span_w = pl.ds(pl.multiple_of(r * pitch + other * SIDE, SIDE), reach)
            if not first:
                total = total + GW[span_w, :]
            GW[span_w, :] = total
            if last:
                G[top + r, pl.ds(pl.multiple_of(other * SIDE, SIDE), reach)] = total.astype(BF16)
                if n == 3:
                    halo_start(g_halo, (-1, 1))
        if last:
            halo_start(g_halo, (0,))

    if split:
        pl.when(middle)(lambda: take_from(0))
    else:
        take_from(0)
    if split:
        observe(0, True, False)
        pl.when(jnp.logical_not(middle))(lambda: take_from(1))
        observe(1, False, True)
    elif batches == 1:
        observe(0, True, True)
    else:
        observe(0, True, False)
        lax.fori_loop(1, batches - 1, lambda g, _: observe(g, False, False) or 0, 0)
        observe(batches - 1, False, True)

    def grad_rows(first, count):
        back = conv(X3, 2, first, count)
        for i, r in enumerate(f + n for f in first for n in range(count)):
            row = back[i * pitch : (i + 1) * pitch] * slope[r * pitch : (r + 1) * pitch, :]
            f = edge_factor(r)
            if f is not None:
                row = row * f
            put_row(H3, r, row.astype(BF16).astype(F32))

    halo_finish(g_halo, (0,))
    for r in range(top, top + rows):
        put_row(X3, r, G[r].astype(F32))
    for r0 in range(HALO, rows, 2):
        grad_rows([r0], 2)
    back_home = []

    def finish_rows(first, count):
        acc = conv(H3, 3, first, count)
        for i, r in enumerate(f + n for f in first for n in range(count)):
            grad = GW[r * pitch + left : r * pitch + left + width, :] + acc[i * pitch + left : i * pitch + left + width]
            res = (base[r * width : (r + 1) * width, :] - guide_rate * grad).T
            out_s[r] = jnp.where(ch == 0, res[half:chans], res[0:half]).astype(BF16)
            out_h[0, pl.ds(r, half, stride=rows), :] = jnp.where(ch == 0, res[0:half], res[half:chans])
        for f in first:
            part = pl.ds(f, count)
            back_home.append((f, count, pair_copy(out_s.at[part], out_r.at[part], 1 + len(swaps) + len(back_home))))
            back_home[-1][2].start()

    for first, count in inner:
        finish_rows(first, count)
    each(n_lat - 1, lambda j: patch_copy(peer_of(j), peer_of(j)).wait_recv())
    drain_all()

    def innovate(b):
        slot = plan[b]
        part = pat_r[slot // CAP, slot % CAP].astype(F32)
        patch = jnp.concatenate([part, pltpu.roll(part, half, 1)], axis=0).astype(BF16)
        predicted = jnp.dot(weight[b], patch, preferred_element_type=F32).T
        inn_out[b] = (predicted[0:half] - values[b].astype(F32)).astype(BF16)

    each(blocks, innovate)
    halo_finish(g_halo, (-1, 1))
    for r in (0, 1, top + rows, top + rows + 1):
        put_row(X3, r, G[r].astype(F32))
    grad_rows([0, rows], HALO)
    for first, count in outer:
        finish_rows(first, count)
    mine = pl.ds(pl.multiple_of(ch * width, width), width)
    theirs = pl.ds(pl.multiple_of(other * width, width), width)
    out[:, mine] = out_h[0]

    for r0, count, copy in back_home:
        copy.wait()
        for r in range(r0, r0 + count):
            out_h[1, pl.ds(r, half, stride=rows), :] = out_r[r].astype(F32)
    out[:, theirs] = out_h[1]


def store(out, innovation, out_hbm, innovation_hbm, sem):
    copies = [
        pltpu.make_async_copy(out, out_hbm, sem.at[0]),
        pltpu.make_async_copy(innovation, innovation_hbm, sem.at[1]),
    ]
    for copy in copies:
        copy.start()
    for copy in copies:
        copy.wait()


def body(n_lat, n_lon, noisy_state, kernel_in, bias_in, kernel_out, interp_weight, observed,
         obs_precision, dest_tile, row_offset, col_offset):
    half, rows, cols = noisy_state.shape
    chans = 2 * half
    width = cols // 2
    blocks, obs, cells = interp_weight.shape
    slots = n_lat * CAP
    pitch = width + 2 * SIDE
    reach = width + SIDE
    px = rows * width
    pairs = 1 + 2 * (2 - (HALO + HALO - rows) // WIDE)
    vmem = pl.BlockSpec(memory_space=pltpu.VMEM)
    hbm = pl.BlockSpec(memory_space=pltpu.HBM)
    dma = pltpu.SemaphoreType.DMA
    call = pl.pallas_call(
        functools.partial(kernel, n_lat, n_lon, rows, width, half, blocks),
        out_shape=(
            pltpu.VMEM((half * rows, cols), F32),
            pltpu.VMEM((blocks, half, obs), BF16),
        ),
        in_specs=[hbm] * 10,
        out_specs=(vmem, vmem),
        scratch_shapes=[
            pltpu.SMEM((blocks,), I32),
            pltpu.SMEM((blocks,), I32),
            pltpu.SMEM((blocks,), I32),
            pltpu.VMEM((1, chans), F32),
            pltpu.VMEM((half, rows, cols), BF16),
            pltpu.VMEM((2, half * rows, width), F32),
            pltpu.VMEM((rows, half, width), BF16),
            pltpu.VMEM(kernel_in.shape, BF16),
            pltpu.VMEM(kernel_out.shape, BF16),
            pltpu.VMEM(interp_weight.shape, BF16),
            pltpu.VMEM(observed.shape, BF16),
            pltpu.VMEM(obs_precision.shape, BF16),
            pltpu.VMEM(obs_precision.shape, F32),
            pltpu.VMEM((4, 3, 3 * chans, chans), BF16),
            dma((10,)),
            pltpu.VMEM((2, rows, half, width), BF16),
            pltpu.VMEM((4, half, width), BF16),
            pltpu.VMEM((2, 2, half, width), BF16),
            pltpu.VMEM((2, 2, HALO, half, width), BF16),
            dma, dma((4,)),
            dma((2,)), dma((4,)),
            pltpu.VMEM((rows + 4, pitch, chans), BF16),
            pltpu.VMEM(((rows + 4) * pitch, 3 * chans), BF16),
            pltpu.VMEM(((rows + 2) * pitch, 3 * chans), BF16),
            pltpu.VMEM(((rows + 2) * pitch, chans), F32),
            pltpu.VMEM((px, chans), F32),
            pltpu.VMEM((rows * cols, chans), F32),
            pltpu.VMEM((rows, width, chans), BF16),
            pltpu.VMEM((rows, width, chans), BF16),
            pltpu.VMEM((blocks, half, cells), F32),
            pltpu.VMEM((blocks, half, cells), F32),
            pltpu.VMEM((blocks, cells), F32),
            pltpu.VMEM((n_lat, CAP, chans, cells), BF16),
            pltpu.VMEM((n_lat, SMALL, obs), I32),
            pltpu.VMEM((n_lat, SMALL, obs), F32),
            pltpu.VMEM((n_lat, 2, CAP, chans, cells), BF16),
            pltpu.VMEM((n_lat, SMALL, obs), F32),
            pltpu.SMEM((n_lat, SMALL, obs), I32),
            pltpu.VMEM((n_lat, CAP, cells, chans), BF16),
            pltpu.VMEM((n_lat, CAP, half, chans), BF16),
            pltpu.VMEM((n_lat, CAP, half, chans), BF16),
            pltpu.VMEM((GROUP * PH * (2 * reach + PW) + reach, chans), F32),
            pltpu.VMEM((rows + 4, pitch, chans), BF16),
            pltpu.VMEM((rows * pitch, chans), F32),
            pltpu.VMEM((2, half * rows, width), F32),
            pltpu.VMEM((rows, half, width), BF16),
            pltpu.VMEM((rows, half, width), BF16),
            pltpu.SMEM((blocks,), I32),
            pltpu.SemaphoreType.REGULAR,
            pltpu.SemaphoreType.REGULAR,
            dma((9,)), dma((9,)),
            dma((pairs,)), dma((pairs,)),
            dma, dma((n_lat,)),
            dma, dma((n_lat,)),
            dma, dma((n_lat,)),
            dma, dma((n_lat,)),
            dma,
            dma,
            dma, dma((n_lat,)),
        ],
        compiler_params=pltpu.CompilerParams(
            collective_id=0, has_side_effects=True, vmem_limit_bytes=(63 if slots <= 2 * GROUP else 48) * 1024 * 1024
        ),
    )
    out, innovation = call(
        dest_tile, row_offset, col_offset, noisy_state, kernel_in, kernel_out,
        bias_in.reshape(1, chans), interp_weight, observed, obs_precision,
    )
    out, innovation = pl.pallas_call(
        store,
        out_shape=(
            jax.ShapeDtypeStruct((half * rows, cols), F32),
            jax.ShapeDtypeStruct((blocks, half, obs), BF16),
        ),
        in_specs=[vmem, vmem],
        out_specs=(hbm, hbm),
        scratch_shapes=[dma((2,))],
    )(*(pltpu.with_memory_space_constraint(a, pltpu.VMEM) for a in (out, innovation)))
    return out.reshape(half, rows, cols), innovation


def solution(mesh):
    return jax.shard_map(
        functools.partial(body, mesh.shape["lat"], mesh.shape["lon"]),
        mesh=mesh,
        in_specs=(
            P(("grp", "ch"), "lat", "lon"),
            P(),
            P(),
            P(),
            P(("grp", "lat", "lon"), None, None),
            P(("grp", "lat", "lon"), "ch", None),
            P(("grp", "lat", "lon"), None),
            P(("grp", "lat", "lon")),
            P(("grp", "lat", "lon")),
            P(("grp", "lat", "lon")),
        ),
        out_specs=(P(("grp", "ch"), "lat", "lon"), P(("grp", "lat", "lon"), "ch", None)),
        check_vma=False,
    )
```

```python
import functools

import jax
import jax.numpy as jnp
from jax import lax
from jax.experimental import pallas as pl
from jax.experimental.pallas import tpu as pltpu
from jax.sharding import PartitionSpec as P

PH = 4
PW = 32
CAP = 2
HALO = 2
SIDE = 16
GROUP = 4
WIDE = 4
SMALL = 8

keep_rate = 0.6
blend_rate = 0.4
guide_rate = 0.3

MESH = pl.DeviceIdType.MESH
F32 = jnp.float32
BF16 = jnp.bfloat16
I32 = jnp.int32


def sigmoid(v):
    return 0.5 + 0.5 * jnp.tanh(0.5 * v)


def each(count, fn):
    if count <= 8:
        for i in range(count):
            fn(i)
    else:
        lax.fori_loop(0, count, lambda i, _: fn(i) or 0, 0)


def kernel(
    n_lat, n_lon, rows, width, half, blocks,
    dest_hbm, row_hbm, col_hbm, x_hbm, kin_hbm, kout_hbm, bias_hbm, weight_hbm, values_hbm, scale_hbm,
    out, inn_out,
    dest, row_off, col_off, bias,
    xv, xs, x_send, kin, kout, weight, values, scale_raw, scale, kw, load_sem,
    both, edge, edge_r, raw, edge_ss, edge_rs, raw_s, raw_r, X, X3, H3, slope, base, DF, den_s, den_r, block_a, block_b, block_d,
    pay, pay_at, pay_p, R, R_p, at_s, patches, pat_s, pat_r, Z, G, GW, out_h, out_s, out_r,
    plan, heard_up, heard_down,
    halo_s, halo_r, pair_s, pair_r, pay_ss, pay_rs, at_ss, at_rs, p_ss, p_rs, fwd_s, fwd_r, fp_s, copy_sem, pat_ss, pat_rs,
):
    lat, lon, ch = lax.axis_index("lat"), lax.axis_index("lon"), lax.axis_index("ch")
    other = 1 - ch
    chans = 2 * half
    obs = weight_hbm.shape[1]
    cells = PH * PW
    cols = 2 * width
    pitch = width + 2 * SIDE
    reach = width + SIDE
    strip = 2 * reach + PW
    blank = GROUP * PH * strip
    slots = n_lat * CAP
    sources = GROUP // CAP
    px = rows * width
    top, left = HALO, SIDE
    lon_right = lax.rem(lon + ch, n_lon)
    lon_left = lax.rem(lon + n_lon - other, n_lon)
    has_up = lat > 0
    has_down = lat < n_lat - 1
    sibling = {"ch": other}

    def at(dlat, side):
        place = {"lat": lat + dlat}
        if side:
            place["lon"] = lon_right if side > 0 else lon_left
            place["ch"] = other
        return place

    def outward(dlat):
        return {"lat": lat + dlat, "lon": jnp.where(ch == 0, lon_left, lon_right), "ch": other}

    def peer_of(j):
        m = jnp.minimum(lat, n_lat - 1 - lat)
        step = jnp.where(j < 2 * m, j // 2 + 1, j - m + 1)
        below = jnp.where(j < 2 * m, j % 2 == 0, lat > n_lat - 1 - lat)
        return jnp.where(below, lat - step, lat + step)

    loads = [
        pltpu.make_async_copy(src, dst, load_sem.at[i])
        for i, (src, dst) in enumerate(
            [(x_hbm, xv), (dest_hbm, dest), (row_hbm, row_off), (col_hbm, col_off),
             (weight_hbm, weight), (values_hbm, values), (scale_hbm, scale_raw),
             (kin_hbm, kin), (kout_hbm, kout), (bias_hbm, bias)]
        )
    ]
    for load in loads:
        load.start()
    barrier = pltpu.get_barrier_semaphore()

    def greet(place):
        pl.semaphore_signal(barrier, inc=1, device_id=place, device_id_type=MESH)

    greet(at(0, -1))
    greet(at(0, 1))
    chip_left = lax.rem(lon + n_lon - 1, n_lon)
    chip_right = lax.rem(lon + 1, n_lon)
    greet({"lon": chip_left})
    greet({"lon": chip_right})

    @pl.when(has_up)
    def _():
        for side in (-1, 0, 1):
            greet(at(-1, side))

    @pl.when(has_down)
    def _():
        for side in (-1, 0, 1):
            greet(at(1, side))

    def corner():
        return (
            lax.broadcasted_iota(I32, (half, cells), 0), lax.broadcasted_iota(I32, (half, cells), 1)
        )

    def prepare(b):
        row, lane = corner()
        w = weight[b]
        p = scale[pl.ds(b, 1), :]
        normal = jnp.dot((w.astype(F32).T * p).astype(BF16), w, preferred_element_type=F32)
        low = normal[half:cells]
        tri = jnp.where((lane < half) & (lane > row), pltpu.roll(low, half, 1), normal[0:half])
        tri = jnp.where(lane == row, 0.5 * tri, tri)
        block_a[b] = tri
        block_d[pl.ds(b, 1), :] = jnp.sum(jnp.where(lane == row + half, 0.5 * low, 0.0), axis=0, keepdims=True)
        block_b[b] = jnp.dot((values[b].astype(F32) * p).astype(BF16), w, preferred_element_type=F32)

    def pack_slot(s):
        def look(b, found):
            return jnp.where(plan[b] == s, b, found)

        found = lax.fori_loop(0, blocks, look, -1, unroll=blocks <= 8)
        source = jnp.maximum(found, 0)
        fill = jnp.where(found >= 0, 1.0, 0.0)
        t = s // CAP
        k = s % CAP
        pay[t, k, 0:half] = (block_b[source] * fill).astype(BF16)
        pay[t, k, half:chans] = (block_a[source] * fill).astype(BF16)
        pay_p[t, pl.ds(k, 1), :] = block_d[pl.ds(source, 1), :] * fill
        pay_at[t, pl.ds(2 * k, 1), :] = jnp.full((1, obs), row_off[source], I32)
        pay_at[t, pl.ds(2 * k + 1, 1), :] = jnp.full((1, obs), col_off[source], I32)

    loads[0].wait()
    for h in range(2):
        part = xv[:, :, h * width : (h + 1) * width].astype(F32)
        xs[h] = part.reshape(half * rows, width)
    for r in range(rows):
        both[ch, r] = xs[ch, pl.ds(r, half, stride=rows), :].astype(BF16)
        x_send[r] = xs[other, pl.ds(r, half, stride=rows), :].astype(BF16)
    lane = lax.broadcasted_iota(I32, (half, width), 1)
    for n, (h, first) in enumerate(((0, True), (1, False), (1, True), (0, False))):
        tile = None
        for r in range(rows):
            v = pltpu.roll(xs[h, pl.ds(r, half, stride=rows), :], (SIDE * r + (0 if first else SIDE)) % width, 1)
            tile = v if tile is None else jnp.where(lane // SIDE == r, v, tile)
        edge[n] = tile.astype(BF16)
    edge_r[other, ch] = edge[2 + ch]

    tops = (lat + n_lat - 1) // n_lat
    bottoms = (2 * n_lat - 2 - lat) // n_lat
    pl.semaphore_wait(barrier, 4 + 3 * tops + 3 * bottoms)

    def tell(sem, dlat):
        pl.semaphore_signal(sem, inc=1, device_id={"lat": lat + dlat}, device_id_type=MESH)

    @pl.when((lat == 1) & has_down)
    def _():
        tell(heard_up, 1)

    @pl.when((lat == n_lat - 2) & has_up)
    def _():
        tell(heard_down, -1)

    def pair_copy(src, dst, i):
        return pltpu.make_async_remote_copy(
            src_ref=src, dst_ref=dst, send_sem=pair_s.at[i], recv_sem=pair_r.at[i],
            device_id=sibling, device_id_type=MESH,
        )

    reshard = pair_copy(x_send, both.at[ch], 0)
    reshard.start()

    def raw_row(dl, mine):
        row = 0 if dl < 0 else rows - HALO
        src = both.at[ch, pl.ds(row, HALO)] if mine else x_send.at[pl.ds(row, HALO)]
        side = 1 if dl < 0 else 0
        return pltpu.make_async_remote_copy(
            src_ref=src, dst_ref=raw.at[side, ch], send_sem=raw_s.at[side],
            recv_sem=raw_r.at[side],
            device_id={"lat": lat + dl, "ch": ch if mine else other}, device_id_type=MESH,
        )

    def edge_copy(n, src, side, place):
        return pltpu.make_async_remote_copy(
            src_ref=edge.at[src], dst_ref=edge_r.at[side, ch], send_sem=edge_ss,
            recv_sem=edge_rs.at[n // 2], device_id=place, device_id_type=MESH,
        )

    def edge_got(n, count):
        part = pl.ds(0, count)
        return pltpu.make_async_remote_copy(
            src_ref=edge.at[part], dst_ref=edge.at[part], send_sem=edge_ss,
            recv_sem=edge_rs.at[n], device_id=sibling, device_id_type=MESH,
        )

    for dl in (-1, 1):
        @pl.when(has_up if dl < 0 else has_down)
        def _(dl=dl):
            raw_row(dl, 0).start()
            raw_row(dl, 1).start()

    edges = [
        edge_copy(0, 0, 1, {"lon": chip_left, "ch": 1}),
        edge_copy(1, 1, 0, {"lon": chip_right, "ch": 0}),
        edge_copy(2, 3 - ch, ch, sibling),
    ]
    for copy in edges:
        copy.start()
    for load in loads[1:7]:
        load.wait()
    def count_block(b, _):
        def earlier(e, rank):
            return rank + jnp.where(dest[e] == dest[b], 1, 0)

        plan[b] = dest[b] * CAP + lax.fori_loop(0, b, earlier, 0)
        return 0

    for b in range(blocks) if blocks <= 8 else ():
        rank = 0
        for e in range(b):
            rank = rank + jnp.where(dest[e] == dest[b], 1, 0)
        plan[b] = dest[b] * CAP + rank
    if blocks > 8:
        lax.fori_loop(0, blocks, count_block, 0)

    scale[...] = scale_raw[...].astype(F32)
    pay_at[...] = jnp.zeros(pay_at.shape, I32)
    pay_p[...] = jnp.zeros(pay_p.shape, F32)
    each(blocks, prepare)
    each(slots, pack_slot)
    def by_core(fn):
        for c in (0, 1):
            pl.when(ch == c)(functools.partial(fn, c))

    def big(peer, landing, c):
        part = pl.ds(0, half * (1 + c))
        return pltpu.make_async_remote_copy(
            src_ref=pay.at[peer, :, part], dst_ref=R.at[landing, c, :, part],
            send_sem=pay_ss, recv_sem=pay_rs.at[landing],
            device_id={"lat": peer}, device_id_type=MESH,
        )

    def small(peer, landing, kind):
        src, dst, ss, rs = ((pay_at, at_s, at_ss, at_rs), (pay_p, R_p, p_ss, p_rs.at[landing]))[kind]
        return pltpu.make_async_remote_copy(
            src_ref=src.at[peer], dst_ref=dst.at[landing], send_sem=ss, recv_sem=rs,
            device_id={"lat": peer}, device_id_type=MESH,
        )

    def start_small(peer):
        small(peer, lat, 0).start()

        @pl.when(ch == 1)
        def _():
            small(peer, lat, 1).start()

    def start_big(peer):
        by_core(lambda c: big(peer, lat, c).start())

    middle = has_up & has_down

    def upward(j):
        return j + jnp.where(lat <= j, 1, 0)

    def send_far():
        each(n_lat - 1, lambda j: pl.when(far_off(upward(j)))(lambda: start_small(upward(j))))
        each(n_lat - 1, lambda j: start_big(upward(j)))

    def far_off(peer):
        return (peer > lat + 1) | (peer < lat - 1)

    def send_near_small():
        pl.when(has_up)(lambda: start_small(lat - 1))
        pl.when(has_down)(lambda: start_small(lat + 1))

    def put_row(taps, r, v):
        taps[r * pitch : (r + 1) * pitch, 0:chans] = pltpu.roll(v, 1, 0).astype(BF16)
        taps[r * pitch : (r + 1) * pitch, chans : 2 * chans] = v.astype(BF16)
        taps[r * pitch : (r + 1) * pitch, 2 * chans :] = pltpu.roll(v, pitch - 1, 0).astype(BF16)

    def conv(taps, kind, first, count):
        acc = None
        for a in range(3):
            parts = [taps[(f + a) * pitch : (f + a + count) * pitch, :] for f in first]
            part = jnp.dot(jnp.concatenate(parts, axis=0), kw[kind, a], preferred_element_type=F32)
            acc = part if acc is None else acc + part
        return acc

    def edge_factor(r):
        if r == 0:
            return jnp.where(has_up, 1.0, 0.0)
        if r == rows + 1:
            return jnp.where(has_down, 1.0, 0.0)
        return None

    def guarded(dl, fn):
        if dl == 0:
            fn()
        else:
            pl.when(has_up if dl < 0 else has_down)(fn)

    def span(start, size):
        return pl.ds(start if isinstance(start, int) else pl.multiple_of(start, SIDE), size)

    def remote(buf, place, sr, dr, nr, sc, dc, nc, i):
        return pltpu.make_async_remote_copy(
            src_ref=buf.at[pl.ds(sr, nr), span(sc, nc)], dst_ref=buf.at[pl.ds(dr, nr), span(dc, nc)],
            send_sem=halo_s.at[i], recv_sem=halo_r.at[i], device_id=place, device_id_type=MESH,
        )

    span_r = {-1: (top, rows + top, HALO), 0: (top, top, rows), 1: (top + rows - HALO, 0, HALO)}
    span_c = {-1: (left, left + width, SIDE), 0: (left, left, width), 1: (left + width - SIDE, 0, SIDE)}

    def x_routes():
        routes = {-1: [], 1: []}
        for i, dl in enumerate((-1, 1)):
            sr, dr, nr = span_r[dl]
            for side in (-1, 1):
                sc, dc, nc = span_c[side]
                routes[dl].append(remote(X, at(dl, side), sr, dr, nr, sc, dc, nc, i))
        return routes, {-1: (X, HALO, 2 * SIDE, 0), 1: (X, HALO, 2 * SIDE, 1)}

    out_src = left + ch * (width - SIDE)
    out_dst = other * (left + width)

    def g_side():
        copy = remote(G, outward(0), top, top, rows, out_src, out_dst, SIDE, 4)
        return {0: [copy]}, {0: (G, rows, SIDE, 4)}

    def g_rows(depth):
        routes, whole = {}, {}
        for n, dl in enumerate((-1, 1)):
            i = 2 + n if depth == 0 else 5 + n
            sr = top + depth if dl < 0 else top + rows - 1 - depth
            dr = rows + top + depth if dl < 0 else HALO - 1 - depth
            routes[dl] = [
                remote(G, at(dl, 0), sr, dr, 1, other * SIDE, other * SIDE, reach, i),
                remote(G, outward(dl), sr, dr, 1, out_src, out_dst, SIDE, i),
            ]
            whole[dl] = (G, 1, pitch, i)
        return routes, whole

    def halo_start(halo, order):
        for dl in order:
            def go(dl=dl):
                for copy in halo[0][dl]:
                    copy.start()

            guarded(dl, go)

    def halo_finish(halo, order):
        for dl in order:
            def whole(dl=dl):
                buf, nr, nc, i = halo[1][dl]
                return remote(buf, sibling, 0, 0, nr, 0, 0, nc, i)

            guarded(dl, lambda: whole().wait_send())
            guarded(-dl, lambda: whole().wait_recv())

    def clear_poles(buf):
        @pl.when(lat == 0)
        def _():
            buf[0:HALO] = jnp.zeros((HALO, pitch, chans), BF16)

        @pl.when(lat == n_lat - 1)
        def _():
            buf[rows + HALO : rows + 2 * HALO] = jnp.zeros((HALO, pitch, chans), BF16)

    clear_poles(X)
    clear_poles(G)

    reshard.wait()
    for r in range(rows):
        X[top + r, left : left + width] = (
            jnp.concatenate([both[0, r], both[1, r]], axis=0).astype(F32).T.astype(BF16)
        )
    x_halo = x_routes()
    halo_start(x_halo, (-1, 1))

    send_near_small()

    @pl.when(middle)
    def _():
        @pl.when(lat >= 2)
        def _():
            pl.semaphore_wait(heard_up, 1)
            tell(heard_up, 1)

        @pl.when(lat <= n_lat - 3)
        def _():
            pl.semaphore_wait(heard_down, 1)
            tell(heard_down, -1)

        send_far()

    R[lat, ch] = pay[lat]
    own_at = pltpu.make_async_copy(pay_at.at[lat], at_s.at[lat], copy_sem)
    own_at.start()
    R_p[lat] = pay_p[lat]

    def forward(t, c):
        part = pl.ds(0, half * (1 + c))
        return pltpu.make_async_remote_copy(
            src_ref=R.at[t, c, :, part], dst_ref=R.at[t, c, :, part], send_sem=fwd_s, recv_sem=fwd_r.at[t],
            device_id=sibling, device_id_type=MESH,
        )

    def forward_small(t):
        return pltpu.make_async_remote_copy(
            src_ref=R_p.at[t], dst_ref=R_p.at[t], send_sem=fp_s, recv_sem=p_rs.at[t],
            device_id=sibling, device_id_type=MESH,
        )

    by_core(lambda c: forward(lat, c).start())
    for load in loads[7:]:
        load.wait()
    for kind, k in enumerate((kin, kout, kout, kin)):
        for a in range(3):
            for b in range(3):
                tap = k[a, b].astype(F32).T.astype(BF16) if kind < 2 else k[2 - a, 2 - b]
                kw[kind, a, b * chans : (b + 1) * chans] = tap
    Z[...] = jnp.zeros(Z.shape, F32)

    @pl.when(jnp.logical_not(middle))
    def _():
        @pl.when(lat >= 2)
        def _():
            pl.semaphore_wait(heard_up, 1)

        @pl.when(lat <= n_lat - 3)
        def _():
            pl.semaphore_wait(heard_down, 1)

        send_far()

    def hidden_rows(first, count):
        acc = conv(X3, 0, first, count) + bias[...]
        s = sigmoid(acc)
        steep = s * (1.0 + acc * (1.0 - s))
        h = acc * s
        for i, r in enumerate(f + n for f in first for n in range(count)):
            own = slice(i * pitch, (i + 1) * pitch)
            slope[r * pitch : (r + 1) * pitch, :] = steep[own]
            row = h[own]
            f = edge_factor(r)
            if f is not None:
                row = row * f
            put_row(H3, r, row.astype(BF16).astype(F32))

    edge_got(0, 3).wait_send()
    edge_got(1, 1).wait_recv()
    edge_got(0, 2).wait_recv()
    for side in (0, 1):
        turned = jnp.concatenate([edge_r[side, 0], edge_r[side, 1]], axis=0).astype(F32).T.astype(BF16)
        for r in range(rows):
            X[top + r, side * (left + width) : side * (left + width) + SIDE] = turned[r * SIDE : (r + 1) * SIDE]
    for r in range(top, top + rows):
        put_row(X3, r, X[r].astype(F32))
    for r0 in range(HALO, rows, 2):
        hidden_rows([r0], 2)
    def denoise_rows(first, count):
        acc = conv(H3, 1, first, count)
        for i, r in enumerate(f + n for f in first for n in range(count)):
            state = X[top + r, left : left + width].astype(F32)
            den = (state + acc[i * pitch + left : i * pitch + left + width]).astype(BF16)
            den_s[r] = den
            wide = den.astype(F32)
            base[r * width : (r + 1) * width, :] = keep_rate * state + blend_rate * wide
            DF[pl.ds(pl.multiple_of(r * cols + ch * width, width), width), :] = wide
        for f in first:
            part = pl.ds(f, count)
            pair_copy(den_s.at[part], den_r.at[part], 1).start()

    inner = [([r0], min(WIDE, rows - HALO - r0)) for r0 in range(HALO, rows - HALO, WIDE)]
    outer = [([0, rows - HALO], HALO)]
    for first, count in inner:
        denoise_rows(first, count)
    halo_finish(x_halo, (-1, 1))
    for dl in (-1, 1):
        @pl.when(has_up if dl < 0 else has_down)
        def _(dl=dl):
            pltpu.make_async_remote_copy(
                src_ref=x_send.at[pl.ds(0, 2 * HALO)], dst_ref=x_send.at[pl.ds(0, 2 * HALO)],
                send_sem=raw_s.at[1 if dl < 0 else 0], recv_sem=raw_r.at[0 if dl < 0 else 1],
                device_id=sibling, device_id_type=MESH,
            ).wait()
            for i in range(HALO):
                side = 0 if dl < 0 else 1
                X[side * (top + rows) + i, left : left + width] = (
                    jnp.concatenate([raw[side, 0, i], raw[side, 1, i]], axis=0).astype(F32).T.astype(BF16)
                )

    for r in (0, 1, top + rows, top + rows + 1):
        put_row(X3, r, X[r].astype(F32))
    hidden_rows([0, rows], HALO)
    for first, count in outer:
        denoise_rows(first, count)

    own_at.wait()
    pltpu.make_async_remote_copy(
        src_ref=pay_at.at[pl.ds(0, n_lat - 1)], dst_ref=at_s.at[pl.ds(0, n_lat - 1)], send_sem=at_ss, recv_sem=at_rs,
        device_id=sibling, device_id_type=MESH,
    ).wait_recv()

    def take_pay(j):
        peer = peer_of(j)

        def go(c):
            big(peer, peer, c).wait_recv()
            forward(peer, c).start()
            if c == 1:
                small(peer, peer, 1).wait_recv()
                forward_small(peer).start()

        by_core(go)

    def take_from(j0):
        each(n_lat - 1 - j0, lambda j: take_pay(j + j0))

    batches = slots // GROUP
    split = batches == 2
    if split:
        pl.when(jnp.logical_not(middle))(lambda: take_pay(0))
    pair_copy(den_s, den_r, 1).wait()
    for r in range(rows):
        DF[pl.ds(pl.multiple_of(r * cols + other * width, width), width), :] = den_r[r].astype(F32)

    def gather(t):
        lane = lax.broadcasted_iota(I32, (half, chans), 1)
        for k in range(CAP):
            r0 = at_s[t, 2 * k, 0]
            q0 = at_s[t, 2 * k + 1, 0]
            cut = [DF[pl.ds((r0 + a) * cols + q0, PW), :] for a in range(PH)]
            first = jnp.concatenate(cut[: PH // 2], axis=0)
            second = jnp.concatenate(cut[PH // 2 :], axis=0)
            patches[t, k, 0:half] = first.astype(BF16)
            patches[t, k, half:cells] = second.astype(BF16)
            keep_first = jnp.where(ch == 0, first, pltpu.roll(first, half, 1))
            keep_second = jnp.where(ch == 0, pltpu.roll(second, half, 1), second)
            pat_s[t, k] = jnp.where(lane < half, keep_first, keep_second).astype(BF16)

    each(n_lat, gather)

    def patch_copy(peer, landing):
        return pltpu.make_async_remote_copy(
            src_ref=pat_s.at[peer], dst_ref=pat_r.at[landing],
            send_sem=pat_ss, recv_sem=pat_rs,
            device_id={"lat": peer}, device_id_type=MESH,
        )

    each(n_lat - 1, lambda j: patch_copy(peer_of(j), lat).start())
    pat_r[lat] = pat_s[lat]
    start = ch * (cols - reach)

    def source_of(j):
        return jnp.where(j == 0, lat, peer_of(jnp.maximum(j - 1, 0)))

    def settle(t):
        by_core(lambda c: forward(t, 1 - c).wait_recv())

        @pl.when((ch == 0) & (t != lat))
        def _():
            forward_small(t).wait_recv()

    def drain(src, dst, sem):
        pltpu.make_async_remote_copy(
            src_ref=src, dst_ref=dst, send_sem=sem, recv_sem=pay_rs.at[0],
            device_id=sibling, device_id_type=MESH,
        ).wait_send()

    def drain_all():
        others = pl.ds(0, n_lat - 1)

        def go(c):
            part = pl.ds(0, half * (1 + c))
            drain(pay.at[others, :, part], R.at[others, c, :, part], pay_ss)
            drain(R.at[:, c, :, part], R.at[:, c, :, part], fwd_s)
            if c == 1:
                drain(pay_p.at[others], R_p.at[others], p_ss)
                drain(R_p.at[others], R_p.at[others], fp_s)

        by_core(go)
        drain(pay_at.at[others], at_s.at[others], at_ss)
        drain(pat_s.at[others], pat_r.at[others], pat_ss)

    g_halo = [g_rows(depth) for depth in range(HALO)]
    g_edge = g_side()

    def observe(g, first, last):
        owners = [source_of(g * sources + i) for i in range(sources)]
        for t in owners:
            settle(t)
        for i in range(GROUP):
            t, k = owners[i // CAP], i % CAP
            row, lane = corner()
            tri = R[t, 1, k, half:chans].astype(F32)
            upper = jnp.where((lane <= row) | (lane >= half), tri, 0.0)
            lower = jnp.where(lane > row + half, pltpu.roll(tri, half, 1), 0.0)
            lower = jnp.where(lane == row + half, R_p[t, k : k + 1, :], lower)
            side = jnp.concatenate([upper, lower], axis=0).astype(BF16)
            normal = side + side.T
            pull = jnp.concatenate([R[t, 0, k, 0:half], R[t, 1, k, 0:half]], axis=0)
            pulled = jnp.dot(normal, patches[t, k], preferred_element_type=F32) - pull.astype(F32).T
            for a in range(PH):
                Z[pl.ds((i * PH + a) * strip + reach, PW), :] = pulled[a * PW : (a + 1) * PW]
        for n, r in enumerate((0, rows - 1, 1, rows - 2, *range(2, rows - 2))):
            total = None
            for i in range(GROUP):
                t, k = owners[i // CAP], i % CAP
                r0 = at_s[t, 2 * k, 0]
                place = jnp.clip(at_s[t, 2 * k + 1, 0] - start, -PW, reach)
                inside = (r >= r0) & (r < r0 + PH)
                begin = jnp.where(inside, (i * PH + r - r0) * strip + reach - place, blank)
                v = Z[pl.ds(begin, reach), :]
                total = v if total is None else total + v
            span_w = pl.ds(pl.multiple_of(r * pitch + other * SIDE, SIDE), reach)
            if not first:
                total = total + GW[span_w, :]
            GW[span_w, :] = total
            if last:
                G[top + r, pl.ds(pl.multiple_of(other * SIDE, SIDE), reach)] = total.astype(BF16)
                if n in (1, 3):
                    halo_start(g_halo[n // 2], (-1, 1))
        if last:
            halo_start(g_edge, (0,))

    if split:
        pl.when(middle)(lambda: take_from(0))
    else:
        take_from(0)
    if split:
        observe(0, True, False)
        pl.when(jnp.logical_not(middle))(lambda: take_from(1))
        observe(1, False, True)
    elif batches == 1:
        observe(0, True, True)
    else:
        observe(0, True, False)
        lax.fori_loop(1, batches - 1, lambda g, _: observe(g, False, False) or 0, 0)
        observe(batches - 1, False, True)

    def grad_rows(first, count):
        back = conv(X3, 2, first, count)
        for i, r in enumerate(f + n for f in first for n in range(count)):
            row = back[i * pitch : (i + 1) * pitch] * slope[r * pitch : (r + 1) * pitch, :]
            f = edge_factor(r)
            if f is not None:
                row = row * f
            put_row(H3, r, row.astype(BF16).astype(F32))

    halo_finish(g_edge, (0,))
    for r in range(top, top + rows):
        put_row(X3, r, G[r].astype(F32))
    for r0 in range(HALO, rows, 2):
        grad_rows([r0], 2)

    def finish_rows(first, count, sem):
        acc = conv(H3, 3, first, count)
        order = [f + n for f in first for n in range(count)]
        kept = []
        for i, r in enumerate(order):
            grad = GW[r * pitch + left : r * pitch + left + width, :] + acc[i * pitch + left : i * pitch + left + width]
            res = (base[r * width : (r + 1) * width, :] - guide_rate * grad).T
            out_s[r] = jnp.where(ch == 0, res[half:chans], res[0:half]).astype(BF16)
            kept.append(jnp.where(ch == 0, res[0:half], res[half:chans]))
        for f in first:
            part = pl.ds(f, count)
            pair_copy(out_s.at[part], out_r.at[part], sem).start()
        for r, mine_r in zip(order, kept):
            out_h[0, pl.ds(r, half, stride=rows), :] = mine_r

    for first, count in inner:
        finish_rows(first, count, 2)
    others = pl.ds(0, n_lat - 1)
    pltpu.make_async_remote_copy(
        src_ref=pat_s.at[others], dst_ref=pat_r.at[others], send_sem=pat_ss, recv_sem=pat_rs,
        device_id=sibling, device_id_type=MESH,
    ).wait_recv()
    drain_all()

    def innovate(b):
        slot = plan[b]
        part = pat_r[slot // CAP, slot % CAP].astype(F32)
        patch = jnp.concatenate([part, pltpu.roll(part, half, 1)], axis=0).astype(BF16)
        predicted = jnp.dot(weight[b], patch, preferred_element_type=F32).T
        inn_out[b] = (predicted[0:half] - values[b].astype(F32)).astype(BF16)

    each(blocks, innovate)
    for depth in range(HALO):
        halo_finish(g_halo[depth], (-1, 1))
        for r in (HALO - 1 - depth, top + rows + depth):
            put_row(X3, r, G[r].astype(F32))
        grad_rows([HALO - 1 - depth, rows + depth], 1)
        finish_rows([HALO - 1 - depth, rows - HALO + depth], 1, 3)
    mine = pl.ds(pl.multiple_of(ch * width, width), width)
    theirs = pl.ds(pl.multiple_of(other * width, width), width)
    out[:, mine] = out_h[0]

    middle_rows = tuple(range(HALO, rows - HALO))
    edge_rows = (*range(HALO), *range(rows - HALO, rows))
    for sem, which in ((2, middle_rows), (3, edge_rows)):
        part = pl.ds(0, len(which))
        pair_copy(out_s.at[part], out_r.at[part], sem).wait()
        for r in which:
            out_h[1, pl.ds(r, half, stride=rows), :] = out_r[r].astype(F32)
    out[:, theirs] = out_h[1]


def store(out, innovation, out_hbm, innovation_hbm, sem):
    copies = [
        pltpu.make_async_copy(out, out_hbm, sem.at[0]),
        pltpu.make_async_copy(innovation, innovation_hbm, sem.at[1]),
    ]
    for copy in copies:
        copy.start()
    for copy in copies:
        copy.wait()


def body(n_lat, n_lon, noisy_state, kernel_in, bias_in, kernel_out, interp_weight, observed,
         obs_precision, dest_tile, row_offset, col_offset):
    half, rows, cols = noisy_state.shape
    chans = 2 * half
    width = cols // 2
    blocks, obs, cells = interp_weight.shape
    slots = n_lat * CAP
    pitch = width + 2 * SIDE
    reach = width + SIDE
    px = rows * width
    vmem = pl.BlockSpec(memory_space=pltpu.VMEM)
    hbm = pl.BlockSpec(memory_space=pltpu.HBM)
    dma = pltpu.SemaphoreType.DMA
    call = pl.pallas_call(
        functools.partial(kernel, n_lat, n_lon, rows, width, half, blocks),
        out_shape=(
            pltpu.VMEM((half * rows, cols), F32),
            pltpu.VMEM((blocks, half, obs), BF16),
        ),
        in_specs=[hbm] * 10,
        out_specs=(vmem, vmem),
        scratch_shapes=[
            pltpu.SMEM((blocks,), I32),
            pltpu.SMEM((blocks,), I32),
            pltpu.SMEM((blocks,), I32),
            pltpu.VMEM((1, chans), F32),
            pltpu.VMEM((half, rows, cols), BF16),
            pltpu.VMEM((2, half * rows, width), F32),
            pltpu.VMEM((rows, half, width), BF16),
            pltpu.VMEM(kernel_in.shape, BF16),
            pltpu.VMEM(kernel_out.shape, BF16),
            pltpu.VMEM(interp_weight.shape, BF16),
            pltpu.VMEM(observed.shape, BF16),
            pltpu.VMEM(obs_precision.shape, BF16),
            pltpu.VMEM(obs_precision.shape, F32),
            pltpu.VMEM((4, 3, 3 * chans, chans), BF16),
            dma((10,)),
            pltpu.VMEM((2, rows, half, width), BF16),
            pltpu.VMEM((4, half, width), BF16),
            pltpu.VMEM((2, 2, half, width), BF16),
            pltpu.VMEM((2, 2, HALO, half, width), BF16),
            dma, dma((2,)),
            dma((2,)), dma((2,)),
            pltpu.VMEM((rows + 4, pitch, chans), BF16),
            pltpu.VMEM(((rows + 4) * pitch, 3 * chans), BF16),
            pltpu.VMEM(((rows + 2) * pitch, 3 * chans), BF16),
            pltpu.VMEM(((rows + 2) * pitch, chans), F32),
            pltpu.VMEM((px, chans), F32),
            pltpu.VMEM((rows * cols, chans), F32),
            pltpu.VMEM((rows, width, chans), BF16),
            pltpu.VMEM((rows, width, chans), BF16),
            pltpu.VMEM((blocks, half, cells), F32),
            pltpu.VMEM((blocks, half, cells), F32),
            pltpu.VMEM((blocks, cells), F32),
            pltpu.VMEM((n_lat, CAP, chans, cells), BF16),
            pltpu.VMEM((n_lat, SMALL, obs), I32),
            pltpu.VMEM((n_lat, SMALL, obs), F32),
            pltpu.VMEM((n_lat, 2, CAP, chans, cells), BF16),
            pltpu.VMEM((n_lat, SMALL, obs), F32),
            pltpu.SMEM((n_lat, SMALL, obs), I32),
            pltpu.VMEM((n_lat, CAP, cells, chans), BF16),
            pltpu.VMEM((n_lat, CAP, half, chans), BF16),
            pltpu.VMEM((n_lat, CAP, half, chans), BF16),
            pltpu.VMEM((GROUP * PH * (2 * reach + PW) + reach, chans), F32),
            pltpu.VMEM((rows + 4, pitch, chans), BF16),
            pltpu.VMEM((rows * pitch, chans), F32),
            pltpu.VMEM((2, half * rows, width), F32),
            pltpu.VMEM((rows, half, width), BF16),
            pltpu.VMEM((rows, half, width), BF16),
            pltpu.SMEM((blocks,), I32),
            pltpu.SemaphoreType.REGULAR,
            pltpu.SemaphoreType.REGULAR,
            dma((7,)), dma((7,)),
            dma((4,)), dma((4,)),
            dma, dma((n_lat,)),
            dma, dma,
            dma, dma((n_lat,)),
            dma, dma((n_lat,)),
            dma,
            dma,
            dma, dma,
        ],
        compiler_params=pltpu.CompilerParams(
            collective_id=0, has_side_effects=True, vmem_limit_bytes=(63 if slots <= 2 * GROUP else 48) * 1024 * 1024
        ),
    )
    out, innovation = call(
        dest_tile, row_offset, col_offset, noisy_state, kernel_in, kernel_out,
        bias_in.reshape(1, chans), interp_weight, observed, obs_precision,
    )
    out, innovation = pl.pallas_call(
        store,
        out_shape=(
            jax.ShapeDtypeStruct((half * rows, cols), F32),
            jax.ShapeDtypeStruct((blocks, half, obs), BF16),
        ),
        in_specs=[vmem, vmem],
        out_specs=(hbm, hbm),
        scratch_shapes=[dma((2,))],
    )(*(pltpu.with_memory_space_constraint(a, pltpu.VMEM) for a in (out, innovation)))
    return out.reshape(half, rows, cols), innovation


def solution(mesh):
    return jax.shard_map(
        functools.partial(body, mesh.shape["lat"], mesh.shape["lon"]),
        mesh=mesh,
        in_specs=(
            P(("grp", "ch"), "lat", "lon"),
            P(),
            P(),
            P(),
            P(("grp", "lat", "lon"), None, None),
            P(("grp", "lat", "lon"), "ch", None),
            P(("grp", "lat", "lon"), None),
            P(("grp", "lat", "lon")),
            P(("grp", "lat", "lon")),
            P(("grp", "lat", "lon")),
        ),
        out_specs=(P(("grp", "ch"), "lat", "lon"), P(("grp", "lat", "lon"), "ch", None)),
        check_vma=False,
    )
```

```python
import functools

import jax
import jax.numpy as jnp
from jax import lax
from jax.experimental import pallas as pl
from jax.experimental.pallas import tpu as pltpu
from jax.sharding import PartitionSpec as P

PH = 4
PW = 32
CAP = 2
HALO = 2
SIDE = 16
GROUP = 4
WIDE = 4
SMALL = 8

keep_rate = 0.6
blend_rate = 0.4
guide_rate = 0.3

MESH = pl.DeviceIdType.MESH
F32 = jnp.float32
BF16 = jnp.bfloat16
I32 = jnp.int32


def sigmoid(v):
    return 0.5 + 0.5 * jnp.tanh(0.5 * v)


def each(count, fn):
    if count <= 8:
        for i in range(count):
            fn(i)
    else:
        lax.fori_loop(0, count, lambda i, _: fn(i) or 0, 0)


def kernel(
    n_lat, n_lon, rows, width, half, blocks,
    dest_hbm, row_hbm, col_hbm, x_hbm, kin_hbm, kout_hbm, bias_hbm, weight_hbm, values_hbm, scale_hbm,
    out, inn_out,
    dest, row_off, col_off, bias,
    xv, xs, x_send, kin, kout, weight, values, scale_raw, scale, kw, load_sem,
    both, edge, edge_r, raw, edge_ss, edge_rs, raw_s, raw_r, X, X3, H3, slope, base, DF, den_s, den_r, block_a, block_b, block_d,
    pay, pay_at, pay_p, R, R_p, at_s, patches, pat_s, pat_r, Z, G, GW, out_h, out_s, out_r,
    plan, heard_up, heard_down,
    halo_s, halo_r, pair_s, pair_r, pay_ss, pay_rs, at_ss, at_rs, p_ss, p_rs, fwd_s, fwd_r, fp_s, copy_sem, pat_ss, pat_rs,
):
    lat, lon, ch = lax.axis_index("lat"), lax.axis_index("lon"), lax.axis_index("ch")
    other = 1 - ch
    chans = 2 * half
    obs = weight_hbm.shape[1]
    cells = PH * PW
    cols = 2 * width
    pitch = width + 2 * SIDE
    reach = width + SIDE
    strip = 2 * reach + PW
    blank = GROUP * PH * strip
    slots = n_lat * CAP
    sources = GROUP // CAP
    px = rows * width
    top, left = HALO, SIDE
    lon_right = lax.rem(lon + ch, n_lon)
    lon_left = lax.rem(lon + n_lon - other, n_lon)
    has_up = lat > 0
    has_down = lat < n_lat - 1
    sibling = {"ch": other}

    def at(dlat, side):
        place = {"lat": lat + dlat}
        if side:
            place["lon"] = lon_right if side > 0 else lon_left
            place["ch"] = other
        return place

    def outward(dlat):
        return {"lat": lat + dlat, "lon": jnp.where(ch == 0, lon_left, lon_right), "ch": other}

    def peer_of(j):
        m = jnp.minimum(lat, n_lat - 1 - lat)
        step = jnp.where(j < 2 * m, j // 2 + 1, j - m + 1)
        below = jnp.where(j < 2 * m, j % 2 == 0, lat > n_lat - 1 - lat)
        return jnp.where(below, lat - step, lat + step)

    loads = [
        pltpu.make_async_copy(src, dst, load_sem.at[i])
        for i, (src, dst) in enumerate(
            [(x_hbm, xv), (dest_hbm, dest), (row_hbm, row_off), (col_hbm, col_off),
             (weight_hbm, weight), (values_hbm, values), (scale_hbm, scale_raw),
             (kin_hbm, kin), (kout_hbm, kout), (bias_hbm, bias)]
        )
    ]
    for load in loads:
        load.start()
    barrier = pltpu.get_barrier_semaphore()

    def greet(place):
        pl.semaphore_signal(barrier, inc=1, device_id=place, device_id_type=MESH)

    greet(at(0, -1))
    greet(at(0, 1))
    chip_left = lax.rem(lon + n_lon - 1, n_lon)
    chip_right = lax.rem(lon + 1, n_lon)
    greet({"lon": chip_left})
    greet({"lon": chip_right})

    @pl.when(has_up)
    def _():
        for side in (-1, 0, 1):
            greet(at(-1, side))

    @pl.when(has_down)
    def _():
        for side in (-1, 0, 1):
            greet(at(1, side))

    def corner():
        return (
            lax.broadcasted_iota(I32, (half, cells), 0), lax.broadcasted_iota(I32, (half, cells), 1)
        )

    def prepare(b):
        row, lane = corner()
        w = weight[b]
        p = scale[pl.ds(b, 1), :]
        normal = jnp.dot((w.astype(F32).T * p).astype(BF16), w, preferred_element_type=F32)
        low = normal[half:cells]
        tri = jnp.where((lane < half) & (lane > row), pltpu.roll(low, half, 1), normal[0:half])
        tri = jnp.where(lane == row, 0.5 * tri, tri)
        block_a[b] = tri
        block_d[pl.ds(b, 1), :] = jnp.sum(jnp.where(lane == row + half, 0.5 * low, 0.0), axis=0, keepdims=True)
        block_b[b] = jnp.dot((values[b].astype(F32) * p).astype(BF16), w, preferred_element_type=F32)

    def pack_slot(s):
        def look(b, found):
            return jnp.where(plan[b] == s, b, found)

        found = lax.fori_loop(0, blocks, look, -1, unroll=blocks <= 8)
        source = jnp.maximum(found, 0)
        fill = jnp.where(found >= 0, 1.0, 0.0)
        t = s // CAP
        k = s % CAP
        pay[t, k, 0:half] = (block_b[source] * fill).astype(BF16)
        pay[t, k, half:chans] = (block_a[source] * fill).astype(BF16)
        pay_p[t, pl.ds(k, 1), :] = block_d[pl.ds(source, 1), :] * fill
        pay_at[t, pl.ds(2 * k, 1), :] = jnp.full((1, obs), row_off[source], I32)
        pay_at[t, pl.ds(2 * k + 1, 1), :] = jnp.full((1, obs), col_off[source], I32)

    loads[0].wait()
    for h in range(2):
        part = xv[:, :, h * width : (h + 1) * width].astype(F32)
        xs[h] = part.reshape(half * rows, width)
    for r in range(rows):
        both[ch, r] = xs[ch, pl.ds(r, half, stride=rows), :].astype(BF16)
        x_send[r] = xs[other, pl.ds(r, half, stride=rows), :].astype(BF16)
    lane = lax.broadcasted_iota(I32, (half, width), 1)
    for n, (h, first) in enumerate(((0, True), (1, False), (1, True), (0, False))):
        tile = None
        for r in range(rows):
            v = pltpu.roll(xs[h, pl.ds(r, half, stride=rows), :], (SIDE * r + (0 if first else SIDE)) % width, 1)
            tile = v if tile is None else jnp.where(lane // SIDE == r, v, tile)
        edge[n] = tile.astype(BF16)
    edge_r[other, ch] = edge[2 + ch]

    tops = (lat + n_lat - 1) // n_lat
    bottoms = (2 * n_lat - 2 - lat) // n_lat
    pl.semaphore_wait(barrier, 4 + 3 * tops + 3 * bottoms)

    def tell(sem, dlat):
        pl.semaphore_signal(sem, inc=1, device_id={"lat": lat + dlat}, device_id_type=MESH)

    @pl.when((lat == 1) & has_down)
    def _():
        tell(heard_up, 1)

    @pl.when((lat == n_lat - 2) & has_up)
    def _():
        tell(heard_down, -1)

    def pair_copy(src, dst, i):
        return pltpu.make_async_remote_copy(
            src_ref=src, dst_ref=dst, send_sem=pair_s.at[i], recv_sem=pair_r.at[i],
            device_id=sibling, device_id_type=MESH,
        )

    reshard = pair_copy(x_send, both.at[ch], 0)
    reshard.start()

    def raw_row(dl, mine):
        row = 0 if dl < 0 else rows - HALO
        src = both.at[ch, pl.ds(row, HALO)] if mine else x_send.at[pl.ds(row, HALO)]
        side = 1 if dl < 0 else 0
        return pltpu.make_async_remote_copy(
            src_ref=src, dst_ref=raw.at[side, ch], send_sem=raw_s.at[side],
            recv_sem=raw_r.at[side],
            device_id={"lat": lat + dl, "ch": ch if mine else other}, device_id_type=MESH,
        )

    def edge_copy(n, src, side, place):
        return pltpu.make_async_remote_copy(
            src_ref=edge.at[src], dst_ref=edge_r.at[side, ch], send_sem=edge_ss,
            recv_sem=edge_rs.at[n // 2], device_id=place, device_id_type=MESH,
        )

    def edge_got(n, count):
        part = pl.ds(0, count)
        return pltpu.make_async_remote_copy(
            src_ref=edge.at[part], dst_ref=edge.at[part], send_sem=edge_ss,
            recv_sem=edge_rs.at[n], device_id=sibling, device_id_type=MESH,
        )

    for dl in (-1, 1):
        @pl.when(has_up if dl < 0 else has_down)
        def _(dl=dl):
            raw_row(dl, 0).start()
            raw_row(dl, 1).start()

    edges = [
        edge_copy(0, 0, 1, {"lon": chip_left, "ch": 1}),
        edge_copy(1, 1, 0, {"lon": chip_right, "ch": 0}),
        edge_copy(2, 3 - ch, ch, sibling),
    ]
    for copy in edges:
        copy.start()
    for load in loads[1:7]:
        load.wait()
    def count_block(b, _):
        def earlier(e, rank):
            return rank + jnp.where(dest[e] == dest[b], 1, 0)

        plan[b] = dest[b] * CAP + lax.fori_loop(0, b, earlier, 0)
        return 0

    for b in range(blocks) if blocks <= 8 else ():
        rank = 0
        for e in range(b):
            rank = rank + jnp.where(dest[e] == dest[b], 1, 0)
        plan[b] = dest[b] * CAP + rank
    if blocks > 8:
        lax.fori_loop(0, blocks, count_block, 0)

    scale[...] = scale_raw[...].astype(F32)
    pay_at[...] = jnp.zeros(pay_at.shape, I32)
    pay_p[...] = jnp.zeros(pay_p.shape, F32)
    each(blocks, prepare)
    each(slots, pack_slot)
    def by_core(fn):
        for c in (0, 1):
            pl.when(ch == c)(functools.partial(fn, c))

    def big(peer, landing, c):
        part = pl.ds(0, half * (1 + c))
        return pltpu.make_async_remote_copy(
            src_ref=pay.at[peer, :, part], dst_ref=R.at[landing, c, :, part],
            send_sem=pay_ss, recv_sem=pay_rs.at[landing],
            device_id={"lat": peer}, device_id_type=MESH,
        )

    def small(peer, landing, kind):
        src, dst, ss, rs = ((pay_at, at_s, at_ss, at_rs), (pay_p, R_p, p_ss, p_rs.at[landing]))[kind]
        return pltpu.make_async_remote_copy(
            src_ref=src.at[peer], dst_ref=dst.at[landing], send_sem=ss, recv_sem=rs,
            device_id={"lat": peer}, device_id_type=MESH,
        )

    def start_small(peer):
        small(peer, lat, 0).start()

        @pl.when(ch == 1)
        def _():
            small(peer, lat, 1).start()

    def start_big(peer):
        by_core(lambda c: big(peer, lat, c).start())

    middle = has_up & has_down

    def upward(j):
        return j + jnp.where(lat <= j, 1, 0)

    def send_far():
        each(n_lat - 1, lambda j: pl.when(far_off(upward(j)))(lambda: start_small(upward(j))))
        each(n_lat - 1, lambda j: start_big(upward(j)))

    def far_off(peer):
        return (peer > lat + 1) | (peer < lat - 1)

    def send_near_small():
        pl.when(has_up)(lambda: start_small(lat - 1))
        pl.when(has_down)(lambda: start_small(lat + 1))

    def put_row(taps, r, v):
        taps[r * pitch : (r + 1) * pitch, 0:chans] = pltpu.roll(v, 1, 0).astype(BF16)
        taps[r * pitch : (r + 1) * pitch, chans : 2 * chans] = v.astype(BF16)
        taps[r * pitch : (r + 1) * pitch, 2 * chans :] = pltpu.roll(v, pitch - 1, 0).astype(BF16)

    def conv(taps, kind, first, count):
        acc = None
        for a in range(3):
            parts = [taps[(f + a) * pitch : (f + a + count) * pitch, :] for f in first]
            part = jnp.dot(jnp.concatenate(parts, axis=0), kw[kind, a], preferred_element_type=F32)
            acc = part if acc is None else acc + part
        return acc

    def edge_factor(r):
        if r == 0:
            return jnp.where(has_up, 1.0, 0.0)
        if r == rows + 1:
            return jnp.where(has_down, 1.0, 0.0)
        return None

    def guarded(dl, fn):
        if dl == 0:
            fn()
        else:
            pl.when(has_up if dl < 0 else has_down)(fn)

    def span(start, size):
        return pl.ds(start if isinstance(start, int) else pl.multiple_of(start, SIDE), size)

    def remote(buf, place, sr, dr, nr, sc, dc, nc, i):
        return pltpu.make_async_remote_copy(
            src_ref=buf.at[pl.ds(sr, nr), span(sc, nc)], dst_ref=buf.at[pl.ds(dr, nr), span(dc, nc)],
            send_sem=halo_s.at[i], recv_sem=halo_r.at[i], device_id=place, device_id_type=MESH,
        )

    span_r = {-1: (top, rows + top, HALO), 0: (top, top, rows), 1: (top + rows - HALO, 0, HALO)}
    span_c = {-1: (left, left + width, SIDE), 0: (left, left, width), 1: (left + width - SIDE, 0, SIDE)}

    def x_routes():
        routes = {-1: [], 1: []}
        for i, dl in enumerate((-1, 1)):
            sr, dr, nr = span_r[dl]
            for side in (-1, 1):
                sc, dc, nc = span_c[side]
                routes[dl].append(remote(X, at(dl, side), sr, dr, nr, sc, dc, nc, i))
        return routes, {-1: (X, HALO, 2 * SIDE, 0), 1: (X, HALO, 2 * SIDE, 1)}

    out_src = left + ch * (width - SIDE)
    out_dst = other * (left + width)

    def g_side():
        copy = remote(G, outward(0), top, top, rows, out_src, out_dst, SIDE, 4)
        return {0: [copy]}, {0: (G, rows, SIDE, 4)}

    def g_rows(depth):
        routes, whole = {}, {}
        for n, dl in enumerate((-1, 1)):
            i = 2 + n if depth == 0 else 5 + n
            sr = top + depth if dl < 0 else top + rows - 1 - depth
            dr = rows + top + depth if dl < 0 else HALO - 1 - depth
            routes[dl] = [
                remote(G, at(dl, 0), sr, dr, 1, other * SIDE, other * SIDE, reach, i),
                remote(G, outward(dl), sr, dr, 1, out_src, out_dst, SIDE, i),
            ]
            whole[dl] = (G, 1, pitch, i)
        return routes, whole

    def halo_start(halo, order):
        for dl in order:
            def go(dl=dl):
                for copy in halo[0][dl]:
                    copy.start()

            guarded(dl, go)

    def halo_finish(halo, order):
        for dl in order:
            def whole(dl=dl):
                buf, nr, nc, i = halo[1][dl]
                return remote(buf, sibling, 0, 0, nr, 0, 0, nc, i)

            guarded(dl, lambda: whole().wait_send())
            guarded(-dl, lambda: whole().wait_recv())

    def clear_poles(buf):
        @pl.when(lat == 0)
        def _():
            buf[0:HALO] = jnp.zeros((HALO, pitch, chans), BF16)

        @pl.when(lat == n_lat - 1)
        def _():
            buf[rows + HALO : rows + 2 * HALO] = jnp.zeros((HALO, pitch, chans), BF16)

    clear_poles(X)
    clear_poles(G)

    reshard.wait()
    for r in range(rows):
        X[top + r, left : left + width] = (
            jnp.concatenate([both[0, r], both[1, r]], axis=0).astype(F32).T.astype(BF16)
        )
    x_halo = x_routes()
    halo_start(x_halo, (-1, 1))

    send_near_small()

    @pl.when(middle)
    def _():
        @pl.when(lat >= 2)
        def _():
            pl.semaphore_wait(heard_up, 1)
            tell(heard_up, 1)

        @pl.when(lat <= n_lat - 3)
        def _():
            pl.semaphore_wait(heard_down, 1)
            tell(heard_down, -1)

        send_far()

    R[lat, ch] = pay[lat]
    own_at = pltpu.make_async_copy(pay_at.at[lat], at_s.at[lat], copy_sem)
    own_at.start()
    R_p[lat] = pay_p[lat]

    def forward(t, c):
        part = pl.ds(0, half * (1 + c))
        return pltpu.make_async_remote_copy(
            src_ref=R.at[t, c, :, part], dst_ref=R.at[t, c, :, part], send_sem=fwd_s, recv_sem=fwd_r.at[t],
            device_id=sibling, device_id_type=MESH,
        )

    def forward_small(t):
        return pltpu.make_async_remote_copy(
            src_ref=R_p.at[t], dst_ref=R_p.at[t], send_sem=fp_s, recv_sem=p_rs.at[t],
            device_id=sibling, device_id_type=MESH,
        )

    by_core(lambda c: forward(lat, c).start())
    for load in loads[7:]:
        load.wait()
    for kind, k in enumerate((kin, kout, kout, kin)):
        for a in range(3):
            for b in range(3):
                tap = k[a, b].astype(F32).T.astype(BF16) if kind < 2 else k[2 - a, 2 - b]
                kw[kind, a, b * chans : (b + 1) * chans] = tap
    Z[...] = jnp.zeros(Z.shape, F32)

    @pl.when(jnp.logical_not(middle))
    def _():
        @pl.when(lat >= 2)
        def _():
            pl.semaphore_wait(heard_up, 1)

        @pl.when(lat <= n_lat - 3)
        def _():
            pl.semaphore_wait(heard_down, 1)

        send_far()

    def hidden_rows(first, count):
        acc = conv(X3, 0, first, count) + bias[...]
        s = sigmoid(acc)
        steep = s * (1.0 + acc * (1.0 - s))
        h = acc * s
        for i, r in enumerate(f + n for f in first for n in range(count)):
            own = slice(i * pitch, (i + 1) * pitch)
            slope[r * pitch : (r + 1) * pitch, :] = steep[own]
            row = h[own]
            f = edge_factor(r)
            if f is not None:
                row = row * f
            put_row(H3, r, row.astype(BF16).astype(F32))

    edge_got(0, 3).wait_send()
    edge_got(1, 1).wait_recv()
    edge_got(0, 2).wait_recv()
    for side in (0, 1):
        turned = jnp.concatenate([edge_r[side, 0], edge_r[side, 1]], axis=0).astype(F32).T.astype(BF16)
        for r in range(rows):
            X[top + r, side * (left + width) : side * (left + width) + SIDE] = turned[r * SIDE : (r + 1) * SIDE]
    for r in range(top, top + rows):
        put_row(X3, r, X[r].astype(F32))
    for r0 in range(HALO, rows, 2):
        hidden_rows([r0], 2)
    def denoise_rows(first, count):
        acc = conv(H3, 1, first, count)
        for i, r in enumerate(f + n for f in first for n in range(count)):
            state = X[top + r, left : left + width].astype(F32)
            den = (state + acc[i * pitch + left : i * pitch + left + width]).astype(BF16)
            den_s[r] = den
            wide = den.astype(F32)
            base[r * width : (r + 1) * width, :] = keep_rate * state + blend_rate * wide
            DF[pl.ds(pl.multiple_of(r * cols + ch * width, width), width), :] = wide
        for f in first:
            part = pl.ds(f, count)
            pair_copy(den_s.at[part], den_r.at[part], 1).start()

    inner = [([r0], min(WIDE, rows - HALO - r0)) for r0 in range(HALO, rows - HALO, WIDE)]
    outer = [([0, rows - HALO], HALO)]
    for first, count in inner:
        denoise_rows(first, count)
    halo_finish(x_halo, (-1, 1))
    for dl in (-1, 1):
        @pl.when(has_up if dl < 0 else has_down)
        def _(dl=dl):
            pltpu.make_async_remote_copy(
                src_ref=x_send.at[pl.ds(0, 2 * HALO)], dst_ref=x_send.at[pl.ds(0, 2 * HALO)],
                send_sem=raw_s.at[1 if dl < 0 else 0], recv_sem=raw_r.at[0 if dl < 0 else 1],
                device_id=sibling, device_id_type=MESH,
            ).wait()
            for i in range(HALO):
                side = 0 if dl < 0 else 1
                X[side * (top + rows) + i, left : left + width] = (
                    jnp.concatenate([raw[side, 0, i], raw[side, 1, i]], axis=0).astype(F32).T.astype(BF16)
                )

    for r in (0, 1, top + rows, top + rows + 1):
        put_row(X3, r, X[r].astype(F32))
    hidden_rows([0, rows], HALO)
    for first, count in outer:
        denoise_rows(first, count)

    own_at.wait()
    pltpu.make_async_remote_copy(
        src_ref=pay_at.at[pl.ds(0, n_lat - 1)], dst_ref=at_s.at[pl.ds(0, n_lat - 1)], send_sem=at_ss, recv_sem=at_rs,
        device_id=sibling, device_id_type=MESH,
    ).wait_recv()

    def take_pay(j):
        peer = peer_of(j)

        def go(c):
            big(peer, peer, c).wait_recv()
            forward(peer, c).start()
            if c == 1:
                small(peer, peer, 1).wait_recv()
                forward_small(peer).start()

        by_core(go)

    def take_from(j0):
        each(n_lat - 1 - j0, lambda j: take_pay(j + j0))

    batches = slots // GROUP
    split = batches == 2
    if split:
        pl.when(jnp.logical_not(middle))(lambda: take_pay(0))
    pair_copy(den_s, den_r, 1).wait()
    for r in range(rows):
        DF[pl.ds(pl.multiple_of(r * cols + other * width, width), width), :] = den_r[r].astype(F32)

    def gather(t):
        lane = lax.broadcasted_iota(I32, (half, chans), 1)
        for k in range(CAP):
            r0 = at_s[t, 2 * k, 0]
            q0 = at_s[t, 2 * k + 1, 0]
            cut = [DF[pl.ds((r0 + a) * cols + q0, PW), :] for a in range(PH)]
            first = jnp.concatenate(cut[: PH // 2], axis=0)
            second = jnp.concatenate(cut[PH // 2 :], axis=0)
            patches[t, k, 0:half] = first.astype(BF16)
            patches[t, k, half:cells] = second.astype(BF16)
            keep_first = jnp.where(ch == 0, first, pltpu.roll(first, half, 1))
            keep_second = jnp.where(ch == 0, pltpu.roll(second, half, 1), second)
            pat_s[t, k] = jnp.where(lane < half, keep_first, keep_second).astype(BF16)

    each(n_lat, gather)

    def patch_copy(peer, landing):
        return pltpu.make_async_remote_copy(
            src_ref=pat_s.at[peer], dst_ref=pat_r.at[landing],
            send_sem=pat_ss, recv_sem=pat_rs,
            device_id={"lat": peer}, device_id_type=MESH,
        )

    each(n_lat - 1, lambda j: patch_copy(peer_of(j), lat).start())
    pat_r[lat] = pat_s[lat]
    start = ch * (cols - reach)

    def source_of(j):
        return jnp.where(j == 0, lat, peer_of(jnp.maximum(j - 1, 0)))

    def settle(t):
        by_core(lambda c: forward(t, 1 - c).wait_recv())

        @pl.when((ch == 0) & (t != lat))
        def _():
            forward_small(t).wait_recv()

    def drain(src, dst, sem):
        pltpu.make_async_remote_copy(
            src_ref=src, dst_ref=dst, send_sem=sem, recv_sem=pay_rs.at[0],
            device_id=sibling, device_id_type=MESH,
        ).wait_send()

    def drain_all():
        others = pl.ds(0, n_lat - 1)

        def go(c):
            part = pl.ds(0, half * (1 + c))
            drain(pay.at[others, :, part], R.at[others, c, :, part], pay_ss)
            drain(R.at[:, c, :, part], R.at[:, c, :, part], fwd_s)
            if c == 1:
                drain(pay_p.at[others], R_p.at[others], p_ss)
                drain(R_p.at[others], R_p.at[others], fp_s)

        by_core(go)
        drain(pay_at.at[others], at_s.at[others], at_ss)
        drain(pat_s.at[others], pat_r.at[others], pat_ss)

    g_halo = [g_rows(depth) for depth in range(HALO)]
    g_edge = g_side()

    def observe(g, first, last):
        owners = [source_of(g * sources + i) for i in range(sources)]
        for t in owners:
            settle(t)
        for i in range(GROUP):
            t, k = owners[i // CAP], i % CAP
            row, lane = corner()
            tri = R[t, 1, k, half:chans].astype(F32)
            upper = jnp.where((lane <= row) | (lane >= half), tri, 0.0)
            lower = jnp.where(lane > row + half, pltpu.roll(tri, half, 1), 0.0)
            lower = jnp.where(lane == row + half, R_p[t, k : k + 1, :], lower)
            side = jnp.concatenate([upper, lower], axis=0).astype(BF16)
            normal = side + side.T
            pull = jnp.concatenate([R[t, 0, k, 0:half], R[t, 1, k, 0:half]], axis=0)
            pulled = jnp.dot(normal, patches[t, k], preferred_element_type=F32) - pull.astype(F32).T
            for a in range(PH):
                Z[pl.ds((i * PH + a) * strip + reach, PW), :] = pulled[a * PW : (a + 1) * PW]
        for n, r in enumerate((0, rows - 1, 1, rows - 2, *range(2, rows - 2))):
            total = None
            for i in range(GROUP):
                t, k = owners[i // CAP], i % CAP
                r0 = at_s[t, 2 * k, 0]
                place = jnp.clip(at_s[t, 2 * k + 1, 0] - start, -PW, reach)
                inside = (r >= r0) & (r < r0 + PH)
                begin = jnp.where(inside, (i * PH + r - r0) * strip + reach - place, blank)
                v = Z[pl.ds(begin, reach), :]
                total = v if total is None else total + v
            span_w = pl.ds(pl.multiple_of(r * pitch + other * SIDE, SIDE), reach)
            if not first:
                total = total + GW[span_w, :]
            GW[span_w, :] = total
            if last:
                G[top + r, pl.ds(pl.multiple_of(other * SIDE, SIDE), reach)] = total.astype(BF16)
                if n in (1, 3):
                    halo_start(g_halo[n // 2], (-1, 1))
        if last:
            halo_start(g_edge, (0,))

    if split:
        pl.when(middle)(lambda: take_from(0))
    else:
        take_from(0)
    if split:
        observe(0, True, False)
        pl.when(jnp.logical_not(middle))(lambda: take_from(1))
        observe(1, False, True)
    elif batches == 1:
        observe(0, True, True)
    else:
        observe(0, True, False)
        lax.fori_loop(1, batches - 1, lambda g, _: observe(g, False, False) or 0, 0)
        observe(batches - 1, False, True)

    def grad_rows(first, count):
        back = conv(X3, 2, first, count)
        for i, r in enumerate(f + n for f in first for n in range(count)):
            row = back[i * pitch : (i + 1) * pitch] * slope[r * pitch : (r + 1) * pitch, :]
            f = edge_factor(r)
            if f is not None:
                row = row * f
            put_row(H3, r, row.astype(BF16).astype(F32))

    halo_finish(g_edge, (0,))
    for r in range(top, top + rows):
        put_row(X3, r, G[r].astype(F32))
    for r0 in range(HALO, rows, 2):
        grad_rows([r0], 2)

    def finish_rows(first, count, sem):
        acc = conv(H3, 3, first, count)
        order = [f + n for f in first for n in range(count)]
        kept = []
        for i, r in enumerate(order):
            grad = GW[r * pitch + left : r * pitch + left + width, :] + acc[i * pitch + left : i * pitch + left + width]
            res = (base[r * width : (r + 1) * width, :] - guide_rate * grad).T
            out_s[r] = jnp.where(ch == 0, res[half:chans], res[0:half]).astype(BF16)
            kept.append(jnp.where(ch == 0, res[0:half], res[half:chans]))
        for f in first:
            part = pl.ds(f, count)
            pair_copy(out_s.at[part], out_r.at[part], sem).start()
        for r, mine_r in zip(order, kept):
            out_h[0, pl.ds(r, half, stride=rows), :] = mine_r

    for first, count in inner:
        finish_rows(first, count, 2)
    for depth in range(HALO):
        halo_finish(g_halo[depth], (-1, 1))
        for r in (HALO - 1 - depth, top + rows + depth):
            put_row(X3, r, G[r].astype(F32))
        grad_rows([HALO - 1 - depth, rows + depth], 1)
        finish_rows([HALO - 1 - depth, rows - HALO + depth], 1, 3)
    mine = pl.ds(pl.multiple_of(ch * width, width), width)
    theirs = pl.ds(pl.multiple_of(other * width, width), width)
    out[:, mine] = out_h[0]

    others = pl.ds(0, n_lat - 1)
    pltpu.make_async_remote_copy(
        src_ref=pat_s.at[others], dst_ref=pat_r.at[others], send_sem=pat_ss, recv_sem=pat_rs,
        device_id=sibling, device_id_type=MESH,
    ).wait_recv()
    drain_all()

    def innovate(b):
        slot = plan[b]
        part = pat_r[slot // CAP, slot % CAP].astype(F32)
        patch = jnp.concatenate([part, pltpu.roll(part, half, 1)], axis=0).astype(BF16)
        predicted = jnp.dot(weight[b], patch, preferred_element_type=F32).T
        inn_out[b] = (predicted[0:half] - values[b].astype(F32)).astype(BF16)

    each(blocks, innovate)
    middle_rows = tuple(range(HALO, rows - HALO))
    edge_rows = (*range(HALO), *range(rows - HALO, rows))
    for sem, which in ((2, middle_rows), (3, edge_rows)):
        part = pl.ds(0, len(which))
        pair_copy(out_s.at[part], out_r.at[part], sem).wait()
        for r in which:
            out_h[1, pl.ds(r, half, stride=rows), :] = out_r[r].astype(F32)
    out[:, theirs] = out_h[1]


def store(out, innovation, out_hbm, innovation_hbm, sem):
    copies = [
        pltpu.make_async_copy(out, out_hbm, sem.at[0]),
        pltpu.make_async_copy(innovation, innovation_hbm, sem.at[1]),
    ]
    for copy in copies:
        copy.start()
    for copy in copies:
        copy.wait()


def body(n_lat, n_lon, noisy_state, kernel_in, bias_in, kernel_out, interp_weight, observed,
         obs_precision, dest_tile, row_offset, col_offset):
    half, rows, cols = noisy_state.shape
    chans = 2 * half
    width = cols // 2
    blocks, obs, cells = interp_weight.shape
    slots = n_lat * CAP
    pitch = width + 2 * SIDE
    reach = width + SIDE
    px = rows * width
    vmem = pl.BlockSpec(memory_space=pltpu.VMEM)
    hbm = pl.BlockSpec(memory_space=pltpu.HBM)
    dma = pltpu.SemaphoreType.DMA
    call = pl.pallas_call(
        functools.partial(kernel, n_lat, n_lon, rows, width, half, blocks),
        out_shape=(
            pltpu.VMEM((half * rows, cols), F32),
            pltpu.VMEM((blocks, half, obs), BF16),
        ),
        in_specs=[hbm] * 10,
        out_specs=(vmem, vmem),
        scratch_shapes=[
            pltpu.SMEM((blocks,), I32),
            pltpu.SMEM((blocks,), I32),
            pltpu.SMEM((blocks,), I32),
            pltpu.VMEM((1, chans), F32),
            pltpu.VMEM((half, rows, cols), BF16),
            pltpu.VMEM((2, half * rows, width), F32),
            pltpu.VMEM((rows, half, width), BF16),
            pltpu.VMEM(kernel_in.shape, BF16),
            pltpu.VMEM(kernel_out.shape, BF16),
            pltpu.VMEM(interp_weight.shape, BF16),
            pltpu.VMEM(observed.shape, BF16),
            pltpu.VMEM(obs_precision.shape, BF16),
            pltpu.VMEM(obs_precision.shape, F32),
            pltpu.VMEM((4, 3, 3 * chans, chans), BF16),
            dma((10,)),
            pltpu.VMEM((2, rows, half, width), BF16),
            pltpu.VMEM((4, half, width), BF16),
            pltpu.VMEM((2, 2, half, width), BF16),
            pltpu.VMEM((2, 2, HALO, half, width), BF16),
            dma, dma((2,)),
            dma((2,)), dma((2,)),
            pltpu.VMEM((rows + 4, pitch, chans), BF16),
            pltpu.VMEM(((rows + 4) * pitch, 3 * chans), BF16),
            pltpu.VMEM(((rows + 2) * pitch, 3 * chans), BF16),
            pltpu.VMEM(((rows + 2) * pitch, chans), F32),
            pltpu.VMEM((px, chans), F32),
            pltpu.VMEM((rows * cols, chans), F32),
            pltpu.VMEM((rows, width, chans), BF16),
            pltpu.VMEM((rows, width, chans), BF16),
            pltpu.VMEM((blocks, half, cells), F32),
            pltpu.VMEM((blocks, half, cells), F32),
            pltpu.VMEM((blocks, cells), F32),
            pltpu.VMEM((n_lat, CAP, chans, cells), BF16),
            pltpu.VMEM((n_lat, SMALL, obs), I32),
            pltpu.VMEM((n_lat, SMALL, obs), F32),
            pltpu.VMEM((n_lat, 2, CAP, chans, cells), BF16),
            pltpu.VMEM((n_lat, SMALL, obs), F32),
            pltpu.SMEM((n_lat, SMALL, obs), I32),
            pltpu.VMEM((n_lat, CAP, cells, chans), BF16),
            pltpu.VMEM((n_lat, CAP, half, chans), BF16),
            pltpu.VMEM((n_lat, CAP, half, chans), BF16),
            pltpu.VMEM((GROUP * PH * (2 * reach + PW) + reach, chans), F32),
            pltpu.VMEM((rows + 4, pitch, chans), BF16),
            pltpu.VMEM((rows * pitch, chans), F32),
            pltpu.VMEM((2, half * rows, width), F32),
            pltpu.VMEM((rows, half, width), BF16),
            pltpu.VMEM((rows, half, width), BF16),
            pltpu.SMEM((blocks,), I32),
            pltpu.SemaphoreType.REGULAR,
            pltpu.SemaphoreType.REGULAR,
            dma((7,)), dma((7,)),
            dma((4,)), dma((4,)),
            dma, dma((n_lat,)),
            dma, dma,
            dma, dma((n_lat,)),
            dma, dma((n_lat,)),
            dma,
            dma,
            dma, dma,
        ],
        compiler_params=pltpu.CompilerParams(
            collective_id=0, has_side_effects=True, vmem_limit_bytes=(63 if slots <= 2 * GROUP else 48) * 1024 * 1024
        ),
    )
    out, innovation = call(
        dest_tile, row_offset, col_offset, noisy_state, kernel_in, kernel_out,
        bias_in.reshape(1, chans), interp_weight, observed, obs_precision,
    )
    out, innovation = pl.pallas_call(
        store,
        out_shape=(
            jax.ShapeDtypeStruct((half * rows, cols), F32),
            jax.ShapeDtypeStruct((blocks, half, obs), BF16),
        ),
        in_specs=[vmem, vmem],
        out_specs=(hbm, hbm),
        scratch_shapes=[dma((2,))],
    )(*(pltpu.with_memory_space_constraint(a, pltpu.VMEM) for a in (out, innovation)))
    return out.reshape(half, rows, cols), innovation


def solution(mesh):
    return jax.shard_map(
        functools.partial(body, mesh.shape["lat"], mesh.shape["lon"]),
        mesh=mesh,
        in_specs=(
            P(("grp", "ch"), "lat", "lon"),
            P(),
            P(),
            P(),
            P(("grp", "lat", "lon"), None, None),
            P(("grp", "lat", "lon"), "ch", None),
            P(("grp", "lat", "lon"), None),
            P(("grp", "lat", "lon")),
            P(("grp", "lat", "lon")),
            P(("grp", "lat", "lon")),
        ),
        out_specs=(P(("grp", "ch"), "lat", "lon"), P(("grp", "lat", "lon"), "ch", None)),
        check_vma=False,
    )
```
